128 devices in a mesh: grp: 4 (over y), row: 32 (over z, x, core).
Axes of the slice: x: 4, y: 4, z: 4, core: 2. Of those that a mesh axis runs over, the one named last changes fastest.
Arguments:
- tiles: bfloat16 [4, 32, 32, 256, 256], P('grp', 'row'), may hold values from -0.046875 to 0.046875
- tile_rows: int32 [4, 32, 32], P('grp', 'row'), may hold values from 0 to 3, as said below
- tile_cols: int32 [4, 32, 32], P('grp', 'row'), may hold values from 0 to 31, as said below
- live_tiles: int32 [4, 32], P('grp', 'row'), may hold values from 16 to 32, as said below
- dual_shift: float32 [32768], P('row'), may hold values from 0.5 to 2
- start_block: float32 [32, 32768], P(None, 'row'), may hold values from -6 to 6
Outputs:
- projections: float32 [4, 32, 128], replicated
- factors: float32 [4, 32, 32], replicated
- next_block: float32 [32, 32768], P(None, 'row')
The draws below stay inside these ranges and needn't reach their ends.
Inputs may be any that keep to these rules, and one draw needn't show every extreme that they name: `tile_rows`: the tile slots of one device sit at distinct positions (block row, column block), padding slots included. `tile_cols`: column block j of group g is global block column (j // 1) * 4 + g * 1 + j % 1. Slots from live_tiles on are padding with arbitrary values; in every draw some device has all 32 slots live.
All inputs are finite; a program needn't handle non-finite values.
Results may differ from the reference program's by a relative error of at most 0.013.
Values may be sent and summed in bfloat16 or wider, within the bound.
A program may use at most 64 MiB of HBM per device.

```python
import math
import jax
import jax.numpy as jnp
from jax import lax

K = 32
BS = 256
BR_DEV = 4
KB = 32
ITERS = 4
N = 32768
QB = 1
NCG = 32
M = 128
N_GRP = 4
N_ROW = 32


def tile_slots(key):
    keys = jax.random.split(jax.random.fold_in(key, 7), N_GRP * N_ROW)
    slots = jax.vmap(lambda one_key: jax.random.permutation(one_key, BR_DEV * NCG)[:KB])(keys)
    return slots.reshape(N_GRP, N_ROW, KB).astype(jnp.int32)


def draw_tile_rows(key, part):
    return (tile_slots(key) // NCG).astype(jnp.int32)


def draw_tile_cols(key, part):
    return (tile_slots(key) % NCG).astype(jnp.int32)


def draw_live_tiles(key, part):
    count_key = jax.random.fold_in(key, 11)
    pick_key = jax.random.fold_in(key, 13)
    counts = jax.random.randint(count_key, (N_GRP * N_ROW,), KB // 2, KB + 1)
    picked = jax.random.randint(pick_key, (), 0, N_GRP * N_ROW)
    counts = jnp.where(jnp.arange(N_GRP * N_ROW) == picked, KB, counts)
    return counts.reshape(N_GRP, N_ROW).astype(jnp.int32)


def steps_of(own_key, shape, pieces, low, largest):
    level = 1.0
    for dim, shards_of in pieces:
        heights = jax.random.uniform(jax.random.fold_in(jax.random.fold_in(own_key, 6), dim), (shards_of,), jnp.float32, low / len(pieces), largest / len(pieces))
        level = level * jnp.repeat(jnp.exp(heights), shape[dim] // shards_of).reshape((-1,) + (1,) * (len(shape) - 1 - dim))
    return level


def noise(key, shape, width, reach, shards=(), dtype=jnp.bfloat16):
    array = jax.random.normal(key, shape, jnp.float32) * width
    if len(shards) > 0:
        array = steps_of(key, shape, shards, -0.22, 0.18) * array
    return jnp.clip(array, min=-reach, max=reach).astype(dtype)


def setup_inputs(seed: int = 0) -> dict:
    seeds = jax.random.split(jax.random.key(seed), 7)
    return {
        "tiles": noise(seeds[0], (N_GRP, N_ROW, KB, BS, BS), (KB * N_GRP * 2 * BS // BR_DEV) ** -0.5, 0.046875, ((0, 4), (1, 32))),
        "tile_rows": draw_tile_rows(jax.random.fold_in(seeds[6], 71), 0),
        "tile_cols": draw_tile_cols(jax.random.fold_in(seeds[6], 71), 0),
        "live_tiles": draw_live_tiles(jax.random.fold_in(seeds[6], 71), 0),
        "dual_shift": jnp.clip(jnp.exp(math.log(2.0) - 1.3862944 * jax.random.uniform(seeds[4], (N,), jnp.float32) ** steps_of(seeds[4], (N,), ((0, 32),), -0.2, 0.2)), 0.5, 2.0),
        "start_block": noise(seeds[5], (K, N), 1.0, 6.0, ((1, 32),), jnp.float32),
    }


def inner_product(left, right):
    return lax.dot_general(left.astype(jnp.float32), right.astype(jnp.float32), (((1,), (1,)), ((), ())), precision=lax.Precision.HIGHEST, preferred_element_type=jnp.float32)

def apply_matrix(left, right):
    return jnp.dot(left.astype(jnp.float32), right.astype(jnp.float32), precision=lax.Precision.HIGHEST, preferred_element_type=jnp.float32)

def operate(vectors, tiles, tile_rows, tile_cols, live_tiles):
    rounded = vectors.astype(jnp.bfloat16).astype(jnp.float32).reshape(K, N_ROW, BR_DEV, BS)

    def visit(device, totals):
        direct_sum, back_sum = totals
        group = (device // N_ROW).astype(jnp.int32)
        owner = (device % N_ROW).astype(jnp.int32)
        matrix = tiles[group, owner].astype(jnp.float32)
        rows_here = tile_rows[group, owner]
        cols_here = tile_cols[group, owner]
        live_mask = (jnp.arange(KB) < live_tiles[group, owner]).astype(jnp.float32)
        column_part = lax.dynamic_slice_in_dim(rounded, group * QB, QB, 2).reshape(K, NCG, BS)
        own_part = lax.dynamic_index_in_dim(rounded, owner, 1, False)
        forward = jnp.einsum('kbc,brc->kbr', column_part[:, cols_here], matrix)
        row_table = (rows_here[:, None] == jnp.arange(BR_DEV)[None, :]).astype(jnp.float32) * live_mask[:, None]
        direct = jnp.einsum('kbr,bi->kir', forward, row_table)
        backward = jnp.einsum('kbr,brc->kbc', own_part[:, rows_here], matrix)
        col_table = (cols_here[:, None] == jnp.arange(NCG)[None, :]).astype(jnp.float32) * live_mask[:, None]
        spread = jnp.einsum('kbc,bj->kjc', backward, col_table).reshape(K, N_ROW, QB, BS)
        old_direct = lax.dynamic_index_in_dim(direct_sum, owner, 1, False)
        direct_sum = lax.dynamic_update_index_in_dim(direct_sum, old_direct + direct, owner, 1)
        old_back = lax.dynamic_index_in_dim(back_sum, group, 2, False)
        back_sum = lax.dynamic_update_index_in_dim(back_sum, old_back + spread, group, 2)
        return (direct_sum, back_sum)
    begin = (jnp.zeros((K, N_ROW, BR_DEV, BS), jnp.float32), jnp.zeros((K, N_ROW, N_GRP, QB, BS), jnp.float32))
    direct_sum, back_sum = lax.fori_loop(0, N_GRP * N_ROW, visit, begin)
    return 0.5 * (direct_sum.reshape(K, N) + back_sum.reshape(K, N))

def orthonormal(block):
    lower_factor = jnp.linalg.cholesky(inner_product(block, block))
    return (lax.linalg.triangular_solve(lower_factor, block, left_side=True, lower=True), lower_factor)

def reference(tiles, tile_rows, tile_cols, live_tiles, dual_shift, start_block):
    current, unused = orthonormal(start_block)
    basis_rows = jnp.zeros((M, N), jnp.float32)
    proj_list = []
    factor_list = []
    for step_index in range(ITERS):
        basis_rows = basis_rows.at[step_index * K:(step_index + 1) * K].set(current)
        image = operate(current, tiles, tile_rows, tile_cols, live_tiles) - current * dual_shift[None, :]
        first_coef = inner_product(image, basis_rows)
        image = image - apply_matrix(first_coef, basis_rows)
        current, lower_factor = orthonormal(image)
        proj_list.append(first_coef)
        factor_list.append(lower_factor)
    return (jnp.stack(proj_list), jnp.stack(factor_list), current)
```

```python
import functools

import jax
import jax.numpy as jnp
from jax import lax
from jax.experimental import pallas as pl
from jax.experimental.pallas import tpu as pltpu
from jax.sharding import PartitionSpec as P

ITERS = 4
MESH = pl.DeviceIdType.MESH
HIGH = lax.Precision.HIGHEST
NT = (((1,), (1,)), ((), ()))
MIDDLE = 1.25


def dot_nt(a, b):
    return lax.dot_general(a, b, NT, precision=HIGH, preferred_element_type=jnp.float32)


def dot_nn(a, b):
    return jnp.dot(a, b, precision=HIGH, preferred_element_type=jnp.float32)


def factor_and_inverse(gram):
    n = gram.shape[0]
    row = lax.broadcasted_iota(jnp.int32, (n, 2 * n), 0)
    lane = lax.broadcasted_iota(jnp.int32, (n, 2 * n), 1)
    work = jnp.concatenate([gram, jnp.where(row == lane, 1.0, 0.0)[:, :n]], axis=1)
    lower = jnp.zeros((n, n), jnp.float32)
    pivots = jnp.zeros((n, 2 * n), jnp.float32)
    for k in range(n):
        column = jnp.broadcast_to(work[:, k : k + 1], (n, 2 * n))
        pivot_row = work[k : k + 1, :]
        pivot = column[k : k + 1, :]
        scale = 1.0 / pivot
        below = jnp.where(row > k, column, 0.0)
        lower = jnp.where((lane[:, :n] == k) & (row[:, :n] >= k), column[:, :n] * lax.rsqrt(pivot[:, :n]), lower)
        pivots = jnp.where(row == k, pivot, pivots)
        work = work - below * (pivot_row * scale)
    inverse = (work * lax.rsqrt(pivots))[:, n:]
    return lower, inverse


def kernel(
    steps, group_count, owner_count,
    start_ref, shift_ref, rows_ref, cols_ref, place_ref, tiles_hbm,
    proj_ref, fac_ref, next_ref,
    tiles_ref, products, gathered, stage, own, back_out, back_in, direct, direct_out, direct_in,
    pair_out, pair_in, dots_pair, dots_grp, dots_row, basis, images, current, operand, coef, last, tile_sem,
    gather_row_send, gather_row_recv, gather_grp_send, gather_grp_recv,
    back_send, back_recv, direct_send, direct_recv,
    dgrp_send, dgrp_recv, drow_send, drow_recv, last_send, last_recv,
    relay_send, pair_send, pair_recv, dpair_send, dpair_recv,
):
    g = lax.axis_index("grp")
    r = lax.axis_index("row")
    width = start_ref.shape[0]
    row_count = start_ref.shape[1]
    part = row_count // group_count
    tile_count = tiles_ref.shape[0]
    owned = row_count // tiles_ref.shape[1]
    chips = owner_count // 2
    chip, core = r // 2, lax.rem(r, 2)
    partner = chip * 2 + 1 - core
    chip_peers = [lax.rem(chip + d, chips) for d in range(1, chips)]
    row_peers = [peer * 2 + core for peer in chip_peers] + [partner]
    grp_peers = [lax.rem(g + d, group_count) for d in range(1, group_count)]

    load = pltpu.make_async_copy(tiles_hbm, tiles_ref, tile_sem)
    load.start()
    barrier = pltpu.get_barrier_semaphore()
    for peer in row_peers:
        pl.semaphore_signal(barrier, inc=1, device_id=(g, peer), device_id_type=MESH)
    for peer in grp_peers:
        pl.semaphore_signal(barrier, inc=1, device_id=(peer, r), device_id_type=MESH)
    pl.semaphore_wait(barrier, len(row_peers) + len(grp_peers))

    def to_row(peer, src, dst, send, recv):
        return pltpu.make_async_remote_copy(
            src_ref=src, dst_ref=dst, send_sem=send, recv_sem=recv,
            device_id=(g, peer), device_id_type=MESH,
        )

    def to_grp(peer, src, dst, send, recv):
        return pltpu.make_async_remote_copy(
            src_ref=src, dst_ref=dst, send_sem=send, recv_sem=recv,
            device_id=(peer, r), device_id_type=MESH,
        )

    def send_grp_dots(value):
        dots_grp[g] = value
        sends = []
        for peer in grp_peers:
            copy = to_grp(peer, dots_grp.at[g], dots_grp.at[g], dgrp_send.at[peer], dgrp_recv.at[g])
            copy.start()
            sends.append(copy)
        return sends

    def take_grp_dots():
        for peer in grp_peers:
            to_grp(peer, dots_grp.at[peer], dots_grp.at[peer], dgrp_send.at[peer], dgrp_recv.at[peer]).wait_recv()
        total = dots_grp[0]
        for index in range(1, group_count):
            total = total + dots_grp[index]
        return total

    def send_pair_dots(half, value):
        dots_pair[half, core] = value
        copy = to_row(
            partner, dots_pair.at[half, core], dots_pair.at[half, core], dpair_send, dpair_recv.at[half]
        )
        copy.start()
        return [copy]

    def send_row_dots(half):
        to_row(
            partner, dots_pair.at[half, 1 - core], dots_pair.at[half, 1 - core], dpair_send, dpair_recv.at[half]
        ).wait_recv()
        dots_row[half, chip] = dots_pair[half, 0] + dots_pair[half, 1]
        sends = []
        for peer in chip_peers:
            copy = to_row(
                peer * 2 + core, dots_row.at[half, chip], dots_row.at[half, chip],
                drow_send.at[peer], drow_recv.at[half, chip],
            )
            copy.start()
            sends.append(copy)
        return sends

    def take_row_dots(half):
        for peer in chip_peers:
            to_row(
                peer * 2 + core, dots_row.at[half, peer], dots_row.at[half, peer],
                drow_send.at[peer], drow_recv.at[half, peer],
            ).wait_recv()
        total = dots_row[half, 0]
        for index in range(1, chips):
            total = total + dots_row[half, index]
        return total

    fold = 128 // width

    def pack(square):
        height = width // fold
        return jnp.concatenate([square[i * height : (i + 1) * height] for i in range(fold)], axis=1)

    def unpack(packed):
        return jnp.concatenate([packed[:, i * width : (i + 1) * width] for i in range(fold)], axis=0)

    total_cols = steps * width

    def local_dots(block):
        dots = dot_nt(block, jnp.concatenate([basis[...], block], axis=0))
        return jnp.concatenate([dots[:, :total_cols], pack(dots[:, total_cols:])], axis=0)

    def finish_dots(summed):
        first = summed[:width]
        gram = unpack(summed[width:]) - dot_nt(first, first)
        lower, inverse = factor_and_inverse(gram)
        return first, lower, inverse

    basis[...] = jnp.zeros_like(basis)
    images[...] = jnp.zeros_like(images)
    coef[...] = jnp.zeros_like(coef)
    products[tile_count] = jnp.zeros((width, part), jnp.float32)
    mine = pl.ds(pl.multiple_of(g * part, part), part)
    current[...] = start_ref[:, mine]
    operand[...] = start_ref[:, mine].astype(jnp.bfloat16)
    shift = shift_ref[:, mine]
    load.wait()

    def back_product(slot):
        value = products[place_ref[slot]]
        for i in range(1, owned):
            value = value + products[place_ref[i * owner_count + slot]]
        return value

    def step_body(step, carry):
        half = lax.rem(step, 2)
        block = current[...]
        own[g] = operand[...]
        gathered[half, r] = operand[...]
        stage[r] = operand[...]
        sends = []
        for peer in grp_peers:
            copy = to_grp(peer, own.at[g], own.at[g], gather_grp_send.at[peer], gather_grp_recv.at[g])
            copy.start()
            sends.append(copy)
        for peer in row_peers:
            copy = to_row(
                peer, gathered.at[half, r], gathered.at[half, r],
                gather_row_send.at[peer], gather_row_recv.at[half, r],
            )
            copy.start()
            sends.append(copy)
        sends += send_grp_dots(local_dots(block))
        for peer in grp_peers:
            to_grp(peer, own.at[peer], own.at[peer], gather_grp_send.at[peer], gather_grp_recv.at[peer]).wait_recv()
        for k in range(tile_count):
            products[k] = jnp.dot(own[rows_ref[k]], tiles_ref[k], preferred_element_type=jnp.float32)
        for peer in chip_peers + [chip]:
            pair_out[peer] = back_product(peer * 2 + 1 - core).astype(jnp.bfloat16)
            copy = to_row(
                partner, pair_out.at[peer], pair_in.at[half, peer], pair_send.at[peer], pair_recv.at[half, peer]
            )
            copy.start()
            sends.append(copy)

        def take_pair(peer):
            to_row(
                partner, pair_out.at[peer], pair_in.at[half, peer], pair_send.at[peer], pair_recv.at[half, peer]
            ).wait_recv()
            return pair_in[half, peer].astype(jnp.float32)

        sends += send_pair_dots(half, take_grp_dots())
        for peer in chip_peers:
            back_out[peer] = (back_product(peer * 2 + core) + take_pair(peer)).astype(jnp.bfloat16)
            copy = to_row(
                peer * 2 + core, back_out.at[peer], back_in.at[half, chip],
                back_send.at[peer], back_recv.at[half, chip],
            )
            copy.start()
            sends.append(copy)
        total = back_product(r) + take_pair(chip)
        sends += send_row_dots(half)
        for peer in chip_peers:
            slot = peer * 2 + core
            to_row(
                slot, gathered.at[half, slot], gathered.at[half, slot],
                gather_row_send.at[slot], gather_row_recv.at[half, slot],
            ).wait_recv()
            copy = to_row(
                partner, gathered.at[half, slot], gathered.at[half, slot],
                relay_send.at[peer], gather_row_recv.at[half, slot],
            )
            copy.start()
            sends.append(copy)
            stage[slot] = gathered[half, slot]
        for peer in chip_peers + [chip]:
            slot = peer * 2 + 1 - core
            to_row(
                partner, gathered.at[half, slot], gathered.at[half, slot],
                relay_send.at[peer], gather_row_recv.at[half, slot],
            ).wait_recv()
            stage[slot] = gathered[half, slot]

        forward = jnp.zeros((part, owned * width), jnp.float32)
        for k in range(tile_count):
            vector = stage[cols_ref[k]]
            row = rows_ref[tile_count + k]
            spread = jnp.concatenate(
                [vector * jnp.where(row == i, 1.0, 0.0).astype(jnp.bfloat16) for i in range(owned)], axis=0
            )
            forward = forward + lax.dot_general(tiles_ref[k], spread, NT, preferred_element_type=jnp.float32)
        forward = forward.T
        for i in range(owned):
            direct[i] = forward[i * width : (i + 1) * width]
            direct_out[i] = forward[i * width : (i + 1) * width].astype(jnp.bfloat16)
        for peer in grp_peers:
            copy = to_grp(peer, direct_out.at[peer], direct_in.at[g], direct_send.at[peer], direct_recv.at[g])
            copy.start()
            sends.append(copy)
        total = total + direct[g]

        first, lower, inverse = finish_dots(take_row_dots(half))
        last_step = jnp.maximum(step - 1, 0)
        proj_ref[last_step] = first
        fac_ref[last_step] = lower
        now = dot_nn(inverse, block - dot_nn(first, basis[...]))
        rest = dot_nn(coef[...] - first, images[...])
        before = pl.ds(pl.multiple_of(last_step * width, width), width)
        place = pl.ds(pl.multiple_of(step * width, width), width)
        follow = jnp.where(step > 0, lower, 0.0).T
        ahead = now * (MIDDLE - shift) - dot_nn(follow, basis[before, :])
        lane = lax.broadcasted_iota(jnp.int32, (width, total_cols), 1)
        sub = lax.broadcasted_iota(jnp.int32, (width, total_cols), 0)
        wide = jnp.concatenate([follow] * (total_cols // width), axis=1)
        coef[...] = jnp.where(lane == step * width + sub, -MIDDLE, 0.0) + jnp.where(
            (lane >= last_step * width) & (lane < last_step * width + width), wide, 0.0
        )

        for peer in chip_peers:
            to_row(
                peer * 2 + core, back_out.at[peer], back_in.at[half, peer],
                back_send.at[peer], back_recv.at[half, peer],
            ).wait_recv()
            total = total + back_in[half, peer].astype(jnp.float32)
        for peer in grp_peers:
            to_grp(peer, direct_out.at[peer], direct_in.at[peer], direct_send.at[peer], direct_recv.at[peer]).wait_recv()
            total = total + direct_in[peer].astype(jnp.float32)
        image = dot_nn(inverse, 0.5 * total + rest)
        basis[place, :] = now
        images[place, :] = image
        current[...] = image - now * shift
        operand[...] = (image + ahead).astype(jnp.bfloat16)
        for copy in sends:
            copy.wait_send()
        return carry

    lax.fori_loop(0, steps, step_body, 0)

    block = current[...]
    sends = send_grp_dots(local_dots(block))
    sends += send_pair_dots(steps % 2, take_grp_dots())
    sends += send_row_dots(steps % 2)
    block_parts = take_row_dots(steps % 2)
    first, lower, inverse = finish_dots(block_parts)
    proj_ref[steps - 1] = first
    fac_ref[steps - 1] = lower
    last[g] = dot_nn(inverse, block - dot_nn(first, basis[...]))
    for peer in grp_peers:
        copy = to_grp(peer, last.at[g], last.at[g], last_send.at[peer], last_recv.at[g])
        copy.start()
        sends.append(copy)
    for peer in grp_peers:
        to_grp(peer, last.at[peer], last.at[peer], last_send.at[peer], last_recv.at[peer]).wait_recv()
    for index in range(group_count):
        next_ref[:, index * part : (index + 1) * part] = last[index]
    for copy in sends:
        copy.wait_send()


def hand_on(proj_in, fac_in, next_in, proj_ref, fac_ref, next_ref):
    proj_ref[...] = proj_in[...]
    fac_ref[...] = fac_in[...]
    next_ref[...] = next_in[...]


def per_device(tiles, tile_rows, tile_cols, live_tiles, dual_shift, start_block):
    matrix = tiles[0, 0]
    tile_count, edge = matrix.shape[0], matrix.shape[1]
    width, row_count = start_block.shape
    group_count = lax.axis_size("grp")
    owner_count = lax.axis_size("row")
    owned = row_count // edge
    part = row_count // group_count
    columns = part // edge * owner_count
    total_cols = ITERS * width
    order = jnp.arange(tile_count, dtype=jnp.int32)
    position = tile_rows[0, 0] * columns + tile_cols[0, 0]
    here = (position[None, :] == jnp.arange(owned * columns, dtype=jnp.int32)[:, None]) & (
        order < live_tiles[0, 0]
    )[None, :]
    place = tile_count - jnp.sum(jnp.where(here, tile_count - order[None, :], 0), axis=1).astype(jnp.int32)
    rows = jnp.concatenate([tile_rows[0, 0], jnp.where(order < live_tiles[0, 0], tile_rows[0, 0], owned)])
    cols = tile_cols[0, 0]

    vmem = pl.BlockSpec(memory_space=pltpu.VMEM)
    smem = pl.BlockSpec(memory_space=pltpu.SMEM)
    dma = pltpu.SemaphoreType.DMA
    packed = width + width * width // 128
    grp_sem = dma((group_count,))
    row_sem = dma((owner_count,))
    row_pair = dma((2, owner_count))
    shapes = (
            jax.ShapeDtypeStruct((ITERS, width, total_cols), jnp.float32),
            jax.ShapeDtypeStruct((ITERS, width, width), jnp.float32),
            jax.ShapeDtypeStruct((width, row_count), jnp.float32),
    )
    outs = pl.pallas_call(
        functools.partial(kernel, ITERS, group_count, owner_count),
        out_shape=shapes,
        in_specs=[vmem, vmem, smem, smem, smem, pl.BlockSpec(memory_space=pl.ANY)],
        out_specs=(vmem, vmem, vmem),
        scratch_shapes=[
            pltpu.VMEM(matrix.shape, jnp.bfloat16),
            pltpu.VMEM((tile_count + 1, width, part), jnp.float32),
            pltpu.VMEM((2, owner_count, width, part), jnp.bfloat16),
            pltpu.VMEM((owner_count, width, part), jnp.bfloat16),
            pltpu.VMEM((group_count, width, part), jnp.bfloat16),
            pltpu.VMEM((owner_count // 2, width, part), jnp.bfloat16),
            pltpu.VMEM((2, owner_count // 2, width, part), jnp.bfloat16),
            pltpu.VMEM((group_count, width, part), jnp.float32),
            pltpu.VMEM((group_count, width, part), jnp.bfloat16),
            pltpu.VMEM((group_count, width, part), jnp.bfloat16),
            pltpu.VMEM((owner_count // 2, width, part), jnp.bfloat16),
            pltpu.VMEM((2, owner_count // 2, width, part), jnp.bfloat16),
            pltpu.VMEM((2, 2, packed, total_cols), jnp.float32),
            pltpu.VMEM((group_count, packed, total_cols), jnp.float32),
            pltpu.VMEM((2, owner_count // 2, packed, total_cols), jnp.float32),
            pltpu.VMEM((total_cols, part), jnp.float32),
            pltpu.VMEM((total_cols, part), jnp.float32),
            pltpu.VMEM((width, part), jnp.float32),
            pltpu.VMEM((width, part), jnp.bfloat16),
            pltpu.VMEM((width, total_cols), jnp.float32),
            pltpu.VMEM((group_count, width, part), jnp.float32),
            pltpu.SemaphoreType.DMA,
            row_sem, row_pair, grp_sem, grp_sem,
            row_sem, row_pair, grp_sem, grp_sem,
            grp_sem, grp_sem, row_sem, row_pair, grp_sem, grp_sem,
            row_sem, row_sem, row_pair, dma, dma((2,)),
        ],
        compiler_params=pltpu.CompilerParams(
            collective_id=0, has_side_effects=True, vmem_limit_bytes=60 * 1024 * 1024
        ),
    )(start_block, dual_shift[None, :], rows, cols, place, matrix)
    return pl.pallas_call(hand_on, out_shape=shapes, in_specs=[vmem] * 3, out_specs=(vmem,) * 3)(*outs)


def solution(mesh):
    in_specs = (
        P("grp", "row", None, None, None),
        P("grp", "row", None),
        P("grp", "row", None),
        P("grp", "row"),
        P("row"),
        P(None, "row"),
    )
    out_specs = (P(), P(), P(None, "row"))
    return jax.shard_map(
        per_device, mesh=mesh, in_specs=in_specs, out_specs=out_specs, check_vma=False
    )
```

```python
import functools

import jax
import jax.numpy as jnp
from jax import lax
from jax.experimental import pallas as pl
from jax.experimental.pallas import tpu as pltpu
from jax.sharding import PartitionSpec as P

ITERS = 4
MESH = pl.DeviceIdType.MESH
HIGH = lax.Precision.HIGHEST
NT = (((1,), (1,)), ((), ()))
MIDDLE = 1.25
PANEL = 8


def dot_nt(a, b):
    return lax.dot_general(a, b, NT, precision=HIGH, preferred_element_type=jnp.float32)


def dot_nn(a, b):
    return jnp.dot(a, b, precision=HIGH, preferred_element_type=jnp.float32)


def factor_and_inverse(gram):
    n = gram.shape[0]
    row = lax.broadcasted_iota(jnp.int32, (n, 2 * n), 0)
    lane = lax.broadcasted_iota(jnp.int32, (n, 2 * n), 1)
    work = jnp.concatenate([gram, jnp.where(row == lane, 1.0, 0.0)[:, :n]], axis=1)
    lower = jnp.zeros((n, 2 * n), jnp.float32)
    scales = jnp.zeros((n, 2 * n), jnp.float32)
    for start in range(0, n, PANEL):
        columns = [jnp.broadcast_to(work[:, k : k + 1], (n, 2 * n)) for k in range(start, start + PANEL)]
        rows = [work[k : k + 1, :] for k in range(start, start + PANEL)]
        update = jnp.zeros((n, 2 * n), jnp.float32)
        for i in range(PANEL):
            k = start + i
            scale = lax.rsqrt(columns[i][k : k + 1, :])
            column = columns[i] * scale
            pivot_row = rows[i] * scale
            for later in range(i + 1, PANEL):
                weight = column[start + later : start + later + 1, :]
                columns[later] = columns[later] - column * weight
                rows[later] = rows[later] - pivot_row * weight
            update = update + jnp.where(row > k, column, 0.0) * pivot_row
            lower = jnp.where((lane == k) & (row >= k), column, lower)
            scales = jnp.where(row == k, scale, scales)
        work = work - update
    inverse = (work * scales)[:, n:]
    return lower[:, :n], inverse


def kernel(
    steps, group_count, owner_count,
    start_ref, shift_ref, rows_ref, cols_ref, live_ref, tiles_hbm,
    proj_ref, fac_ref, next_ref,
    tiles_ref, products, gathered, stage, history, own, own_history, back_out, back_in, direct, direct_out, direct_in,
    pair_out, pair_in, dots_grp, basis, images, current, operand, coef, transform, place_vector, place_ref, tile_sem, place_sem,
    gather_row_send, gather_row_recv, gather_grp_send, gather_grp_recv,
    back_send, back_recv, direct_send, direct_recv,
    dgrp_send, dgrp_recv, relay_send, pair_send, pair_recv,
):
    g = lax.axis_index("grp")
    r = lax.axis_index("row")
    width = start_ref.shape[0]
    row_count = start_ref.shape[1]
    part = row_count // group_count
    tile_count = tiles_ref.shape[0]
    owned = row_count // tiles_ref.shape[1]
    chips = owner_count // 2
    chip, core = r // 2, lax.rem(r, 2)
    partner = chip * 2 + 1 - core
    chip_peers = [lax.rem(chip + d, chips) for d in range(1, chips)]
    row_peers = [peer * 2 + core for peer in chip_peers] + [partner]
    grp_peers = [lax.rem(g + d, group_count) for d in range(1, group_count)]
    total_cols = steps * width

    load = pltpu.make_async_copy(tiles_hbm, tiles_ref, tile_sem)
    load.start()
    barrier = pltpu.get_barrier_semaphore()
    for peer in row_peers:
        pl.semaphore_signal(barrier, inc=1, device_id=(g, peer), device_id_type=MESH)
    for peer in grp_peers:
        pl.semaphore_signal(barrier, inc=1, device_id=(peer, r), device_id_type=MESH)

    lanes = lax.broadcasted_iota(jnp.int32, place_vector.shape, 1)
    place = jnp.full(place_vector.shape, tile_count, jnp.int32)
    for k in range(tile_count):
        position = jnp.where(k < live_ref[0, 0], rows_ref[k] * owner_count + cols_ref[k], -1)
        place = jnp.where(lanes == position, k, place)
    place_vector[...] = place
    place_copy = pltpu.make_async_copy(place_vector, place_ref, place_sem)
    place_copy.start()
    basis[...] = jnp.zeros_like(basis)
    images[...] = jnp.zeros_like(images)
    coef[...] = jnp.zeros_like(coef)
    transform[...] = jnp.zeros_like(transform)
    history[...] = jnp.zeros_like(history)
    products[tile_count] = jnp.zeros((width, part), jnp.float32)
    mine = pl.ds(pl.multiple_of(g * part, part), part)
    current[...] = start_ref[:, mine]
    operand[...] = start_ref[:, mine].astype(jnp.bfloat16)
    shift = shift_ref[:, mine]
    place_copy.wait()
    pl.semaphore_wait(barrier, len(row_peers) + len(grp_peers))

    def to_row(peer, src, dst, send, recv):
        return pltpu.make_async_remote_copy(
            src_ref=src, dst_ref=dst, send_sem=send, recv_sem=recv,
            device_id=(g, peer), device_id_type=MESH,
        )

    def to_grp(peer, src, dst, send, recv):
        return pltpu.make_async_remote_copy(
            src_ref=src, dst_ref=dst, send_sem=send, recv_sem=recv,
            device_id=(peer, r), device_id_type=MESH,
        )

    def send_vectors(half):
        own[g] = operand[...]
        gathered[half, r] = operand[...]
        stage[r] = operand[...]
        sends = []
        for peer in row_peers:
            copy = to_row(
                peer, gathered.at[half, r], gathered.at[half, r],
                gather_row_send.at[peer], gather_row_recv.at[half, r],
            )
            copy.start()
            sends.append(copy)
        for peer in grp_peers:
            copy = to_grp(peer, own.at[g], own.at[g], gather_grp_send.at[peer], gather_grp_recv.at[g])
            copy.start()
            sends.append(copy)
        return sends

    def take_own(step):
        for peer in grp_peers:
            to_grp(peer, own.at[peer], own.at[peer], gather_grp_send.at[peer], gather_grp_recv.at[peer]).wait_recv()
        rows = pl.ds(pl.multiple_of(step * width, width), width)
        for i in range(group_count):
            own_history[rows, i * part : (i + 1) * part] = own[i]

    def relay_vectors(half):
        sends = []
        for peer in chip_peers:
            slot = peer * 2 + core
            to_row(
                slot, gathered.at[half, slot], gathered.at[half, slot],
                gather_row_send.at[slot], gather_row_recv.at[half, slot],
            ).wait_recv()
            copy = to_row(
                partner, gathered.at[half, slot], gathered.at[half, slot],
                relay_send.at[peer], gather_row_recv.at[half, slot],
            )
            copy.start()
            sends.append(copy)
            stage[slot] = gathered[half, slot]
        return sends

    def take_relayed(half):
        for peer in [chip] + chip_peers:
            slot = peer * 2 + 1 - core
            to_row(
                partner, gathered.at[half, slot], gathered.at[half, slot],
                relay_send.at[peer], gather_row_recv.at[half, slot],
            ).wait_recv()
            stage[slot] = gathered[half, slot]

    fold = 128 // width

    def pack(square):
        height = width // fold
        return jnp.concatenate([square[i * height : (i + 1) * height] for i in range(fold)], axis=1)

    def unpack(packed):
        return jnp.concatenate([packed[:, i * width : (i + 1) * width] for i in range(fold)], axis=0)

    def send_dots(half):
        dots = jnp.zeros((total_cols + width, width), jnp.float32)
        for slot in range(owner_count):
            vector = stage[slot]
            dots = dots + lax.dot_general(
                jnp.concatenate([history[slot], vector], axis=0), vector, NT, preferred_element_type=jnp.float32
            )
        dots = dots.T
        dots_grp[half, g] = jnp.concatenate([dots[:, :total_cols], pack(dots[:, total_cols:])], axis=0)
        sends = []
        for peer in grp_peers:
            copy = to_grp(
                peer, dots_grp.at[half, g], dots_grp.at[half, g], dgrp_send.at[peer], dgrp_recv.at[half, g]
            )
            copy.start()
            sends.append(copy)
        return sends

    def take_dots(half):
        for peer in grp_peers:
            to_grp(
                peer, dots_grp.at[half, peer], dots_grp.at[half, peer], dgrp_send.at[peer], dgrp_recv.at[half, peer]
            ).wait_recv()
        summed = dots_grp[half, 0]
        for index in range(1, group_count):
            summed = summed + dots_grp[half, index]
        return summed

    def finish_dots(summed):
        cross = dot_nt(summed[:width], transform[...])
        gram = unpack(summed[width:]) - dot_nt(cross, cross)
        lower, inverse = factor_and_inverse(gram)
        return cross, lower, inverse

    def back_product(slot):
        value = products[place_ref[0, slot]]
        for i in range(1, owned):
            value = value + products[place_ref[0, i * owner_count + slot]]
        return value

    lane = lax.broadcasted_iota(jnp.int32, (width, total_cols), 1)
    sub = lax.broadcasted_iota(jnp.int32, (width, total_cols), 0)

    def step_body(step, carry):
        half = lax.rem(step, 2)
        sends = send_vectors(half)
        take_own(step)
        for k in range(tile_count):
            products[k] = jnp.dot(own[rows_ref[k]], tiles_ref[k], preferred_element_type=jnp.float32)
        for peer in chip_peers + [chip]:
            pair_out[peer] = back_product(peer * 2 + 1 - core).astype(jnp.bfloat16)
            copy = to_row(
                partner, pair_out.at[peer], pair_in.at[half, peer], pair_send.at[peer], pair_recv.at[half, peer]
            )
            copy.start()
            sends.append(copy)

        def take_pair(peer):
            to_row(
                partner, pair_out.at[peer], pair_in.at[half, peer], pair_send.at[peer], pair_recv.at[half, peer]
            ).wait_recv()
            return pair_in[half, peer].astype(jnp.float32)

        sends += relay_vectors(half)
        for peer in chip_peers:
            back_out[peer] = (back_product(peer * 2 + core) + take_pair(peer)).astype(jnp.bfloat16)
            copy = to_row(
                peer * 2 + core, back_out.at[peer], back_in.at[half, chip],
                back_send.at[peer], back_recv.at[half, chip],
            )
            copy.start()
            sends.append(copy)
        total = back_product(r) + take_pair(chip)
        take_relayed(half)
        sends += send_dots(half)
        forward = jnp.zeros((part, owned * width), jnp.float32)
        for k in range(tile_count):
            vector = stage[cols_ref[k]]
            row = jnp.where(k < live_ref[0, 0], rows_ref[k], owned)
            spread = jnp.concatenate(
                [vector * jnp.where(row == i, 1.0, 0.0).astype(jnp.bfloat16) for i in range(owned)], axis=0
            )
            forward = forward + lax.dot_general(tiles_ref[k], spread, NT, preferred_element_type=jnp.float32)
        forward = forward.T
        for i in range(owned):
            direct[i] = forward[i * width : (i + 1) * width]
            direct_out[i] = forward[i * width : (i + 1) * width].astype(jnp.bfloat16)
        for peer in grp_peers:
            copy = to_grp(peer, direct_out.at[peer], direct_in.at[g], direct_send.at[peer], direct_recv.at[g])
            copy.start()
            sends.append(copy)
        total = total + direct[g]
        place = pl.ds(pl.multiple_of(step * width, width), width)
        for slot in range(owner_count):
            history[slot, place, :] = stage[slot]

        summed = take_dots(half)
        cross, lower, inverse = finish_dots(summed)
        last_step = jnp.maximum(step - 1, 0)
        proj_ref[last_step] = cross + coef[...]
        fac_ref[last_step] = lower
        now = dot_nn(inverse, current[...] - dot_nn(cross, basis[...]))
        rest = dot_nn(cross, images[...])
        transform[place, :] = dot_nn(
            inverse, jnp.where(lane == step * width + sub, 1.0, 0.0) - dot_nn(cross, transform[...])
        )
        before = pl.ds(pl.multiple_of(last_step * width, width), width)
        follow = jnp.where(step > 0, lower, 0.0).T
        ahead = now * (MIDDLE - shift) - dot_nn(follow, basis[before, :])
        wide = jnp.concatenate([follow] * (total_cols // width), axis=1)
        coef[...] = jnp.where(lane == step * width + sub, -MIDDLE, 0.0) + jnp.where(
            (lane >= last_step * width) & (lane < last_step * width + width), wide, 0.0
        )
        basis[place, :] = now

        for peer in chip_peers:
            to_row(
                peer * 2 + core, back_out.at[peer], back_in.at[half, peer],
                back_send.at[peer], back_recv.at[half, peer],
            ).wait_recv()
            total = total + back_in[half, peer].astype(jnp.float32)
        for peer in grp_peers:
            to_grp(peer, direct_out.at[peer], direct_in.at[peer], direct_send.at[peer], direct_recv.at[peer]).wait_recv()
            total = total + direct_in[peer].astype(jnp.float32)
        image = dot_nn(inverse, 0.5 * total - rest)
        images[place, :] = image
        current[...] = image + ahead
        operand[...] = (image + ahead).astype(jnp.bfloat16)
        for copy in sends:
            copy.wait_send()
        return carry

    load.wait()
    lax.fori_loop(0, steps, step_body, 0)

    half = steps % 2
    sends = send_vectors(half)
    sends += relay_vectors(half)
    take_relayed(half)
    sends += send_dots(half)
    take_own(steps)
    summed = take_dots(half)
    cross, lower, inverse = finish_dots(summed)
    proj_ref[steps - 1] = cross + coef[...]
    fac_ref[steps - 1] = lower
    combine = jnp.concatenate([-dot_nn(inverse, dot_nn(cross, transform[...])), inverse], axis=1)
    high = combine.astype(jnp.bfloat16)
    low = (combine - high.astype(jnp.float32)).astype(jnp.bfloat16)
    both = jnp.dot(jnp.concatenate([high, low], axis=0), own_history[...], preferred_element_type=jnp.float32)
    next_ref[...] = both[:width] + both[width:]
    for copy in sends:
        copy.wait_send()


def hand_on(proj_in, fac_in, next_in, proj_ref, fac_ref, next_ref):
    proj_ref[...] = proj_in[...]
    fac_ref[...] = fac_in[...]
    next_ref[...] = next_in[...]


def per_device(tiles, tile_rows, tile_cols, live_tiles, dual_shift, start_block):
    matrix = tiles[0, 0]
    tile_count, edge = matrix.shape[0], matrix.shape[1]
    width, row_count = start_block.shape
    group_count = lax.axis_size("grp")
    owner_count = lax.axis_size("row")
    owned = row_count // edge
    part = row_count // group_count
    total_cols = ITERS * width
    vmem = pl.BlockSpec(memory_space=pltpu.VMEM)
    smem = pl.BlockSpec(memory_space=pltpu.SMEM)
    dma = pltpu.SemaphoreType.DMA
    packed = width + width * width // 128
    grp_sem = dma((group_count,))
    row_sem = dma((owner_count,))
    row_pair = dma((2, owner_count))
    shapes = (
            jax.ShapeDtypeStruct((ITERS, width, total_cols), jnp.float32),
            jax.ShapeDtypeStruct((ITERS, width, width), jnp.float32),
            jax.ShapeDtypeStruct((width, row_count), jnp.float32),
    )
    outs = pl.pallas_call(
        functools.partial(kernel, ITERS, group_count, owner_count),
        out_shape=shapes,
        in_specs=[vmem, vmem, smem, smem, smem, pl.BlockSpec(memory_space=pltpu.HBM)],
        out_specs=(vmem, vmem, vmem),
        scratch_shapes=[
            pltpu.VMEM(matrix.shape, jnp.bfloat16),
            pltpu.VMEM((tile_count + 1, width, part), jnp.float32),
            pltpu.VMEM((2, owner_count, width, part), jnp.bfloat16),
            pltpu.VMEM((owner_count, width, part), jnp.bfloat16),
            pltpu.VMEM((owner_count, total_cols, part), jnp.bfloat16),
            pltpu.VMEM((group_count, width, part), jnp.bfloat16),
            pltpu.VMEM((total_cols + width, row_count), jnp.bfloat16),
            pltpu.VMEM((owner_count // 2, width, part), jnp.bfloat16),
            pltpu.VMEM((2, owner_count // 2, width, part), jnp.bfloat16),
            pltpu.VMEM((group_count, width, part), jnp.float32),
            pltpu.VMEM((group_count, width, part), jnp.bfloat16),
            pltpu.VMEM((group_count, width, part), jnp.bfloat16),
            pltpu.VMEM((owner_count // 2, width, part), jnp.bfloat16),
            pltpu.VMEM((2, owner_count // 2, width, part), jnp.bfloat16),
            pltpu.VMEM((2, group_count, packed, total_cols), jnp.float32),
            pltpu.VMEM((total_cols, part), jnp.float32),
            pltpu.VMEM((total_cols, part), jnp.float32),
            pltpu.VMEM((width, part), jnp.float32),
            pltpu.VMEM((width, part), jnp.bfloat16),
            pltpu.VMEM((width, total_cols), jnp.float32),
            pltpu.VMEM((total_cols, total_cols), jnp.float32),
            pltpu.VMEM((8, owned * owner_count), jnp.int32),
            pltpu.SMEM((8, owned * owner_count), jnp.int32),
            dma, dma,
            row_sem, row_pair, grp_sem, grp_sem,
            row_sem, row_pair, grp_sem, grp_sem,
            grp_sem, dma((2, group_count)), row_sem, row_sem, row_pair,
        ],
        compiler_params=pltpu.CompilerParams(
            collective_id=0, has_side_effects=True, vmem_limit_bytes=24 * 1024 * 1024
        ),
    )(start_block, dual_shift[None, :], tile_rows[0, 0], tile_cols[0, 0], live_tiles, matrix)
    return pl.pallas_call(hand_on, out_shape=shapes, in_specs=[vmem] * 3, out_specs=(vmem,) * 3)(*outs)


def solution(mesh):
    in_specs = (
        P("grp", "row", None, None, None),
        P("grp", "row", None),
        P("grp", "row", None),
        P("grp", "row"),
        P("row"),
        P(None, "row"),
    )
    out_specs = (P(), P(), P(None, "row"))
    return jax.shard_map(
        per_device, mesh=mesh, in_specs=in_specs, out_specs=out_specs, check_vma=False
    )
```

```python
import functools

import jax
import jax.numpy as jnp
from jax import lax
from jax.experimental import pallas as pl
from jax.experimental.pallas import tpu as pltpu
from jax.sharding import PartitionSpec as P

ITERS = 4
MESH = pl.DeviceIdType.MESH
HIGH = lax.Precision.HIGHEST
NT = (((1,), (1,)), ((), ()))
MIDDLE = 1.25
PANEL = 8
SIDE = 4


def dot_nt(a, b):
    return lax.dot_general(a, b, NT, precision=HIGH, preferred_element_type=jnp.float32)


def dot_nn(a, b):
    return jnp.dot(a, b, precision=HIGH, preferred_element_type=jnp.float32)


def factor_and_inverse(gram):
    n = gram.shape[0]
    row = lax.broadcasted_iota(jnp.int32, (n, 2 * n), 0)
    lane = lax.broadcasted_iota(jnp.int32, (n, 2 * n), 1)
    work = jnp.concatenate([gram, jnp.where(row == lane, 1.0, 0.0)[:, :n]], axis=1)
    lower = jnp.zeros((n, 2 * n), jnp.float32)
    scales = jnp.zeros((n, 2 * n), jnp.float32)
    for start in range(0, n, PANEL):
        columns = [jnp.broadcast_to(work[:, k : k + 1], (n, 2 * n)) for k in range(start, start + PANEL)]
        rows = [work[k : k + 1, :] for k in range(start, start + PANEL)]
        update = jnp.zeros((n, 2 * n), jnp.float32)
        for i in range(PANEL):
            k = start + i
            scale = lax.rsqrt(columns[i][k : k + 1, :])
            column = columns[i] * scale
            pivot_row = rows[i] * scale
            for later in range(i + 1, PANEL):
                weight = column[start + later : start + later + 1, :]
                columns[later] = columns[later] - column * weight
                rows[later] = rows[later] - pivot_row * weight
            update = update + jnp.where(row > k, column, 0.0) * pivot_row
            lower = jnp.where((lane == k) & (row >= k), column, lower)
            scales = jnp.where(row == k, scale, scales)
        work = work - update
    inverse = (work * scales)[:, n:]
    return lower[:, :n], inverse


def kernel(
    steps, group_count, owner_count,
    start_ref, shift_ref, rows_ref, cols_ref, live_ref, tiles_hbm,
    proj_ref, fac_ref, next_ref,
    tiles_ref, turned, masks, products, gathered, stage, history, own, own_history, back_out, back_in, direct_out, direct_in,
    pair_out, pair_in, dots_grp, basis, images, transform, place_vector, place_ref, tile_sem, place_sem,
    gather_send, gather_recv, relay_send, relay_recv, own_send, own_recv,
    pair_send, pair_recv, back_send, back_recv, direct_send, direct_recv, dots_send, dots_recv,
):
    g = lax.axis_index("grp")
    r = lax.axis_index("row")
    width = start_ref.shape[0]
    row_count = start_ref.shape[1]
    part = row_count // group_count
    tile_count = tiles_ref.shape[0]
    owned = row_count // tiles_ref.shape[1]
    chips = owner_count // 2
    chip, core = r // 2, lax.rem(r, 2)
    partner = chip * 2 + 1 - core
    chip_x, chip_z = lax.rem(chip, SIDE), chip // SIDE

    def away(d):
        return min(d % SIDE, SIDE - d % SIDE) + min(d // SIDE, chips // SIDE - d // SIDE)

    offsets = sorted(range(1, chips), key=lambda d: -away(d))

    def chip_at(d, sign):
        z_count = chips // SIDE
        return lax.rem(chip_z + (sign * (d // SIDE)) % z_count, z_count) * SIDE + lax.rem(
            chip_x + (sign * (d % SIDE)) % SIDE, SIDE
        )

    sources = [chip_at(d, -1) for d in offsets]
    targets = [chip_at(d, 1) for d in offsets]
    grp_peers = [lax.rem(g + d, group_count) for d in range(1, group_count)]
    total_cols = steps * width

    barrier = pltpu.get_barrier_semaphore()
    for peer in targets:
        pl.semaphore_signal(barrier, inc=1, device_id=(g, peer * 2 + core), device_id_type=MESH)
    pl.semaphore_signal(barrier, inc=1, device_id=(g, partner), device_id_type=MESH)
    for peer in grp_peers:
        pl.semaphore_signal(barrier, inc=1, device_id=(peer, r), device_id_type=MESH)
    load = pltpu.make_async_copy(tiles_hbm, tiles_ref, tile_sem)
    load.start()

    def to_row(peer, src, dst, send, recv):
        return pltpu.make_async_remote_copy(
            src_ref=src, dst_ref=dst, send_sem=send, recv_sem=recv,
            device_id=(g, peer), device_id_type=MESH,
        )

    def to_grp(peer, src, dst, send, recv):
        return pltpu.make_async_remote_copy(
            src_ref=src, dst_ref=dst, send_sem=send, recv_sem=recv,
            device_id=(peer, r), device_id_type=MESH,
        )

    others = group_count - 1

    def send_vectors(half, operand):
        gathered[half, r] = operand
        own[g] = operand
        for peer in grp_peers:
            to_grp(peer, own.at[g], own.at[g], own_send, own_recv).start()
        for i, peer in enumerate(targets):
            to_row(
                peer * 2 + core, gathered.at[half, r], gathered.at[half, r], gather_send, gather_recv.at[i]
            ).start()
        to_row(partner, gathered.at[half, r], gathered.at[half, r], gather_send, relay_recv.at[half]).start()
        stage[r] = operand

    def sent_vectors():
        bulk = gathered.at[0, pl.ds(0, chips)]
        to_row(partner, bulk, bulk, gather_send, gather_send).wait_send()
        bulk = own.at[pl.ds(0, others)]
        to_grp(grp_peers[0], bulk, bulk, own_send, own_send).wait_send()

    def take_own():
        bulk = own.at[pl.ds(0, others)]
        to_grp(grp_peers[0], bulk, bulk, own_recv, own_recv).wait_recv()

    def keep_own(step):
        for i in range(group_count):
            own_history[step * width : (step + 1) * width, i * part : (i + 1) * part] = own[i]

    def relay_vectors(half):
        for i, peer in reversed(list(enumerate(sources))):
            slot = peer * 2 + core
            block = gathered.at[half, slot]
            to_row(slot, block, block, gather_send, gather_recv.at[i]).wait_recv()
            to_row(partner, block, block, relay_send, relay_recv.at[half]).start()
            stage[slot] = gathered[half, slot]

    def relays_sent():
        bulk = gathered.at[0, pl.ds(0, chips - 1)]
        to_row(partner, bulk, bulk, relay_send, relay_send).wait_send()

    def take_relayed(half):
        bulk = gathered.at[half, pl.ds(0, chips)]
        to_row(partner, bulk, bulk, gather_send, relay_recv.at[half]).wait_recv()
        for peer in range(chips):
            slot = peer * 2 + 1 - core
            stage[slot] = gathered[half, slot]

    fold = 128 // width

    def pack(square):
        height = width // fold
        return jnp.concatenate([square[i * height : (i + 1) * height] for i in range(fold)], axis=1)

    def unpack(packed):
        return jnp.concatenate([packed[:, i * width : (i + 1) * width] for i in range(fold)], axis=0)

    def part_dots(step, parity):
        dots = jnp.zeros(((step + 1) * width, width), jnp.float32)
        for peer in range(chips):
            slot = peer * 2 + parity
            vector = stage[slot]
            left = vector
            if step > 0:
                left = jnp.concatenate([history[slot, : step * width, :], vector], axis=0)
            dots = dots + lax.dot_general(left, vector, NT, preferred_element_type=jnp.float32)
        return dots

    def send_dots(step, half, dots):
        height = width // fold
        dots_grp[half, g, :height] = pack(dots[step * width :])
        if step > 0:
            old = dots[: step * width]
            if step < steps:
                old = jnp.concatenate([old, jnp.zeros((total_cols - step * width, width), jnp.float32)], axis=0)
            dots_grp[half, g, height:] = old.T
        rows = height if step == 0 else height + width
        for peer in grp_peers:
            to_grp(
                peer, dots_grp.at[half, g, pl.ds(0, rows)], dots_grp.at[half, g, pl.ds(0, rows)],
                dots_send, dots_recv.at[half],
            ).start()

    def dots_bulk(step, half):
        height = width // fold
        return dots_grp.at[half, pl.ds(0, others), pl.ds(0, height if step == 0 else height + width)]

    def take_dots(step, half):
        height = width // fold
        bulk = dots_bulk(step, half)
        to_grp(grp_peers[0], bulk, bulk, dots_send, dots_recv.at[half]).wait_recv()
        rows = height if step == 0 else height + width
        summed = dots_grp[half, 0, :rows]
        for index in range(1, group_count):
            summed = summed + dots_grp[half, index, :rows]
        gram = unpack(summed[:height])
        if step == 0:
            return None, gram
        cross = dot_nt(summed[height:], transform[...])
        return cross, gram - dot_nt(cross, cross)

    def dots_sent(step, half):
        bulk = dots_bulk(step, half)
        to_grp(grp_peers[0], bulk, bulk, dots_send, dots_recv.at[half]).wait_send()

    def back_product(slot):
        value = products[place_ref[0, slot]]
        for i in range(1, owned):
            value = value + products[place_ref[0, i * owner_count + slot]]
        return value

    def take_pair(peer, half):
        return pair_in[half, peer].astype(jnp.float32)

    mine = pl.ds(pl.multiple_of(g * part, part), part)
    current = start_ref[:, mine]
    shift = shift_ref[:, mine]
    pl.semaphore_wait(barrier, chips + others)
    send_vectors(0, current.astype(jnp.bfloat16))
    lanes = lax.broadcasted_iota(jnp.int32, place_vector.shape, 1)
    place = jnp.full(place_vector.shape, tile_count, jnp.int32)
    for k in range(tile_count):
        alive = k < live_ref[0]
        position = jnp.where(alive, rows_ref[k] * owner_count + cols_ref[k], -1)
        place = jnp.where(lanes == position, k, place)
        row = jnp.full((16, 128), jnp.where(alive, rows_ref[k], -1), jnp.int32)
        for i in range(owned):
            masks[k, i] = jnp.where(row == i, 1.0, 0.0).astype(jnp.bfloat16)
    place_vector[...] = place
    place_copy = pltpu.make_async_copy(place_vector, place_ref, place_sem)
    place_copy.start()
    basis[...] = jnp.zeros_like(basis)
    images[...] = jnp.zeros_like(images)
    transform[...] = jnp.zeros_like(transform)
    products[tile_count] = jnp.zeros((width, part), jnp.float32)
    load.wait()

    def turn(j, carry):
        for i in range(4):
            turned[j * 4 + i] = tiles_ref[j * 4 + i].T
        return carry

    lax.fori_loop(0, tile_count // 4, turn, 0)
    place_copy.wait()

    coef = None
    lane = lax.broadcasted_iota(jnp.int32, (width, total_cols), 1)
    sub = lax.broadcasted_iota(jnp.int32, (width, total_cols), 0)
    for step in range(steps):
        half = step % 2
        take_own()
        for k in range(tile_count):
            products[k] = jnp.dot(own[rows_ref[k]], tiles_ref[k], preferred_element_type=jnp.float32)
        for i, peer in enumerate(targets + [chip]):
            pair_out[peer] = back_product(peer * 2 + 1 - core).astype(jnp.bfloat16)
            to_row(partner, pair_out.at[peer], pair_in.at[half, peer], pair_send, pair_recv.at[half]).start()
        keep_own(step)
        relay_vectors(half)
        dots = part_dots(step, core)
        to_row(partner, pair_out, pair_in.at[half], pair_send, pair_recv.at[half]).wait_recv()
        for peer in targets:
            back_out[peer] = (back_product(peer * 2 + core) + take_pair(peer, half)).astype(jnp.bfloat16)
            to_row(peer * 2 + core, back_out.at[peer], back_in.at[half, chip], back_send, back_recv.at[half]).start()
        total = back_product(r) + take_pair(chip, half)
        take_relayed(half)
        send_dots(step, half, dots + part_dots(step, 1 - core))
        forward = jnp.zeros((owned * width, part), jnp.float32)
        for k in range(tile_count):
            vector = stage[cols_ref[k]]
            spread = []
            for i in range(owned):
                mask = masks[k, i]
                mask = jnp.concatenate([jnp.concatenate([mask, mask], axis=1)] * (width // 16), axis=0)
                spread.append(vector * mask)
            forward = forward + jnp.dot(
                jnp.concatenate(spread, axis=0), turned[k], preferred_element_type=jnp.float32
            )
        for i in range(owned):
            direct_out[i] = forward[i * width : (i + 1) * width].astype(jnp.bfloat16)
        for peer in grp_peers:
            to_grp(peer, direct_out.at[peer], direct_in.at[g], direct_send, direct_recv).start()
        for i in range(owned):
            total = total + forward[i * width : (i + 1) * width] * jnp.where(g == i, 1.0, 0.0)
        for slot in range(owner_count):
            history[slot, step * width : (step + 1) * width, :] = stage[slot]
        sent_vectors()
        relays_sent()
        cross, gram = take_dots(step, half)
        left, rest = current, None
        if step > 0:
            left = left - dot_nn(cross, basis[...])
            rest = dot_nn(cross, images[...])
        lower, inverse = factor_and_inverse(gram)
        now = dot_nn(inverse, left)
        ahead = now * (MIDDLE - shift)
        if step > 0:
            follow = lower.T
            ahead = ahead - dot_nn(follow, basis[(step - 1) * width : step * width, :])
        bulk = back_in.at[half, pl.ds(0, chips - 1)]
        to_row(partner, bulk, bulk, back_send, back_recv.at[half]).wait_recv()
        for peer in sources:
            total = total + back_in[half, peer].astype(jnp.float32)
        bulk = direct_in.at[pl.ds(0, others)]
        to_grp(grp_peers[0], bulk, bulk, direct_send, direct_recv).wait_recv()
        for peer in grp_peers:
            total = total + direct_in[peer].astype(jnp.float32)
        total = 0.5 * total
        if step > 0:
            total = total - rest
        image = dot_nn(inverse, total)
        current = image + ahead
        send_vectors(1 - half, current.astype(jnp.bfloat16))
        basis[step * width : (step + 1) * width, :] = now
        images[step * width : (step + 1) * width, :] = image
        if step > 0:
            proj_ref[step - 1] = cross + coef
            fac_ref[step - 1] = lower
        unit = jnp.where(lane == step * width + sub, 1.0, 0.0)
        if step == 0:
            transform[:width, :] = dot_nn(inverse, unit)
            coef = -MIDDLE * unit
        else:
            transform[step * width : (step + 1) * width, :] = dot_nn(inverse, unit - dot_nn(cross, transform[...]))
            wide = jnp.concatenate([follow] * (total_cols // width), axis=1)
            coef = -MIDDLE * unit + jnp.where((lane >= (step - 1) * width) & (lane < step * width), wide, 0.0)
        to_row(partner, pair_out, pair_out, pair_send, pair_recv.at[half]).wait_send()
        bulk = back_out.at[pl.ds(0, chips - 1)]
        to_row(partner, bulk, bulk, back_send, back_recv.at[half]).wait_send()
        bulk = direct_out.at[pl.ds(0, others)]
        to_grp(grp_peers[0], bulk, bulk, direct_send, direct_recv).wait_send()
        dots_sent(step, half)

    half = steps % 2
    take_own()
    keep_own(steps)
    relay_vectors(half)
    dots = part_dots(steps, core)
    take_relayed(half)
    send_dots(steps, half, dots + part_dots(steps, 1 - core))
    sent_vectors()
    relays_sent()
    cross, gram = take_dots(steps, half)
    lower, inverse = factor_and_inverse(gram)
    proj_ref[steps - 1] = cross + coef
    fac_ref[steps - 1] = lower
    combine = jnp.concatenate([-dot_nn(inverse, dot_nn(cross, transform[...])), inverse], axis=1)
    high = combine.astype(jnp.bfloat16)
    low = (combine - high.astype(jnp.float32)).astype(jnp.bfloat16)
    both = jnp.dot(jnp.concatenate([high, low], axis=0), own_history[...], preferred_element_type=jnp.float32)
    next_ref[...] = both[:width] + both[width:]
    dots_sent(steps, half)


def hand_on(proj_in, fac_in, next_in, proj_ref, fac_ref, next_ref):
    proj_ref[...] = proj_in[...]
    fac_ref[...] = fac_in[...]
    next_ref[...] = next_in[...]


def per_device(tiles, tile_rows, tile_cols, live_tiles, dual_shift, start_block):
    matrix = tiles[0, 0]
    tile_count, edge = matrix.shape[0], matrix.shape[1]
    width, row_count = start_block.shape
    group_count = lax.axis_size("grp")
    owner_count = lax.axis_size("row")
    owned = row_count // edge
    part = row_count // group_count
    total_cols = ITERS * width
    vmem = pl.BlockSpec(memory_space=pltpu.VMEM)
    smem = pl.BlockSpec(memory_space=pltpu.SMEM)
    dma = pltpu.SemaphoreType.DMA
    packed = width + width * width // 128
    shapes = (
            jax.ShapeDtypeStruct((ITERS, width, total_cols), jnp.float32),
            jax.ShapeDtypeStruct((ITERS, width, width), jnp.float32),
            jax.ShapeDtypeStruct((width, row_count), jnp.float32),
    )
    outs = pl.pallas_call(
        functools.partial(kernel, ITERS, group_count, owner_count),
        out_shape=shapes,
        in_specs=[vmem, vmem, smem, smem, smem, pl.BlockSpec(memory_space=pltpu.HBM)],
        out_specs=(vmem, vmem, vmem),
        scratch_shapes=[
            pltpu.VMEM(matrix.shape, jnp.bfloat16),
            pltpu.VMEM(matrix.shape, jnp.bfloat16),
            pltpu.VMEM((tile_count, owned, 16, 128), jnp.bfloat16),
            pltpu.VMEM((tile_count + 1, width, part), jnp.float32),
            pltpu.VMEM((2, owner_count, width, part), jnp.bfloat16),
            pltpu.VMEM((owner_count, width, part), jnp.bfloat16),
            pltpu.VMEM((owner_count, total_cols, part), jnp.bfloat16),
            pltpu.VMEM((group_count, width, part), jnp.bfloat16),
            pltpu.VMEM((total_cols + width, row_count), jnp.bfloat16),
            pltpu.VMEM((owner_count // 2, width, part), jnp.bfloat16),
            pltpu.VMEM((2, owner_count // 2, width, part), jnp.bfloat16),
            pltpu.VMEM((group_count, width, part), jnp.bfloat16),
            pltpu.VMEM((group_count, width, part), jnp.bfloat16),
            pltpu.VMEM((owner_count // 2, width, part), jnp.bfloat16),
            pltpu.VMEM((2, owner_count // 2, width, part), jnp.bfloat16),
            pltpu.VMEM((2, group_count, packed, total_cols), jnp.float32),
            pltpu.VMEM((total_cols, part), jnp.float32),
            pltpu.VMEM((total_cols, part), jnp.float32),
            pltpu.VMEM((total_cols, total_cols), jnp.float32),
            pltpu.VMEM((8, owned * owner_count), jnp.int32),
            pltpu.SMEM((8, owned * owner_count), jnp.int32),
            dma, dma,
            dma, dma((owner_count // 2 - 1,)), dma, dma((2,)), dma, dma,
            dma, dma((2,)), dma, dma((2,)), dma, dma, dma, dma((2,)),
        ],
        compiler_params=pltpu.CompilerParams(
            collective_id=0, has_side_effects=True, vmem_limit_bytes=60 * 1024 * 1024
        ),
    )(start_block, dual_shift[None, :], tile_rows[0, 0], tile_cols[0, 0], live_tiles[0], matrix)
    return pl.pallas_call(hand_on, out_shape=shapes, in_specs=[vmem] * 3, out_specs=(vmem,) * 3)(*outs)


def solution(mesh):
    in_specs = (
        P("grp", "row", None, None, None),
        P("grp", "row", None),
        P("grp", "row", None),
        P("grp", "row"),
        P("row"),
        P(None, "row"),
    )
    out_specs = (P(), P(), P(None, "row"))
    return jax.shard_map(
        per_device, mesh=mesh, in_specs=in_specs, out_specs=out_specs, check_vma=False
    )
```

```python
import functools

import jax
import jax.numpy as jnp
from jax import lax
from jax.experimental import pallas as pl
from jax.experimental.pallas import tpu as pltpu
from jax.sharding import PartitionSpec as P

ITERS = 4
MESH = pl.DeviceIdType.MESH
HIGH = lax.Precision.HIGHEST
NT = (((1,), (1,)), ((), ()))
MIDDLE = 1.25
PANEL = 8
SIDE = 4


def dot_nt(a, b):
    return lax.dot_general(a, b, NT, precision=HIGH, preferred_element_type=jnp.float32)


def dot_nn(a, b):
    return jnp.dot(a, b, precision=HIGH, preferred_element_type=jnp.float32)


def factor_and_inverse(gram):
    n = gram.shape[0]
    row = lax.broadcasted_iota(jnp.int32, (n, 2 * n), 0)
    lane = lax.broadcasted_iota(jnp.int32, (n, 2 * n), 1)
    work = jnp.concatenate([gram, jnp.where(row == lane, 1.0, 0.0)[:, :n]], axis=1)
    lower = jnp.zeros((n, 2 * n), jnp.float32)
    scales = jnp.zeros((n, 2 * n), jnp.float32)
    for start in range(0, n, PANEL):
        columns = [jnp.broadcast_to(work[:, k : k + 1], (n, 2 * n)) for k in range(start, start + PANEL)]
        rows = [work[k : k + 1, :] for k in range(start, start + PANEL)]
        update = jnp.zeros((n, 2 * n), jnp.float32)
        for i in range(PANEL):
            k = start + i
            scale = lax.rsqrt(columns[i][k : k + 1, :])
            column = columns[i] * scale
            pivot_row = rows[i] * scale
            for later in range(i + 1, PANEL):
                weight = column[start + later : start + later + 1, :]
                columns[later] = columns[later] - column * weight
                rows[later] = rows[later] - pivot_row * weight
            update = update + jnp.where(row > k, column, 0.0) * pivot_row
            lower = jnp.where((lane == k) & (row >= k), column, lower)
            scales = jnp.where(row == k, scale, scales)
        work = work - update
    inverse = (work * scales)[:, n:]
    return lower[:, :n], inverse


def kernel(
    steps, group_count, owner_count,
    start_ref, shift_ref, rows_ref, cols_ref, live_ref, tiles_hbm,
    proj_ref, fac_ref, next_ref,
    tiles_ref, turned, masks, products, gathered, stage, history, own, own_history, back_out, back_in, direct_out, direct_in,
    pair_out, pair_in, dots_pair, dots_grp, basis, images, transform, place_vector, place_ref, tile_sem, place_sem,
    gather_send, gather_recv, relay_send, relay_recv, own_send, own_recv,
    pair_send, pair_recv, back_send, back_recv, direct_send, direct_recv, dots_send, dots_recv, dpair_send, dpair_recv,
):
    g = lax.axis_index("grp")
    r = lax.axis_index("row")
    width = start_ref.shape[0]
    row_count = start_ref.shape[1]
    part = row_count // group_count
    tile_count = tiles_ref.shape[0]
    owned = row_count // tiles_ref.shape[1]
    chips = owner_count // 2
    chip, core = r // 2, lax.rem(r, 2)
    partner = chip * 2 + 1 - core
    chip_x, chip_z = lax.rem(chip, SIDE), chip // SIDE

    def away(d):
        return min(d % SIDE, SIDE - d % SIDE) + min(d // SIDE, chips // SIDE - d // SIDE)

    offsets = sorted(range(1, chips), key=lambda d: -away(d))

    def chip_at(d, sign):
        z_count = chips // SIDE
        return lax.rem(chip_z + (sign * (d // SIDE)) % z_count, z_count) * SIDE + lax.rem(
            chip_x + (sign * (d % SIDE)) % SIDE, SIDE
        )

    sources = [chip_at(d, -1) for d in offsets]
    targets = [chip_at(d, 1) for d in offsets]
    grp_order = sorted(range(1, group_count), key=lambda d: -min(d, group_count - d))
    grp_peers = [lax.rem(g + d, group_count) for d in grp_order]
    total_cols = steps * width

    barrier = pltpu.get_barrier_semaphore()
    for peer in targets:
        pl.semaphore_signal(barrier, inc=1, device_id=(g, peer * 2 + core), device_id_type=MESH)
    pl.semaphore_signal(barrier, inc=1, device_id=(g, partner), device_id_type=MESH)
    for peer in grp_peers:
        pl.semaphore_signal(barrier, inc=1, device_id=(peer, r), device_id_type=MESH)
    load = pltpu.make_async_copy(tiles_hbm, tiles_ref, tile_sem)
    load.start()

    def to_row(peer, src, dst, send, recv):
        return pltpu.make_async_remote_copy(
            src_ref=src, dst_ref=dst, send_sem=send, recv_sem=recv,
            device_id=(g, peer), device_id_type=MESH,
        )

    def to_grp(peer, src, dst, send, recv):
        return pltpu.make_async_remote_copy(
            src_ref=src, dst_ref=dst, send_sem=send, recv_sem=recv,
            device_id=(peer, r), device_id_type=MESH,
        )

    others = group_count - 1

    def send_vectors(half, operand, relayed=True):
        gathered[half, r] = operand
        own[g] = operand
        for peer in grp_peers:
            to_grp(peer, own.at[g], own.at[g], own_send, own_recv).start()
        for i, peer in enumerate(targets):
            to_row(
                peer * 2 + core, gathered.at[half, r], gathered.at[half, r], gather_send, gather_recv.at[i]
            ).start()
        if relayed:
            to_row(partner, gathered.at[half, r], gathered.at[half, r], gather_send, relay_recv.at[half]).start()
        stage[r] = operand

    def sent_vectors(relayed=True):
        bulk = gathered.at[0, pl.ds(0, chips if relayed else chips - 1)]
        to_row(partner, bulk, bulk, gather_send, gather_send).wait_send()
        bulk = own.at[pl.ds(0, others)]
        to_grp(grp_peers[0], bulk, bulk, own_send, own_send).wait_send()

    def take_own():
        bulk = own.at[pl.ds(0, others)]
        to_grp(grp_peers[0], bulk, bulk, own_recv, own_recv).wait_recv()

    def keep_own(step):
        for i in range(group_count):
            own_history[step * width : (step + 1) * width, i * part : (i + 1) * part] = own[i]

    def relay_vectors(half):
        for i, peer in reversed(list(enumerate(sources))):
            slot = peer * 2 + core
            block = gathered.at[half, slot]
            to_row(slot, block, block, gather_send, gather_recv.at[i]).wait_recv()
            to_row(partner, block, block, relay_send, relay_recv.at[half]).start()
            stage[slot] = gathered[half, slot]

    def relays_sent():
        bulk = gathered.at[0, pl.ds(0, chips - 1)]
        to_row(partner, bulk, bulk, relay_send, relay_send).wait_send()

    def take_relayed(half):
        bulk = gathered.at[half, pl.ds(0, chips)]
        to_row(partner, bulk, bulk, gather_send, relay_recv.at[half]).wait_recv()
        for peer in range(chips):
            slot = peer * 2 + 1 - core
            stage[slot] = gathered[half, slot]

    def pack(dots):
        pieces, done, count = [], 0, dots.shape[1]
        for size in (128, 64, 32):
            while count - done >= size:
                height = width * size // 128
                piece = dots[:, done : done + size]
                pieces.append(
                    jnp.concatenate([piece[i * height : (i + 1) * height] for i in range(width // height)], axis=1)
                )
                done += size
        return jnp.concatenate(pieces, axis=0)

    def unpack(packed, count):
        pieces, done, row = [], 0, 0
        for size in (128, 64, 32):
            while count - done >= size:
                height = width * size // 128
                piece = packed[row : row + height]
                pieces.append(
                    jnp.concatenate([piece[:, i * size : (i + 1) * size] for i in range(width // height)], axis=0)
                )
                done += size
                row += height
        return pieces

    def packed_rows(step):
        return pl.ds(0, (step + 1) * width * width // 128)

    def send_pair_dots(step, half):
        dots = jnp.zeros((width, (step + 1) * width), jnp.float32)
        for peer in range(chips):
            slot = peer * 2 + core
            vector = stage[slot]
            right = vector
            if step > 0:
                right = jnp.concatenate([vector, history[slot, : step * width, :]], axis=0)
            dots = dots + lax.dot_general(vector, right, NT, preferred_element_type=jnp.float32)
        rows = packed_rows(step)
        dots_pair[half, core, rows] = pack(dots)
        mine = dots_pair.at[half, core, rows]
        to_row(partner, mine, mine, dpair_send, dpair_recv.at[half]).start()

    def send_dots(step, half):
        rows = packed_rows(step)
        block = dots_pair.at[half, 0, rows]
        to_row(partner, block, block, dpair_send, dpair_recv.at[half]).wait()
        dots_grp[half, g, rows] = dots_pair[half, 0, rows] + dots_pair[half, 1, rows]
        for peer in grp_peers:
            to_grp(
                peer, dots_grp.at[half, g, rows], dots_grp.at[half, g, rows], dots_send, dots_recv.at[half]
            ).start()

    def take_dots(step, half):
        rows = packed_rows(step)
        bulk = dots_grp.at[half, pl.ds(0, others), rows]
        to_grp(grp_peers[0], bulk, bulk, dots_send, dots_recv.at[half]).wait_recv()
        summed = dots_grp[half, 0, rows]
        for index in range(1, group_count):
            summed = summed + dots_grp[half, index, rows]
        pieces = unpack(summed, (step + 1) * width)
        gram = pieces[0][:, :width]
        if step == 0:
            return None, gram
        whole = jnp.concatenate(pieces, axis=1) if len(pieces) > 1 else pieces[0]
        cross = dot_nt(whole[:, width:], transform[:, : step * width])
        return cross, gram - dot_nt(cross, cross)

    def dots_sent(step, half):
        bulk = dots_grp.at[half, pl.ds(0, others), packed_rows(step)]
        to_grp(grp_peers[0], bulk, bulk, dots_send, dots_recv.at[half]).wait_send()

    def back_product(slot):
        value = products[place_ref[0, slot]]
        for i in range(1, owned):
            value = value + products[place_ref[0, i * owner_count + slot]]
        return value

    def take_pair(peer, half):
        return pair_in[half, peer].astype(jnp.float32)

    mine = pl.ds(pl.multiple_of(g * part, part), part)
    current = start_ref[:, mine]
    shift = shift_ref[:, mine]
    pl.semaphore_wait(barrier, chips + others)
    send_vectors(0, current.astype(jnp.bfloat16))
    lanes = lax.broadcasted_iota(jnp.int32, place_vector.shape, 1)
    place = jnp.full(place_vector.shape, tile_count, jnp.int32)
    for k in range(tile_count):
        alive = k < live_ref[0]
        position = jnp.where(alive, rows_ref[k] * owner_count + cols_ref[k], -1)
        place = jnp.where(lanes == position, k, place)
        row = jnp.full((16, 128), jnp.where(alive, rows_ref[k], -1), jnp.int32)
        for i in range(owned):
            masks[k, i] = jnp.where(row == i, 1.0, 0.0).astype(jnp.bfloat16)
    place_vector[...] = place
    place_copy = pltpu.make_async_copy(place_vector, place_ref, place_sem)
    place_copy.start()
    basis[...] = jnp.zeros_like(basis)
    images[...] = jnp.zeros_like(images)
    transform[...] = jnp.zeros_like(transform)
    products[tile_count] = jnp.zeros((width, part), jnp.float32)
    load.wait()

    def turn(j, carry):
        for i in range(4):
            turned[j * 4 + i] = tiles_ref[j * 4 + i].T
        return carry

    lax.fori_loop(0, tile_count // 4, turn, 0)
    place_copy.wait()

    coef = None
    lane = lax.broadcasted_iota(jnp.int32, (width, total_cols), 1)
    sub = lax.broadcasted_iota(jnp.int32, (width, total_cols), 0)
    for step in range(steps):
        half = step % 2
        take_own()
        for k in range(tile_count):
            products[k] = jnp.dot(own[rows_ref[k]], tiles_ref[k], preferred_element_type=jnp.float32)
        for i, peer in enumerate(targets + [chip]):
            pair_out[peer] = back_product(peer * 2 + 1 - core).astype(jnp.bfloat16)
            to_row(partner, pair_out.at[peer], pair_in.at[half, peer], pair_send, pair_recv.at[half]).start()
        keep_own(step)
        relay_vectors(half)
        send_pair_dots(step, half)
        to_row(partner, pair_out, pair_in.at[half], pair_send, pair_recv.at[half]).wait_recv()
        for peer in targets:
            back_out[peer] = (back_product(peer * 2 + core) + take_pair(peer, half)).astype(jnp.bfloat16)
            to_row(peer * 2 + core, back_out.at[peer], back_in.at[half, chip], back_send, back_recv.at[half]).start()
        total = back_product(r) + take_pair(chip, half)
        send_dots(step, half)
        take_relayed(half)
        forward = jnp.zeros((owned * width, part), jnp.float32)
        for k in range(tile_count):
            vector = stage[cols_ref[k]]
            spread = []
            for i in range(owned):
                mask = masks[k, i]
                mask = jnp.concatenate([jnp.concatenate([mask, mask], axis=1)] * (width // 16), axis=0)
                spread.append(vector * mask)
            forward = forward + jnp.dot(
                jnp.concatenate(spread, axis=0), turned[k], preferred_element_type=jnp.float32
            )
        for i in range(owned):
            direct_out[i] = forward[i * width : (i + 1) * width].astype(jnp.bfloat16)
        for peer in grp_peers:
            to_grp(peer, direct_out.at[peer], direct_in.at[g], direct_send, direct_recv).start()
        for i in range(owned):
            total = total + forward[i * width : (i + 1) * width] * jnp.where(g == i, 1.0, 0.0)
        for slot in range(owner_count):
            history[slot, step * width : (step + 1) * width, :] = stage[slot]
        sent_vectors()
        relays_sent()
        cross, gram = take_dots(step, half)
        left, rest = current, None
        if step > 0:
            left = left - dot_nn(cross, basis[...])
            rest = dot_nn(cross, images[...])
        lower, inverse = factor_and_inverse(gram)
        bulk = back_in.at[half, pl.ds(0, chips - 1)]
        to_row(partner, bulk, bulk, back_send, back_recv.at[half]).wait_recv()
        for peer in sources:
            total = total + back_in[half, peer].astype(jnp.float32)
        bulk = direct_in.at[pl.ds(0, others)]
        to_grp(grp_peers[0], bulk, bulk, direct_send, direct_recv).wait_recv()
        for peer in grp_peers:
            total = total + direct_in[peer].astype(jnp.float32)
        total = 0.5 * total
        if step > 0:
            total = total - rest
        now = dot_nn(inverse, left)
        ahead = now * (MIDDLE - shift)
        if step > 0:
            follow = lower.T
            ahead = ahead - dot_nn(follow, basis[(step - 1) * width : step * width, :])
        image = dot_nn(inverse, total)
        current = image + ahead
        send_vectors(1 - half, current.astype(jnp.bfloat16), step < steps - 1)
        basis[step * width : (step + 1) * width, :] = now
        images[step * width : (step + 1) * width, :] = image
        if step > 0:
            proj_ref[step - 1] = cross + coef
            fac_ref[step - 1] = lower
        unit = jnp.where(lane == step * width + sub, 1.0, 0.0)
        if step == 0:
            transform[:width, :] = dot_nn(inverse, unit)
            coef = -MIDDLE * unit
        else:
            transform[step * width : (step + 1) * width, :] = dot_nn(inverse, unit - dot_nn(cross, transform[...]))
            wide = jnp.concatenate([follow] * (total_cols // width), axis=1)
            coef = -MIDDLE * unit + jnp.where((lane >= (step - 1) * width) & (lane < step * width), wide, 0.0)
        to_row(partner, pair_out, pair_out, pair_send, pair_recv.at[half]).wait_send()
        bulk = back_out.at[pl.ds(0, chips - 1)]
        to_row(partner, bulk, bulk, back_send, back_recv.at[half]).wait_send()
        bulk = direct_out.at[pl.ds(0, others)]
        to_grp(grp_peers[0], bulk, bulk, direct_send, direct_recv).wait_send()
        dots_sent(step, half)

    half = steps % 2
    for i, peer in reversed(list(enumerate(sources))):
        slot = peer * 2 + core
        block = gathered.at[half, slot]
        to_row(slot, block, block, gather_send, gather_recv.at[i]).wait_recv()
        stage[slot] = gathered[half, slot]
    send_pair_dots(steps, half)
    take_own()
    keep_own(steps)
    sent_vectors(False)
    send_dots(steps, half)
    cross, gram = take_dots(steps, half)
    lower, inverse = factor_and_inverse(gram)
    proj_ref[steps - 1] = cross + coef
    fac_ref[steps - 1] = lower
    combine = jnp.concatenate([-dot_nn(inverse, dot_nn(cross, transform[...])), inverse], axis=1)
    high = combine.astype(jnp.bfloat16)
    low = (combine - high.astype(jnp.float32)).astype(jnp.bfloat16)
    both = jnp.dot(jnp.concatenate([high, low], axis=0), own_history[...], preferred_element_type=jnp.float32)
    next_ref[...] = both[:width] + both[width:]
    dots_sent(steps, half)


def hand_on(proj_in, fac_in, next_in, proj_ref, fac_ref, next_ref):
    proj_ref[...] = proj_in[...]
    fac_ref[...] = fac_in[...]
    next_ref[...] = next_in[...]


def per_device(tiles, tile_rows, tile_cols, live_tiles, dual_shift, start_block):
    matrix = tiles[0, 0]
    tile_count, edge = matrix.shape[0], matrix.shape[1]
    width, row_count = start_block.shape
    group_count = lax.axis_size("grp")
    owner_count = lax.axis_size("row")
    owned = row_count // edge
    part = row_count // group_count
    total_cols = ITERS * width
    vmem = pl.BlockSpec(memory_space=pltpu.VMEM)
    smem = pl.BlockSpec(memory_space=pltpu.SMEM)
    dma = pltpu.SemaphoreType.DMA
    packed = width + width * width // 128
    shapes = (
            jax.ShapeDtypeStruct((ITERS, width, total_cols), jnp.float32),
            jax.ShapeDtypeStruct((ITERS, width, width), jnp.float32),
            jax.ShapeDtypeStruct((width, row_count), jnp.float32),
    )
    outs = pl.pallas_call(
        functools.partial(kernel, ITERS, group_count, owner_count),
        out_shape=shapes,
        in_specs=[vmem, vmem, smem, smem, smem, pl.BlockSpec(memory_space=pltpu.HBM)],
        out_specs=(vmem, vmem, vmem),
        scratch_shapes=[
            pltpu.VMEM(matrix.shape, jnp.bfloat16),
            pltpu.VMEM(matrix.shape, jnp.bfloat16),
            pltpu.VMEM((tile_count, owned, 16, 128), jnp.bfloat16),
            pltpu.VMEM((tile_count + 1, width, part), jnp.float32),
            pltpu.VMEM((2, owner_count, width, part), jnp.bfloat16),
            pltpu.VMEM((owner_count, width, part), jnp.bfloat16),
            pltpu.VMEM((owner_count, total_cols, part), jnp.bfloat16),
            pltpu.VMEM((group_count, width, part), jnp.bfloat16),
            pltpu.VMEM((total_cols + width, row_count), jnp.bfloat16),
            pltpu.VMEM((owner_count // 2, width, part), jnp.bfloat16),
            pltpu.VMEM((2, owner_count // 2, width, part), jnp.bfloat16),
            pltpu.VMEM((group_count, width, part), jnp.bfloat16),
            pltpu.VMEM((group_count, width, part), jnp.bfloat16),
            pltpu.VMEM((owner_count // 2, width, part), jnp.bfloat16),
            pltpu.VMEM((2, owner_count // 2, width, part), jnp.bfloat16),
            pltpu.VMEM((2, 2, packed, total_cols), jnp.float32),
            pltpu.VMEM((2, group_count, packed, total_cols), jnp.float32),
            pltpu.VMEM((total_cols, part), jnp.float32),
            pltpu.VMEM((total_cols, part), jnp.float32),
            pltpu.VMEM((total_cols, total_cols), jnp.float32),
            pltpu.VMEM((8, owned * owner_count), jnp.int32),
            pltpu.SMEM((8, owned * owner_count), jnp.int32),
            dma, dma,
            dma, dma((owner_count // 2 - 1,)), dma, dma((2,)), dma, dma,
            dma, dma((2,)), dma, dma((2,)), dma, dma, dma, dma((2,)), dma, dma((2,)),
        ],
        compiler_params=pltpu.CompilerParams(
            collective_id=0, has_side_effects=True, vmem_limit_bytes=60 * 1024 * 1024
        ),
    )(start_block, dual_shift[None, :], tile_rows[0, 0], tile_cols[0, 0], live_tiles[0], matrix)
    return pl.pallas_call(hand_on, out_shape=shapes, in_specs=[vmem] * 3, out_specs=(vmem,) * 3)(*outs)


def solution(mesh):
    in_specs = (
        P("grp", "row", None, None, None),
        P("grp", "row", None),
        P("grp", "row", None),
        P("grp", "row"),
        P("row"),
        P(None, "row"),
    )
    out_specs = (P(), P(), P(None, "row"))
    return jax.shard_map(
        per_device, mesh=mesh, in_specs=in_specs, out_specs=out_specs, check_vma=False
    )
```

```python
import functools

import jax
import jax.numpy as jnp
from jax import lax
from jax.experimental import pallas as pl
from jax.experimental.pallas import tpu as pltpu
from jax.sharding import PartitionSpec as P

ITERS = 4
MESH = pl.DeviceIdType.MESH
HIGH = lax.Precision.HIGHEST
NT = (((1,), (1,)), ((), ()))
MIDDLE = 1.25
PANEL = 8
SIDE = 4


def dot_nt(a, b):
    return lax.dot_general(a, b, NT, precision=HIGH, preferred_element_type=jnp.float32)


def dot_nn(a, b):
    return jnp.dot(a, b, precision=HIGH, preferred_element_type=jnp.float32)


def factor_and_inverse(gram):
    n = gram.shape[0]
    row = lax.broadcasted_iota(jnp.int32, (n, n), 0)
    lane = lax.broadcasted_iota(jnp.int32, (n, n), 1)
    within = lax.broadcasted_iota(jnp.int32, (PANEL, 2 * n), 0)
    work = jnp.concatenate([gram, jnp.where(row == lane, 1.0, 0.0)], axis=1)
    blocks = []
    for start in range(0, n, PANEL):
        columns = [jnp.broadcast_to(work[:, k : k + 1], work.shape) for k in range(start, start + PANEL)]
        rows = [work[i : i + 1, :] for i in range(PANEL)]
        block = jnp.zeros((PANEL, 2 * n), jnp.float32)
        for i in range(PANEL):
            scale = lax.rsqrt(columns[i][i : i + 1, :])
            columns[i] = columns[i] * scale
            rows[i] = rows[i] * scale
            for later in range(i + 1, PANEL):
                weight = columns[i][later : later + 1, :]
                columns[later] = columns[later] - columns[i] * weight
                rows[later] = rows[later] - rows[i] * weight
            block = jnp.where(within == i, rows[i], block)
        blocks.append(block)
        work = work[PANEL:]
        if start + PANEL < n:
            for i in range(PANEL):
                work = work - columns[i][PANEL:] * rows[i]
    whole = jnp.concatenate(blocks, axis=0)
    return jnp.where(lane >= row, whole[:, :n], 0.0), whole[:, n:]


def kernel(
    steps, group_count, owner_count,
    start_hbm, shift_hbm, rows_hbm, cols_hbm, live_ref, tiles_hbm,
    proj_ref, fac_ref, next_ref,
    start_ref, shift_ref, rows_ref, cols_ref, input_sem, tiles_ref, turned, masks, products, gathered, stage, history, own, own_history, back_out, back_in, direct_out, direct_in,
    pair_out, pair_in, dots_pair, dots_grp, basis, images, transform, place_vector, place_ref, tile_sem, place_sem,
    gather_send, gather_recv, relay_send, relay_recv, own_send, own_recv,
    pair_send, pair_recv, back_send, back_recv, direct_send, direct_recv, dots_send, dots_recv, dpair_send, dpair_recv,
):
    g = lax.axis_index("grp")
    r = lax.axis_index("row")
    width = start_ref.shape[0]
    row_count = start_ref.shape[1]
    part = row_count // group_count
    tile_count = tiles_ref.shape[0]
    owned = row_count // tiles_ref.shape[1]
    chips = owner_count // 2
    chip, core = r // 2, lax.rem(r, 2)
    partner = chip * 2 + 1 - core
    chip_x, chip_z = lax.rem(chip, SIDE), chip // SIDE

    def away(d):
        return min(d % SIDE, SIDE - d % SIDE) + min(d // SIDE, chips // SIDE - d // SIDE)

    offsets = sorted(range(1, chips), key=lambda d: -away(d))

    def chip_at(d, sign):
        z_count = chips // SIDE
        return lax.rem(chip_z + (sign * (d // SIDE)) % z_count, z_count) * SIDE + lax.rem(
            chip_x + (sign * (d % SIDE)) % SIDE, SIDE
        )

    sources = [chip_at(d, -1) for d in offsets]
    targets = [chip_at(d, 1) for d in offsets]
    grp_order = sorted(range(1, group_count), key=lambda d: -min(d, group_count - d))
    grp_peers = [lax.rem(g + d, group_count) for d in grp_order]
    total_cols = steps * width

    barrier = pltpu.get_barrier_semaphore()
    for peer in targets:
        pl.semaphore_signal(barrier, inc=1, device_id=(g, peer * 2 + core), device_id_type=MESH)
    pl.semaphore_signal(barrier, inc=1, device_id=(g, partner), device_id_type=MESH)
    for peer in grp_peers:
        pl.semaphore_signal(barrier, inc=1, device_id=(peer, r), device_id_type=MESH)
    inputs = [
        pltpu.make_async_copy(src, dst, input_sem.at[i])
        for i, (src, dst) in enumerate(
            [(start_hbm, start_ref), (shift_hbm, shift_ref), (rows_hbm, rows_ref), (cols_hbm, cols_ref)]
        )
    ]
    for copy in inputs:
        copy.start()
    load = pltpu.make_async_copy(tiles_hbm, tiles_ref, tile_sem)
    load.start()

    def to_row(peer, src, dst, send, recv):
        return pltpu.make_async_remote_copy(
            src_ref=src, dst_ref=dst, send_sem=send, recv_sem=recv,
            device_id=(g, peer), device_id_type=MESH,
        )

    def to_grp(peer, src, dst, send, recv):
        return pltpu.make_async_remote_copy(
            src_ref=src, dst_ref=dst, send_sem=send, recv_sem=recv,
            device_id=(peer, r), device_id_type=MESH,
        )

    others = group_count - 1

    def send_vectors(half, operand, relayed=True, own_too=True):
        gathered[half, r] = operand
        if own_too:
            own[g] = operand
            for peer in grp_peers:
                to_grp(peer, own.at[g], own.at[g], own_send, own_recv).start()
        for i, peer in enumerate(targets):
            to_row(
                peer * 2 + core, gathered.at[half, r], gathered.at[half, r], gather_send, gather_recv.at[i]
            ).start()
        if relayed:
            to_row(partner, gathered.at[half, r], gathered.at[half, r], gather_send, relay_recv.at[half]).start()
        stage[r] = operand

    def sent_vectors(relayed=True, own_too=True):
        bulk = gathered.at[0, pl.ds(0, chips if relayed else chips - 1)]
        to_row(partner, bulk, bulk, gather_send, gather_send).wait_send()
        if own_too:
            bulk = own.at[pl.ds(0, others)]
            to_grp(grp_peers[0], bulk, bulk, own_send, own_send).wait_send()

    def take_own():
        bulk = own.at[pl.ds(0, others)]
        to_grp(grp_peers[0], bulk, bulk, own_recv, own_recv).wait_recv()

    def keep_own(step):
        for i in range(group_count):
            own_history[step * width : (step + 1) * width, i * part : (i + 1) * part] = own[i]

    def take_gathered(step, half):
        dots, batch = None, [r]
        for count, (i, peer) in enumerate(reversed(list(enumerate(sources)))):
            slot = peer * 2 + core
            block = gathered.at[half, slot]
            to_row(slot, block, block, gather_send, gather_recv.at[i]).wait_recv()
            if step < steps:
                to_row(partner, block, block, relay_send, relay_recv.at[half]).start()
            stage[slot] = gathered[half, slot]
            batch.append(slot)
            if count % 5 == 4:
                value = slot_dots(step, batch)
                dots = value if dots is None else dots + value
                batch = []
        return dots

    def relays_sent():
        bulk = gathered.at[0, pl.ds(0, chips - 1)]
        to_row(partner, bulk, bulk, relay_send, relay_send).wait_send()

    def take_relayed(half):
        bulk = gathered.at[half, pl.ds(0, chips)]
        to_row(partner, bulk, bulk, gather_send, relay_recv.at[half]).wait_recv()
        for peer in range(chips):
            slot = peer * 2 + 1 - core
            stage[slot] = gathered[half, slot]

    def pack(dots):
        pieces, done, count = [], 0, dots.shape[1]
        for size in (128, 64, 32):
            while count - done >= size:
                height = width * size // 128
                piece = dots[:, done : done + size]
                pieces.append(
                    jnp.concatenate([piece[i * height : (i + 1) * height] for i in range(width // height)], axis=1)
                )
                done += size
        return jnp.concatenate(pieces, axis=0)

    def unpack(packed, count):
        pieces, done, row = [], 0, 0
        for size in (128, 64, 32):
            while count - done >= size:
                height = width * size // 128
                piece = packed[row : row + height]
                pieces.append(
                    jnp.concatenate([piece[:, i * size : (i + 1) * size] for i in range(width // height)], axis=0)
                )
                done += size
                row += height
        return pieces

    def packed_rows(step):
        return pl.ds(0, (step + 1) * width * width // 128)

    def slot_dots(step, slots):
        dots = jnp.zeros((width, (step + 1) * width), jnp.float32)
        for slot in slots:
            vector = stage[slot]
            right = vector
            if step > 0:
                right = jnp.concatenate([vector, history[slot, : step * width, :]], axis=0)
            dots = dots + lax.dot_general(vector, right, NT, preferred_element_type=jnp.float32)
        return dots

    def send_pair_dots(step, half, dots):
        rows = packed_rows(step)
        dots_pair[half, core, rows] = pack(dots)
        mine = dots_pair.at[half, core, rows]
        to_row(partner, mine, mine, dpair_send, dpair_recv.at[half]).start()

    def send_dots(step, half):
        rows = packed_rows(step)
        block = dots_pair.at[half, 0, rows]
        to_row(partner, block, block, dpair_send, dpair_recv.at[half]).wait()
        dots_grp[half, g, rows] = dots_pair[half, 0, rows] + dots_pair[half, 1, rows]
        for peer in grp_peers:
            to_grp(
                peer, dots_grp.at[half, g, rows], dots_grp.at[half, g, rows], dots_send, dots_recv.at[half]
            ).start()

    def take_dots(step, half):
        rows = packed_rows(step)
        bulk = dots_grp.at[half, pl.ds(0, others), rows]
        to_grp(grp_peers[0], bulk, bulk, dots_send, dots_recv.at[half]).wait_recv()
        summed = dots_grp[half, 0, rows]
        for index in range(1, group_count):
            summed = summed + dots_grp[half, index, rows]
        pieces = unpack(summed, (step + 1) * width)
        gram = pieces[0][:, :width]
        if step == 0:
            return None, gram
        whole = jnp.concatenate(pieces, axis=1) if len(pieces) > 1 else pieces[0]
        cross = dot_nt(whole[:, width:], transform[:, : step * width])
        return cross, gram - dot_nt(cross, cross)

    def dots_sent(step, half):
        bulk = dots_grp.at[half, pl.ds(0, others), packed_rows(step)]
        to_grp(grp_peers[0], bulk, bulk, dots_send, dots_recv.at[half]).wait_send()

    def back_product(slot):
        value = products[place_ref[0, slot]]
        for i in range(1, owned):
            value = value + products[place_ref[0, i * owner_count + slot]]
        return value

    def take_pair(peer, half):
        return pair_in[half, peer].astype(jnp.float32)

    mine = pl.ds(pl.multiple_of(g * part, part), part)
    for copy in inputs:
        copy.wait()
    current = start_ref[:, mine]
    shift = shift_ref[:, mine]
    pl.semaphore_wait(barrier, chips + others)
    send_vectors(0, current.astype(jnp.bfloat16), own_too=False)
    for i in range(group_count):
        own[i] = start_ref[:, i * part : (i + 1) * part].astype(jnp.bfloat16)
    lanes = lax.broadcasted_iota(jnp.int32, place_vector.shape, 1)
    place = jnp.full(place_vector.shape, tile_count, jnp.int32)
    for k in range(tile_count):
        alive = k < live_ref[0]
        position = jnp.where(alive, rows_ref[k] * owner_count + cols_ref[k], -1)
        place = jnp.where(lanes == position, k, place)
        row = jnp.full((16, 128), jnp.where(alive, rows_ref[k], -1), jnp.int32)
        for i in range(owned):
            masks[k, i] = jnp.where(row == i, 1.0, 0.0).astype(jnp.bfloat16)
    place_vector[...] = place
    place_copy = pltpu.make_async_copy(place_vector, place_ref, place_sem)
    place_copy.start()
    basis[...] = jnp.zeros_like(basis)
    images[...] = jnp.zeros_like(images)
    transform[...] = jnp.zeros_like(transform)
    products[tile_count] = jnp.zeros((width, part), jnp.float32)
    load.wait()
    place_copy.wait()

    def turn(j, carry):
        for i in range(4):
            turned[j * 4 + i] = tiles_ref[j * 4 + i].T
        return carry

    coef = None
    lane = lax.broadcasted_iota(jnp.int32, (width, total_cols), 1)
    sub = lax.broadcasted_iota(jnp.int32, (width, total_cols), 0)
    for step in range(steps):
        half = step % 2
        if step > 0:
            take_own()
        for k in range(tile_count):
            products[k] = jnp.dot(own[rows_ref[k]], tiles_ref[k], preferred_element_type=jnp.float32)
        for i, peer in enumerate(targets + [chip]):
            pair_out[peer] = back_product(peer * 2 + 1 - core).astype(jnp.bfloat16)
            to_row(partner, pair_out.at[peer], pair_in.at[half, peer], pair_send, pair_recv.at[half]).start()
        keep_own(step)
        if step == 0:
            lax.fori_loop(0, tile_count // 4, turn, 0)
        dots = take_gathered(step, half)
        send_pair_dots(step, half, dots)
        to_row(partner, pair_out, pair_in.at[half], pair_send, pair_recv.at[half]).wait_recv()
        for peer in targets:
            back_out[peer] = (back_product(peer * 2 + core) + take_pair(peer, half)).astype(jnp.bfloat16)
            to_row(peer * 2 + core, back_out.at[peer], back_in.at[half, chip], back_send, back_recv.at[half]).start()
        total = back_product(r) + take_pair(chip, half)
        send_dots(step, half)
        take_relayed(half)
        forward = jnp.zeros((owned * width, part), jnp.float32)
        for k in range(tile_count):
            vector = stage[cols_ref[k]]
            spread = []
            for i in range(owned):
                mask = masks[k, i]
                mask = jnp.concatenate([jnp.concatenate([mask, mask], axis=1)] * (width // 16), axis=0)
                spread.append(vector * mask)
            forward = forward + jnp.dot(
                jnp.concatenate(spread, axis=0), turned[k], preferred_element_type=jnp.float32
            )
        for i in range(owned):
            direct_out[i] = forward[i * width : (i + 1) * width].astype(jnp.bfloat16)
        for peer in grp_peers:
            to_grp(peer, direct_out.at[peer], direct_in.at[g], direct_send, direct_recv).start()
        for i in range(owned):
            total = total + forward[i * width : (i + 1) * width] * jnp.where(g == i, 1.0, 0.0)
        for slot in range(owner_count):
            history[slot, step * width : (step + 1) * width, :] = stage[slot]
        sent_vectors(own_too=step > 0)
        relays_sent()
        cross, gram = take_dots(step, half)
        left, rest = current, None
        if step > 0:
            left = left - dot_nn(cross, basis[...])
            rest = dot_nn(cross, images[...])
        upper, inverse = factor_and_inverse(gram)
        now = dot_nn(inverse, left)
        ahead = now * (MIDDLE - shift)
        if step > 0:
            ahead = ahead - dot_nn(upper, basis[(step - 1) * width : step * width, :])
        bulk = back_in.at[half, pl.ds(0, chips - 1)]
        to_row(partner, bulk, bulk, back_send, back_recv.at[half]).wait_recv()
        for peer in sources:
            total = total + back_in[half, peer].astype(jnp.float32)
        bulk = direct_in.at[pl.ds(0, others)]
        to_grp(grp_peers[0], bulk, bulk, direct_send, direct_recv).wait_recv()
        for peer in grp_peers:
            total = total + direct_in[peer].astype(jnp.float32)
        total = 0.5 * total
        if step > 0:
            total = total - rest
        image = dot_nn(inverse, total)
        current = image + ahead
        send_vectors(1 - half, current.astype(jnp.bfloat16), step < steps - 1)
        basis[step * width : (step + 1) * width, :] = now
        images[step * width : (step + 1) * width, :] = image
        if step > 0:
            proj_ref[step - 1] = cross + coef
            fac_ref[step - 1] = upper.T
        unit = jnp.where(lane == step * width + sub, 1.0, 0.0)
        if step == 0:
            transform[:width, :] = dot_nn(inverse, unit)
            coef = -MIDDLE * unit
        else:
            transform[step * width : (step + 1) * width, :] = dot_nn(inverse, unit - dot_nn(cross, transform[...]))
            wide = jnp.concatenate([upper] * (total_cols // width), axis=1)
            coef = -MIDDLE * unit + jnp.where((lane >= (step - 1) * width) & (lane < step * width), wide, 0.0)
        to_row(partner, pair_out, pair_out, pair_send, pair_recv.at[half]).wait_send()
        bulk = back_out.at[pl.ds(0, chips - 1)]
        to_row(partner, bulk, bulk, back_send, back_recv.at[half]).wait_send()
        bulk = direct_out.at[pl.ds(0, others)]
        to_grp(grp_peers[0], bulk, bulk, direct_send, direct_recv).wait_send()
        dots_sent(step, half)

    half = steps % 2
    dots = take_gathered(steps, half)
    send_pair_dots(steps, half, dots)
    take_own()
    keep_own(steps)
    sent_vectors(False)
    send_dots(steps, half)
    cross, gram = take_dots(steps, half)
    upper, inverse = factor_and_inverse(gram)
    proj_ref[steps - 1] = cross + coef
    fac_ref[steps - 1] = upper.T
    combine = jnp.concatenate([-dot_nn(inverse, dot_nn(cross, transform[...])), inverse], axis=1)
    high = combine.astype(jnp.bfloat16)
    low = (combine - high.astype(jnp.float32)).astype(jnp.bfloat16)
    both = jnp.dot(jnp.concatenate([high, low], axis=0), own_history[...], preferred_element_type=jnp.float32)
    next_ref[...] = both[:width] + both[width:]
    dots_sent(steps, half)


def hand_on(proj_in, fac_in, next_in, proj_ref, fac_ref, next_ref):
    proj_ref[...] = proj_in[...]
    fac_ref[...] = fac_in[...]
    next_ref[...] = next_in[...]


def per_device(tiles, tile_rows, tile_cols, live_tiles, dual_shift, start_block):
    matrix = tiles[0, 0]
    tile_count, edge = matrix.shape[0], matrix.shape[1]
    width, row_count = start_block.shape
    group_count = lax.axis_size("grp")
    owner_count = lax.axis_size("row")
    owned = row_count // edge
    part = row_count // group_count
    total_cols = ITERS * width
    vmem = pl.BlockSpec(memory_space=pltpu.VMEM)
    smem = pl.BlockSpec(memory_space=pltpu.SMEM)
    hbm = pl.BlockSpec(memory_space=pltpu.HBM)
    dma = pltpu.SemaphoreType.DMA
    packed = width + width * width // 128
    shapes = (
            jax.ShapeDtypeStruct((ITERS, width, total_cols), jnp.float32),
            jax.ShapeDtypeStruct((ITERS, width, width), jnp.float32),
            jax.ShapeDtypeStruct((width, row_count), jnp.float32),
    )
    outs = pl.pallas_call(
        functools.partial(kernel, ITERS, group_count, owner_count),
        out_shape=tuple(pltpu.VMEM(x.shape, x.dtype) for x in shapes),
        in_specs=[hbm, hbm, hbm, hbm, smem, hbm],
        out_specs=(vmem, vmem, vmem),
        scratch_shapes=[
            pltpu.VMEM((width, row_count), jnp.float32),
            pltpu.VMEM((1, row_count), jnp.float32),
            pltpu.SMEM((tile_count,), jnp.int32),
            pltpu.SMEM((tile_count,), jnp.int32),
            dma((4,)),
            pltpu.VMEM(matrix.shape, jnp.bfloat16),
            pltpu.VMEM(matrix.shape, jnp.bfloat16),
            pltpu.VMEM((tile_count, owned, 16, 128), jnp.bfloat16),
            pltpu.VMEM((tile_count + 1, width, part), jnp.float32),
            pltpu.VMEM((2, owner_count, width, part), jnp.bfloat16),
            pltpu.VMEM((owner_count, width, part), jnp.bfloat16),
            pltpu.VMEM((owner_count, total_cols, part), jnp.bfloat16),
            pltpu.VMEM((group_count, width, part), jnp.bfloat16),
            pltpu.VMEM((total_cols + width, row_count), jnp.bfloat16),
            pltpu.VMEM((owner_count // 2, width, part), jnp.bfloat16),
            pltpu.VMEM((2, owner_count // 2, width, part), jnp.bfloat16),
            pltpu.VMEM((group_count, width, part), jnp.bfloat16),
            pltpu.VMEM((group_count, width, part), jnp.bfloat16),
            pltpu.VMEM((owner_count // 2, width, part), jnp.bfloat16),
            pltpu.VMEM((2, owner_count // 2, width, part), jnp.bfloat16),
            pltpu.VMEM((2, 2, packed, total_cols), jnp.float32),
            pltpu.VMEM((2, group_count, packed, total_cols), jnp.float32),
            pltpu.VMEM((total_cols, part), jnp.float32),
            pltpu.VMEM((total_cols, part), jnp.float32),
            pltpu.VMEM((total_cols, total_cols), jnp.float32),
            pltpu.VMEM((8, owned * owner_count), jnp.int32),
            pltpu.SMEM((8, owned * owner_count), jnp.int32),
            dma, dma,
            dma, dma((owner_count // 2 - 1,)), dma, dma((2,)), dma, dma,
            dma, dma((2,)), dma, dma((2,)), dma, dma, dma, dma((2,)), dma, dma((2,)),
        ],
        compiler_params=pltpu.CompilerParams(
            collective_id=0, has_side_effects=True, vmem_limit_bytes=60 * 1024 * 1024
        ),
    )(start_block, dual_shift[None, :], tile_rows[0, 0], tile_cols[0, 0], live_tiles[0], matrix)
    return pl.pallas_call(hand_on, out_shape=shapes, in_specs=[vmem] * 3, out_specs=(vmem,) * 3,
        compiler_params=pltpu.CompilerParams(vmem_limit_bytes=2 * 1024 * 1024))(*outs)


def solution(mesh):
    in_specs = (
        P("grp", "row", None, None, None),
        P("grp", "row", None),
        P("grp", "row", None),
        P("grp", "row"),
        P("row"),
        P(None, "row"),
    )
    out_specs = (P(), P(), P(None, "row"))
    return jax.shard_map(
        per_device, mesh=mesh, in_specs=in_specs, out_specs=out_specs, check_vma=False
    )
```

```python
import functools

import jax
import jax.numpy as jnp
from jax import lax
from jax.experimental import pallas as pl
from jax.experimental.pallas import tpu as pltpu
from jax.sharding import PartitionSpec as P

ITERS = 4
MESH = pl.DeviceIdType.MESH
HIGH = lax.Precision.HIGHEST
NT = (((1,), (1,)), ((), ()))
MIDDLE = 1.25
PANEL = 16
SIDE = 4
NEAR = 2


def dot_nt(a, b):
    return lax.dot_general(a, b, NT, precision=HIGH, preferred_element_type=jnp.float32)


def dot_nn(a, b):
    return jnp.dot(a, b, precision=HIGH, preferred_element_type=jnp.float32)


def factor_and_inverse(gram):
    n = gram.shape[0]
    row = lax.broadcasted_iota(jnp.int32, (n, n), 0)
    lane = lax.broadcasted_iota(jnp.int32, (n, n), 1)
    within = lax.broadcasted_iota(jnp.int32, (PANEL, 2 * n), 0)
    work = jnp.concatenate([gram, jnp.where(row == lane, 1.0, 0.0)], axis=1)
    blocks = []
    for start in range(0, n, PANEL):
        columns = [jnp.broadcast_to(work[:, k : k + 1], work.shape) for k in range(start, start + PANEL)]
        rows = [work[i : i + 1, :] for i in range(PANEL)]
        block = jnp.zeros((PANEL, 2 * n), jnp.float32)
        for i in range(PANEL):
            scale = lax.rsqrt(columns[i][i : i + 1, :])
            columns[i] = columns[i] * scale
            rows[i] = rows[i] * scale
            for later in range(i + 1, PANEL):
                weight = columns[i][later : later + 1, :]
                columns[later] = columns[later] - columns[i] * weight
                rows[later] = rows[later] - rows[i] * weight
            block = jnp.where(within == i, rows[i], block)
        blocks.append(block)
        work = work[PANEL:]
        if start + PANEL < n:
            for i in range(PANEL):
                work = work - columns[i][PANEL:] * rows[i]
    whole = jnp.concatenate(blocks, axis=0)
    return jnp.where(lane >= row, whole[:, :n], 0.0), whole[:, n:]


def away(d, chips):
    return min(d % SIDE, SIDE - d % SIDE) + min(d // SIDE, chips // SIDE - d // SIDE)


def far_first(chips):
    return sorted(range(1, chips), key=lambda d: -away(d, chips))


def kernel(
    steps, group_count, owner_count,
    start_hbm, shift_hbm, rows_hbm, cols_hbm, live_ref, tiles_hbm,
    proj_ref, fac_ref, next_ref,
    start_ref, shift_ref, rows_ref, cols_ref, input_sem, tiles_ref, turned, masks, products, gathered, stage, history, own, own_history, back_out, back_in, direct_out, direct_in,
    pair_out, pair_in, dots_grp, basis, images, transform, place_vector, place_ref, tile_sem, place_sem,
    gather_send, gather_recv, relay_send, relay_recv, own_send, own_recv,
    pair_send, pair_recv, back_send, back_recv, direct_send, direct_recv, dots_send, dots_recv,
):
    g = lax.axis_index("grp")
    r = lax.axis_index("row")
    width = start_ref.shape[0]
    row_count = start_ref.shape[1]
    part = row_count // group_count
    tile_count = tiles_ref.shape[0]
    owned = row_count // tiles_ref.shape[1]
    chips = owner_count // 2
    chip, core = r // 2, lax.rem(r, 2)
    partner = chip * 2 + 1 - core
    chip_x, chip_z = lax.rem(chip, SIDE), chip // SIDE

    offsets = far_first(chips)

    def chip_at(d, sign):
        z_count = chips // SIDE
        return lax.rem(chip_z + (sign * (d // SIDE)) % z_count, z_count) * SIDE + lax.rem(
            chip_x + (sign * (d % SIDE)) % SIDE, SIDE
        )

    far_count = sum(away(d, chips) > NEAR for d in offsets)
    sources = [chip_at(d, -1) for d in offsets]
    targets = [chip_at(d, 1) for d in offsets]
    grp_order = sorted(range(1, group_count), key=lambda d: -min(d, group_count - d))
    grp_peers = [lax.rem(g + d, group_count) for d in grp_order]
    total_cols = steps * width

    barrier = pltpu.get_barrier_semaphore()
    for peer in targets:
        pl.semaphore_signal(barrier, inc=1, device_id=(g, peer * 2 + core), device_id_type=MESH)
    for peer in targets[:far_count]:
        pl.semaphore_signal(barrier, inc=1, device_id=(g, peer * 2 + 1 - core), device_id_type=MESH)
    pl.semaphore_signal(barrier, inc=1, device_id=(g, partner), device_id_type=MESH)
    for peer in grp_peers:
        pl.semaphore_signal(barrier, inc=1, device_id=(peer, r), device_id_type=MESH)
        pl.semaphore_signal(barrier, inc=1, device_id=(peer, partner), device_id_type=MESH)
    inputs = [
        pltpu.make_async_copy(src, dst, input_sem.at[i])
        for i, (src, dst) in enumerate(
            [(start_hbm, start_ref), (shift_hbm, shift_ref), (rows_hbm, rows_ref), (cols_hbm, cols_ref)]
        )
    ]
    for copy in inputs:
        copy.start()
    load = pltpu.make_async_copy(tiles_hbm, tiles_ref, tile_sem)
    load.start()

    def to_row(peer, src, dst, send, recv):
        return pltpu.make_async_remote_copy(
            src_ref=src, dst_ref=dst, send_sem=send, recv_sem=recv,
            device_id=(g, peer), device_id_type=MESH,
        )

    def to_grp(peer, src, dst, send, recv):
        return pltpu.make_async_remote_copy(
            src_ref=src, dst_ref=dst, send_sem=send, recv_sem=recv,
            device_id=(peer, r), device_id_type=MESH,
        )

    others = group_count - 1

    def send_vectors(half, operand, relayed=True, own_too=True):
        gathered[half, r] = operand
        if own_too:
            own[g] = operand
            for peer in grp_peers:
                to_grp(peer, own.at[g], own.at[g], own_send, own_recv).start()
        for i, peer in enumerate(targets):
            to_row(
                peer * 2 + core, gathered.at[half, r], gathered.at[half, r], gather_send, gather_recv.at[half, i]
            ).start()
        if relayed:
            to_row(partner, gathered.at[half, r], gathered.at[half, r], gather_send, relay_recv.at[half]).start()
        stage[r] = operand

    def sent_vectors(relayed=True, own_too=True):
        bulk = gathered.at[0, pl.ds(0, chips if relayed else chips - 1)]
        to_row(partner, bulk, bulk, gather_send, gather_send).wait_send()
        if own_too:
            bulk = own.at[pl.ds(0, others)]
            to_grp(grp_peers[0], bulk, bulk, own_send, own_send).wait_send()

    def take_own():
        bulk = own.at[pl.ds(0, others)]
        to_grp(grp_peers[0], bulk, bulk, own_recv, own_recv).wait_recv()

    def keep_own(step):
        for i in range(group_count):
            own_history[step * width : (step + 1) * width, i * part : (i + 1) * part] = own[i]

    def take_gathered(step, half):
        dots, batch = None, [r]
        for count, (i, peer) in enumerate(reversed(list(enumerate(sources)))):
            slot = peer * 2 + core
            block = gathered.at[half, slot]
            to_row(slot, block, block, gather_send, gather_recv.at[half, i]).wait_recv()
            if step < steps:
                to_row(partner, block, block, relay_send, relay_recv.at[half]).start()
            stage[slot] = gathered[half, slot]
            batch.append(slot)
            if count % 5 == 4:
                value = slot_dots(step, batch)
                dots = value if dots is None else dots + value
                batch = []
        return dots

    def relays_sent():
        bulk = gathered.at[0, pl.ds(0, chips - 1)]
        to_row(partner, bulk, bulk, relay_send, relay_send).wait_send()

    def take_relayed(half):
        bulk = gathered.at[half, pl.ds(0, chips)]
        to_row(partner, bulk, bulk, gather_send, relay_recv.at[half]).wait_recv()
        for peer in range(chips):
            slot = peer * 2 + 1 - core
            stage[slot] = gathered[half, slot]

    def pack(dots):
        pieces, done, count = [], 0, dots.shape[1]
        for size in (128, 64, 32):
            while count - done >= size:
                height = width * size // 128
                piece = dots[:, done : done + size]
                pieces.append(
                    jnp.concatenate([piece[i * height : (i + 1) * height] for i in range(width // height)], axis=1)
                )
                done += size
        return jnp.concatenate(pieces, axis=0)

    def unpack(packed, count):
        pieces, done, row = [], 0, 0
        for size in (128, 64, 32):
            while count - done >= size:
                height = width * size // 128
                piece = packed[row : row + height]
                pieces.append(
                    jnp.concatenate([piece[:, i * size : (i + 1) * size] for i in range(width // height)], axis=0)
                )
                done += size
                row += height
        return pieces

    def packed_rows(step):
        return pl.ds(0, 16 + (step + 1) // 2 * 16)

    def slot_dots(step, slots):
        dots = jnp.zeros((width, (step + 1) * width), jnp.float32)
        for slot in slots:
            vector = stage[slot]
            right = vector
            if step > 0:
                right = jnp.concatenate([vector, history[slot, : step * width, :]], axis=0)
            dots = dots + lax.dot_general(vector, right, NT, preferred_element_type=jnp.float32)
        return dots

    def send_dots(step, half, dots):
        rows = packed_rows(step)
        me = g * 2 + core
        gram = pack(dots[:, :width])
        high = gram.astype(jnp.bfloat16).astype(jnp.float32)
        dots_grp[half, me, :16] = jnp.concatenate([high, gram - high], axis=0).astype(jnp.bfloat16)
        if step > 0:
            cross = pack(dots[:, width:])
            if step % 2 == 1:
                cross = jnp.concatenate([cross, jnp.zeros((8, 128), jnp.float32)], axis=0)
            dots_grp[half, me, 16 : 16 + cross.shape[0]] = cross.astype(jnp.bfloat16)
        block = dots_grp.at[half, me, rows]
        for peer in grp_peers:
            to_grp(peer, block, block, dots_send, dots_recv.at[half]).start()
            pltpu.make_async_remote_copy(
                src_ref=block, dst_ref=block, send_sem=dots_send, recv_sem=dots_recv.at[half],
                device_id=(peer, partner), device_id_type=MESH,
            ).start()
        to_row(partner, block, block, dots_send, dots_recv.at[half]).start()

    def take_dots(step, half):
        rows = packed_rows(step)
        bulk = dots_grp.at[half, pl.ds(0, 2 * group_count - 1), rows]
        to_grp(grp_peers[0], bulk, bulk, dots_send, dots_recv.at[half]).wait_recv()
        summed = dots_grp[half, 0, rows].astype(jnp.float32)
        for index in range(1, 2 * group_count):
            summed = summed + dots_grp[half, index, rows].astype(jnp.float32)
        gram = unpack(summed[:8] + summed[8:16], width)[0]
        if step == 0:
            return None, gram
        pieces = unpack(summed[16:], step * width)
        whole = jnp.concatenate(pieces, axis=1) if len(pieces) > 1 else pieces[0]
        cross = dot_nt(whole, transform[:, : step * width])
        return cross, gram - dot_nt(cross, cross)

    def dots_sent(step, half):
        bulk = dots_grp.at[half, pl.ds(0, 2 * group_count - 1), packed_rows(step)]
        to_grp(grp_peers[0], bulk, bulk, dots_send, dots_recv.at[half]).wait_send()

    def back_product(slot):
        value = products[place_ref[0, slot]]
        for i in range(1, owned):
            value = value + products[place_ref[0, i * owner_count + slot]]
        return value

    def take_pair(peer, half):
        return pair_in[half, peer].astype(jnp.float32)

    mine = pl.ds(pl.multiple_of(g * part, part), part)
    for copy in inputs:
        copy.wait()
    current = start_ref[:, mine]
    shift = shift_ref[:, mine]
    pl.semaphore_wait(barrier, chips + far_count + 2 * others)
    send_vectors(0, current.astype(jnp.bfloat16), own_too=False)
    for i in range(group_count):
        own[i] = start_ref[:, i * part : (i + 1) * part].astype(jnp.bfloat16)
    lanes = lax.broadcasted_iota(jnp.int32, place_vector.shape, 1)
    place = jnp.full(place_vector.shape, tile_count, jnp.int32)
    for k in range(tile_count):
        alive = k < live_ref[0]
        position = jnp.where(alive, rows_ref[k] * owner_count + cols_ref[k], -1)
        place = jnp.where(lanes == position, k, place)
        row = jnp.full((16, 128), jnp.where(alive, rows_ref[k], -1), jnp.int32)
        for i in range(owned):
            masks[k, i] = jnp.where(row == i, 1.0, 0.0).astype(jnp.bfloat16)
    place_vector[...] = place
    place_copy = pltpu.make_async_copy(place_vector, place_ref, place_sem)
    place_copy.start()
    basis[...] = jnp.zeros_like(basis)
    images[...] = jnp.zeros_like(images)
    transform[...] = jnp.zeros_like(transform)
    products[tile_count] = jnp.zeros((width, part), jnp.float32)
    load.wait()
    place_copy.wait()

    def turn(j, carry):
        for i in range(4):
            turned[j * 4 + i] = tiles_ref[j * 4 + i].T
        return carry

    coef = None
    lane = lax.broadcasted_iota(jnp.int32, (width, total_cols), 1)
    sub = lax.broadcasted_iota(jnp.int32, (width, total_cols), 0)
    for step in range(steps):
        half = step % 2
        far = far_count if step > 0 else 0
        near_rows = pl.ds(0, chips - far)
        if step > 0:
            take_own()
        for k in range(tile_count):
            products[k] = jnp.dot(own[rows_ref[k]], tiles_ref[k], preferred_element_type=jnp.float32)
        for i, peer in enumerate(targets[far:] + [chip]):
            pair_out[i] = back_product(peer * 2 + 1 - core).astype(jnp.bfloat16)
            to_row(partner, pair_out.at[i], pair_in.at[half, i], pair_send, pair_recv.at[half]).start()
        for i, peer in enumerate(targets[:far]):
            for side, slot in enumerate([peer * 2 + core, peer * 2 + 1 - core]):
                index = 2 * i + side
                back_out[index] = back_product(slot).astype(jnp.bfloat16)
                to_row(
                    slot, back_out.at[index], back_in.at[half, index], back_send, back_recv.at[half]
                ).start()
        keep_own(step)
        if step == 0:
            lax.fori_loop(0, tile_count // 4, turn, 0)
        def send_back():
            to_row(
                partner, pair_out.at[near_rows], pair_in.at[half, near_rows], pair_send, pair_recv.at[half]
            ).wait_recv()
            for i, peer in enumerate(targets[far:]):
                index = 2 * far + i
                back_out[index] = (back_product(peer * 2 + core) + take_pair(i, half)).astype(jnp.bfloat16)
                to_row(
                    peer * 2 + core, back_out.at[index], back_in.at[half, index], back_send, back_recv.at[half]
                ).start()
            total = back_product(r) + take_pair(len(targets) - far, half)
            return total

        if step == 0:
            total = send_back()
        dots = take_gathered(step, half)
        send_dots(step, half, dots)
        if step > 0:
            total = send_back()
        take_relayed(half)
        forward = jnp.zeros((owned * width, part), jnp.float32)
        for k in range(tile_count):
            vector = stage[cols_ref[k]]
            spread = []
            for i in range(owned):
                mask = masks[k, i]
                mask = jnp.concatenate([jnp.concatenate([mask, mask], axis=1)] * (width // 16), axis=0)
                spread.append(vector * mask)
            forward = forward + jnp.dot(
                jnp.concatenate(spread, axis=0), turned[k], preferred_element_type=jnp.float32
            )
        for i in range(owned):
            direct_out[i] = forward[i * width : (i + 1) * width].astype(jnp.bfloat16)
        for peer in grp_peers:
            to_grp(peer, direct_out.at[peer], direct_in.at[g], direct_send, direct_recv).start()
        for i in range(owned):
            total = total + forward[i * width : (i + 1) * width] * jnp.where(g == i, 1.0, 0.0)
        for slot in range(owner_count):
            history[slot, step * width : (step + 1) * width, :] = stage[slot]
        sent_vectors(own_too=step > 0)
        relays_sent()
        cross, gram = take_dots(step, half)
        left, rest = current, None
        if step > 0:
            left = left - dot_nn(cross, basis[...])
            rest = dot_nn(cross, images[...])
        upper, inverse = factor_and_inverse(gram)
        now = dot_nn(inverse, left)
        ahead = now * (MIDDLE - shift)
        if step > 0:
            ahead = ahead - dot_nn(upper, basis[(step - 1) * width : step * width, :])
        bulk = back_in.at[half, pl.ds(0, chips - 1 + far)]
        to_row(partner, bulk, bulk, back_send, back_recv.at[half]).wait_recv()
        for index in range(chips - 1 + far):
            total = total + back_in[half, index].astype(jnp.float32)
        bulk = direct_in.at[pl.ds(0, others)]
        to_grp(grp_peers[0], bulk, bulk, direct_send, direct_recv).wait_recv()
        for peer in grp_peers:
            total = total + direct_in[peer].astype(jnp.float32)
        total = 0.5 * total
        if step > 0:
            total = total - rest
        image = dot_nn(inverse, total)
        current = image + ahead
        send_vectors(1 - half, current.astype(jnp.bfloat16), step < steps - 1)
        basis[step * width : (step + 1) * width, :] = now
        images[step * width : (step + 1) * width, :] = image
        if step > 0:
            proj_ref[step - 1] = cross + coef
            fac_ref[step - 1] = upper.T
        unit = jnp.where(lane == step * width + sub, 1.0, 0.0)
        if step == 0:
            transform[:width, :] = dot_nn(inverse, unit)
            coef = -MIDDLE * unit
        else:
            transform[step * width : (step + 1) * width, :] = dot_nn(inverse, unit - dot_nn(cross, transform[...]))
            wide = jnp.concatenate([upper] * (total_cols // width), axis=1)
            coef = -MIDDLE * unit + jnp.where((lane >= (step - 1) * width) & (lane < step * width), wide, 0.0)
        bulk = pair_out.at[near_rows]
        to_row(partner, bulk, bulk, pair_send, pair_recv.at[half]).wait_send()
        bulk = back_out.at[pl.ds(0, chips - 1 + far)]
        to_row(partner, bulk, bulk, back_send, back_recv.at[half]).wait_send()
        bulk = direct_out.at[pl.ds(0, others)]
        to_grp(grp_peers[0], bulk, bulk, direct_send, direct_recv).wait_send()
        dots_sent(step, half)

    half = steps % 2
    dots = take_gathered(steps, half)
    send_dots(steps, half, dots)
    take_own()
    keep_own(steps)
    sent_vectors(False)
    cross, gram = take_dots(steps, half)
    combine = dot_nn(cross, transform[...])
    high = combine.astype(jnp.bfloat16)
    low = (combine - high.astype(jnp.float32)).astype(jnp.bfloat16)
    both = jnp.dot(
        jnp.concatenate([high, low], axis=0), own_history[:total_cols, :], preferred_element_type=jnp.float32
    )
    left = own_history[total_cols:, :].astype(jnp.float32) - both[:width] - both[width:]
    upper, inverse = factor_and_inverse(gram)
    proj_ref[steps - 1] = cross + coef
    fac_ref[steps - 1] = upper.T
    next_ref[...] = dot_nn(inverse, left)
    dots_sent(steps, half)


def hand_on(proj_in, fac_in, next_in, proj_ref, fac_ref, next_ref):
    proj_ref[...] = proj_in[...]
    fac_ref[...] = fac_in[...]
    next_ref[...] = next_in[...]


def per_device(tiles, tile_rows, tile_cols, live_tiles, dual_shift, start_block):
    matrix = tiles[0, 0]
    tile_count, edge = matrix.shape[0], matrix.shape[1]
    width, row_count = start_block.shape
    group_count = lax.axis_size("grp")
    owner_count = lax.axis_size("row")
    owned = row_count // edge
    part = row_count // group_count
    total_cols = ITERS * width
    vmem = pl.BlockSpec(memory_space=pltpu.VMEM)
    smem = pl.BlockSpec(memory_space=pltpu.SMEM)
    hbm = pl.BlockSpec(memory_space=pltpu.HBM)
    dma = pltpu.SemaphoreType.DMA
    chips = owner_count // 2
    far = sum(away(d, chips) > NEAR for d in far_first(chips))
    back_count = chips - 1 + far
    pair_count = chips
    packed = 16 + (ITERS + 1) // 2 * 16
    shapes = (
            jax.ShapeDtypeStruct((ITERS, width, total_cols), jnp.float32),
            jax.ShapeDtypeStruct((ITERS, width, width), jnp.float32),
            jax.ShapeDtypeStruct((width, row_count), jnp.float32),
    )
    outs = pl.pallas_call(
        functools.partial(kernel, ITERS, group_count, owner_count),
        out_shape=tuple(pltpu.VMEM(x.shape, x.dtype) for x in shapes),
        in_specs=[hbm, hbm, hbm, hbm, smem, hbm],
        out_specs=(vmem, vmem, vmem),
        scratch_shapes=[
            pltpu.VMEM((width, row_count), jnp.float32),
            pltpu.VMEM((1, row_count), jnp.float32),
            pltpu.SMEM((tile_count,), jnp.int32),
            pltpu.SMEM((tile_count,), jnp.int32),
            dma((4,)),
            pltpu.VMEM(matrix.shape, jnp.bfloat16),
            pltpu.VMEM(matrix.shape, jnp.bfloat16),
            pltpu.VMEM((tile_count, owned, 16, 128), jnp.bfloat16),
            pltpu.VMEM((tile_count + 1, width, part), jnp.float32),
            pltpu.VMEM((2, owner_count, width, part), jnp.bfloat16),
            pltpu.VMEM((owner_count, width, part), jnp.bfloat16),
            pltpu.VMEM((owner_count, total_cols, part), jnp.bfloat16),
            pltpu.VMEM((group_count, width, part), jnp.bfloat16),
            pltpu.VMEM((total_cols + width, row_count), jnp.bfloat16),
            pltpu.VMEM((back_count, width, part), jnp.bfloat16),
            pltpu.VMEM((2, back_count, width, part), jnp.bfloat16),
            pltpu.VMEM((group_count, width, part), jnp.bfloat16),
            pltpu.VMEM((group_count, width, part), jnp.bfloat16),
            pltpu.VMEM((pair_count, width, part), jnp.bfloat16),
            pltpu.VMEM((2, pair_count, width, part), jnp.bfloat16),
            pltpu.VMEM((2, 2 * group_count, packed, total_cols), jnp.bfloat16),
            pltpu.VMEM((total_cols, part), jnp.float32),
            pltpu.VMEM((total_cols, part), jnp.float32),
            pltpu.VMEM((total_cols, total_cols), jnp.float32),
            pltpu.VMEM((8, owned * owner_count), jnp.int32),
            pltpu.SMEM((8, owned * owner_count), jnp.int32),
            dma, dma,
            dma, dma((2, owner_count // 2 - 1)), dma, dma((2,)), dma, dma,
            dma, dma((2,)), dma, dma((2,)), dma, dma, dma, dma((2,)),
        ],
        compiler_params=pltpu.CompilerParams(
            collective_id=0, has_side_effects=True, vmem_limit_bytes=60 * 1024 * 1024
        ),
    )(start_block, dual_shift[None, :], tile_rows[0, 0], tile_cols[0, 0], live_tiles[0], matrix)
    return pl.pallas_call(hand_on, out_shape=shapes, in_specs=[vmem] * 3, out_specs=(vmem,) * 3,
        compiler_params=pltpu.CompilerParams(vmem_limit_bytes=2 * 1024 * 1024))(*outs)


def solution(mesh):
    in_specs = (
        P("grp", "row", None, None, None),
        P("grp", "row", None),
        P("grp", "row", None),
        P("grp", "row"),
        P("row"),
        P(None, "row"),
    )
    out_specs = (P(), P(), P(None, "row"))
    return jax.shard_map(
        per_device, mesh=mesh, in_specs=in_specs, out_specs=out_specs, check_vma=False
    )
```

```python
import functools

import jax
import jax.numpy as jnp
from jax import lax
from jax.experimental import pallas as pl
from jax.experimental.pallas import tpu as pltpu
from jax.sharding import PartitionSpec as P

ITERS = 4
MESH = pl.DeviceIdType.MESH
HIGH = lax.Precision.HIGHEST
NT = (((1,), (1,)), ((), ()))
MIDDLE = 1.25
PANEL = 16
SIDE = 4
NEAR = 2


def dot_nt(a, b):
    return lax.dot_general(a, b, NT, precision=HIGH, preferred_element_type=jnp.float32)


def dot_nn(a, b):
    return jnp.dot(a, b, precision=HIGH, preferred_element_type=jnp.float32)


def factor_and_inverse(gram):
    n = gram.shape[0]
    row = lax.broadcasted_iota(jnp.int32, (n, n), 0)
    lane = lax.broadcasted_iota(jnp.int32, (n, n), 1)
    within = lax.broadcasted_iota(jnp.int32, (PANEL, 2 * n), 0)
    work = jnp.concatenate([gram, jnp.where(row == lane, 1.0, 0.0)], axis=1)
    blocks = []
    for start in range(0, n, PANEL):
        columns = [jnp.broadcast_to(work[:, k : k + 1], work.shape) for k in range(start, start + PANEL)]
        rows = [work[i : i + 1, :] for i in range(PANEL)]
        block = jnp.zeros((PANEL, 2 * n), jnp.float32)
        for i in range(0, PANEL, 2):
            first, second = columns[i], columns[i + 1]
            corner, cross, other = first[i : i + 1, :], first[i + 1 : i + 2, :], second[i + 1 : i + 2, :]
            det = corner * other - cross * cross
            scale, root = lax.rsqrt(corner), lax.rsqrt(det)
            left, right = root * scale * corner, root * scale * cross
            columns[i] = first * scale
            columns[i + 1] = second * left - first * right
            upper_row, lower_row = rows[i], rows[i + 1]
            rows[i] = upper_row * scale
            rows[i + 1] = lower_row * left - upper_row * right
            for later in range(i + 2, PANEL):
                for k in (i, i + 1):
                    weight = columns[k][later : later + 1, :]
                    columns[later] = columns[later] - columns[k] * weight
                    rows[later] = rows[later] - rows[k] * weight
            block = jnp.where(within == i, rows[i], block)
            block = jnp.where(within == i + 1, rows[i + 1], block)
        blocks.append(block)
        work = work[PANEL:]
        if start + PANEL < n:
            for i in range(PANEL):
                work = work - columns[i][PANEL:] * rows[i]
    whole = jnp.concatenate(blocks, axis=0)
    return jnp.where(lane >= row, whole[:, :n], 0.0), whole[:, n:]


def away(d, chips):
    return min(d % SIDE, SIDE - d % SIDE) + min(d // SIDE, chips // SIDE - d // SIDE)


def far_first(chips):
    return sorted(range(1, chips), key=lambda d: -away(d, chips))


def kernel(
    steps, group_count, owner_count,
    start_hbm, shift_hbm, rows_hbm, cols_hbm, live_ref, tiles_hbm,
    proj_ref, fac_ref, next_ref,
    start_ref, shift_ref, rows_ref, cols_ref, input_sem, tiles_ref, turned, masks, products, gathered, stage, history, own, own_history, back_out, back_in, direct_out, direct_in,
    pair_out, pair_in, dots_grp, basis, images, transform, place_vector, place_ref, tile_sem, place_sem,
    gather_send, gather_recv, relay_send, relay_recv, own_send, own_recv,
    pair_send, pair_recv, back_send, back_recv, direct_send, direct_recv, dots_send, dots_recv,
):
    g = lax.axis_index("grp")
    r = lax.axis_index("row")
    width = start_ref.shape[0]
    row_count = start_ref.shape[1]
    part = row_count // group_count
    tile_count = tiles_ref.shape[0]
    owned = row_count // tiles_ref.shape[1]
    chips = owner_count // 2
    chip, core = r // 2, lax.rem(r, 2)
    partner = chip * 2 + 1 - core
    chip_x, chip_z = lax.rem(chip, SIDE), chip // SIDE

    offsets = far_first(chips)

    def chip_at(d, sign):
        z_count = chips // SIDE
        return lax.rem(chip_z + (sign * (d // SIDE)) % z_count, z_count) * SIDE + lax.rem(
            chip_x + (sign * (d % SIDE)) % SIDE, SIDE
        )

    far_count = sum(away(d, chips) > NEAR for d in offsets)
    sources = [chip_at(d, -1) for d in offsets]
    targets = [chip_at(d, 1) for d in offsets]
    grp_order = sorted(range(1, group_count), key=lambda d: -min(d, group_count - d))
    grp_peers = [lax.rem(g + d, group_count) for d in grp_order]
    total_cols = steps * width

    inputs = [
        pltpu.make_async_copy(src, dst, input_sem.at[i])
        for i, (src, dst) in enumerate(
            [(start_hbm, start_ref), (shift_hbm, shift_ref), (rows_hbm, rows_ref), (cols_hbm, cols_ref)]
        )
    ]
    for copy in inputs:
        copy.start()
    load = pltpu.make_async_copy(tiles_hbm, tiles_ref, tile_sem)
    load.start()
    barrier = pltpu.get_barrier_semaphore()
    for peer in targets:
        pl.semaphore_signal(barrier, inc=1, device_id=(g, peer * 2 + core), device_id_type=MESH)
    pl.semaphore_signal(barrier, inc=1, device_id=(g, partner), device_id_type=MESH)
    for peer in grp_peers:
        pl.semaphore_signal(barrier, inc=1, device_id=(peer, r), device_id_type=MESH)

    def to_row(peer, src, dst, send, recv):
        return pltpu.make_async_remote_copy(
            src_ref=src, dst_ref=dst, send_sem=send, recv_sem=recv,
            device_id=(g, peer), device_id_type=MESH,
        )

    def to_grp(peer, src, dst, send, recv):
        return pltpu.make_async_remote_copy(
            src_ref=src, dst_ref=dst, send_sem=send, recv_sem=recv,
            device_id=(peer, r), device_id_type=MESH,
        )

    others = group_count - 1

    def send_vectors(half, operand, relayed=True, own_too=True):
        gathered[half, r] = operand
        if own_too:
            own[g] = operand
            for peer in grp_peers:
                to_grp(peer, own.at[g], own.at[g], own_send, own_recv).start()
        for i, peer in enumerate(targets):
            to_row(
                peer * 2 + core, gathered.at[half, r], gathered.at[half, r], gather_send, gather_recv.at[half, i]
            ).start()
        if relayed:
            to_row(partner, gathered.at[half, r], gathered.at[half, r], gather_send, relay_recv.at[half]).start()
        stage[r] = operand

    def sent_vectors(relayed=True, own_too=True):
        bulk = gathered.at[0, pl.ds(0, chips if relayed else chips - 1)]
        to_row(partner, bulk, bulk, gather_send, gather_send).wait_send()
        if own_too:
            bulk = own.at[pl.ds(0, others)]
            to_grp(grp_peers[0], bulk, bulk, own_send, own_send).wait_send()

    def take_own():
        bulk = own.at[pl.ds(0, others)]
        to_grp(grp_peers[0], bulk, bulk, own_recv, own_recv).wait_recv()

    def keep_own(step):
        for i in range(group_count):
            own_history[step * width : (step + 1) * width, i * part : (i + 1) * part] = own[i]

    def take_gathered(step, half):
        dots, batch = None, [r]
        for count, (i, peer) in enumerate(reversed(list(enumerate(sources)))):
            slot = peer * 2 + core
            block = gathered.at[half, slot]
            to_row(slot, block, block, gather_send, gather_recv.at[half, i]).wait_recv()
            if step < steps:
                to_row(partner, block, block, relay_send, relay_recv.at[half]).start()
            stage[slot] = gathered[half, slot]
            batch.append(slot)
            if count % 5 == 4:
                value = slot_dots(step, batch)
                dots = value if dots is None else dots + value
                batch = []
        return dots

    def relays_sent():
        bulk = gathered.at[0, pl.ds(0, chips - 1)]
        to_row(partner, bulk, bulk, relay_send, relay_send).wait_send()

    def take_relayed(half):
        bulk = gathered.at[half, pl.ds(0, chips)]
        to_row(partner, bulk, bulk, gather_send, relay_recv.at[half]).wait_recv()
        for peer in range(chips):
            slot = peer * 2 + 1 - core
            stage[slot] = gathered[half, slot]

    def pack(dots):
        pieces, done, count = [], 0, dots.shape[1]
        for size in (128, 64, 32):
            while count - done >= size:
                height = width * size // 128
                piece = dots[:, done : done + size]
                pieces.append(
                    jnp.concatenate([piece[i * height : (i + 1) * height] for i in range(width // height)], axis=1)
                )
                done += size
        return jnp.concatenate(pieces, axis=0)

    def unpack(packed, count):
        pieces, done, row = [], 0, 0
        for size in (128, 64, 32):
            while count - done >= size:
                height = width * size // 128
                piece = packed[row : row + height]
                pieces.append(
                    jnp.concatenate([piece[:, i * size : (i + 1) * size] for i in range(width // height)], axis=0)
                )
                done += size
                row += height
        return pieces

    def packed_rows(step):
        return pl.ds(0, 16 + (step + 1) // 2 * 16)

    def slot_dots(step, slots):
        dots = jnp.zeros((width, (step + 1) * width), jnp.float32)
        for slot in slots:
            vector = stage[slot]
            right = vector
            if step > 0:
                right = jnp.concatenate([vector, history[slot, : step * width, :]], axis=0)
            dots = dots + lax.dot_general(vector, right, NT, preferred_element_type=jnp.float32)
        return dots

    def send_dots(step, half, dots):
        rows = packed_rows(step)
        me = g * 2 + core
        gram = pack(dots[:, :width])
        high = gram.astype(jnp.bfloat16).astype(jnp.float32)
        dots_grp[half, me, :16] = jnp.concatenate([high, gram - high], axis=0).astype(jnp.bfloat16)
        if step > 0:
            cross = pack(dots[:, width:])
            if step % 2 == 1:
                cross = jnp.concatenate([cross, jnp.zeros((8, 128), jnp.float32)], axis=0)
            dots_grp[half, me, 16 : 16 + cross.shape[0]] = cross.astype(jnp.bfloat16)
        block = dots_grp.at[half, me, rows]
        for peer in grp_peers:
            to_grp(peer, block, block, dots_send, dots_recv.at[half]).start()
            pltpu.make_async_remote_copy(
                src_ref=block, dst_ref=block, send_sem=dots_send, recv_sem=dots_recv.at[half],
                device_id=(peer, partner), device_id_type=MESH,
            ).start()
        to_row(partner, block, block, dots_send, dots_recv.at[half]).start()

    def take_dots(step, half):
        rows = packed_rows(step)
        bulk = dots_grp.at[half, pl.ds(0, 2 * group_count - 1), rows]
        to_grp(grp_peers[0], bulk, bulk, dots_send, dots_recv.at[half]).wait_recv()
        summed = dots_grp[half, 0, rows].astype(jnp.float32)
        for index in range(1, 2 * group_count):
            summed = summed + dots_grp[half, index, rows].astype(jnp.float32)
        gram = unpack(summed[:8] + summed[8:16], width)[0]
        if step == 0:
            return None, gram
        pieces = unpack(summed[16:], step * width)
        whole = jnp.concatenate(pieces, axis=1) if len(pieces) > 1 else pieces[0]
        cross = dot_nt(whole, transform[:, : step * width])
        return cross, gram - dot_nt(cross, cross)

    def dots_sent(step, half):
        bulk = dots_grp.at[half, pl.ds(0, 2 * group_count - 1), packed_rows(step)]
        to_grp(grp_peers[0], bulk, bulk, dots_send, dots_recv.at[half]).wait_send()

    def back_product(slot):
        value = products[place_ref[0, slot]]
        for i in range(1, owned):
            value = value + products[place_ref[0, i * owner_count + slot]]
        return value

    def take_pair(peer, half):
        return pair_in[half, peer].astype(jnp.float32)

    mine = pl.ds(pl.multiple_of(g * part, part), part)
    for copy in inputs:
        copy.wait()
    current = start_ref[:, mine]
    shift = shift_ref[:, mine]
    pl.semaphore_wait(barrier, chips + others)
    send_vectors(0, current.astype(jnp.bfloat16), own_too=False)
    for i in range(group_count):
        own[i] = start_ref[:, i * part : (i + 1) * part].astype(jnp.bfloat16)
    lanes = lax.broadcasted_iota(jnp.int32, place_vector.shape, 1)
    place = jnp.full(place_vector.shape, tile_count, jnp.int32)
    for k in range(tile_count):
        alive = k < live_ref[0]
        position = jnp.where(alive, rows_ref[k] * owner_count + cols_ref[k], -1)
        place = jnp.where(lanes == position, k, place)
        row = jnp.full((8, 128), jnp.where(alive, rows_ref[k], -1), jnp.int32)
        for i in range(owned):
            masks[k, i] = jnp.where(row == i, 1.0, 0.0)
    place_vector[...] = place
    place_copy = pltpu.make_async_copy(place_vector, place_ref, place_sem)
    place_copy.start()
    basis[...] = jnp.zeros_like(basis)
    images[...] = jnp.zeros_like(images)
    transform[...] = jnp.zeros_like(transform)
    products[tile_count] = jnp.zeros((width, part), jnp.float32)
    load.wait()
    place_copy.wait()

    def turn(j, carry):
        for i in range(4):
            turned[j * 4 + i] = tiles_ref[j * 4 + i].T
        return carry

    coef = None
    lane = lax.broadcasted_iota(jnp.int32, (width, total_cols), 1)
    sub = lax.broadcasted_iota(jnp.int32, (width, total_cols), 0)
    for step in range(steps):
        half = step % 2
        far = far_count if step > 0 else 0
        near_rows = pl.ds(0, chips - far)
        if step > 0:
            take_own()
        for k in range(tile_count):
            products[k] = jnp.dot(own[rows_ref[k]], tiles_ref[k], preferred_element_type=jnp.float32)
        for i, peer in enumerate(targets[far:] + [chip]):
            pair_out[i] = back_product(peer * 2 + 1 - core).astype(jnp.bfloat16)
            to_row(partner, pair_out.at[i], pair_in.at[half, i], pair_send, pair_recv.at[half]).start()
        for i, peer in enumerate(targets[:far]):
            for side, slot in enumerate([peer * 2 + core, peer * 2 + 1 - core]):
                index = 2 * i + side
                back_out[index] = back_product(slot).astype(jnp.bfloat16)
                to_row(
                    slot, back_out.at[index], back_in.at[half, index], back_send, back_recv.at[half]
                ).start()
        keep_own(step)
        if step == 0:
            lax.fori_loop(0, tile_count // 4, turn, 0)
        def send_back():
            to_row(
                partner, pair_out.at[near_rows], pair_in.at[half, near_rows], pair_send, pair_recv.at[half]
            ).wait_recv()
            for i, peer in enumerate(targets[far:]):
                index = 2 * far + i
                back_out[index] = (back_product(peer * 2 + core) + take_pair(i, half)).astype(jnp.bfloat16)
                to_row(
                    peer * 2 + core, back_out.at[index], back_in.at[half, index], back_send, back_recv.at[half]
                ).start()
            total = back_product(r) + take_pair(len(targets) - far, half)
            return total

        if step == 0:
            total = send_back()
        dots = take_gathered(step, half)
        send_dots(step, half, dots)
        if step > 0:
            total = send_back()
        take_relayed(half)
        forward = [jnp.zeros((width, part), jnp.float32)] * owned
        for k in range(tile_count):
            value = jnp.dot(stage[cols_ref[k]], turned[k], preferred_element_type=jnp.float32)
            for i in range(owned):
                mask = jnp.concatenate([masks[k, i]] * (part // 128), axis=1)
                forward[i] = forward[i] + value * jnp.concatenate([mask] * (width // 8), axis=0)
        for i in range(owned):
            direct_out[i] = forward[i].astype(jnp.bfloat16)
        for peer in grp_peers:
            to_grp(peer, direct_out.at[peer], direct_in.at[g], direct_send, direct_recv).start()
        for i in range(owned):
            total = total + forward[i] * jnp.where(g == i, 1.0, 0.0)
        for slot in range(owner_count):
            history[slot, step * width : (step + 1) * width, :] = stage[slot]
        sent_vectors(own_too=step > 0)
        relays_sent()
        cross, gram = take_dots(step, half)
        left, rest = current, None
        if step > 0:
            left = left - dot_nn(cross, basis[...])
            rest = dot_nn(cross, images[...])
        upper, inverse = factor_and_inverse(gram)
        now = dot_nn(inverse, left)
        ahead = now * (MIDDLE - shift)
        if step > 0:
            ahead = ahead - dot_nn(upper, basis[(step - 1) * width : step * width, :])
        bulk = back_in.at[half, pl.ds(0, chips - 1 + far)]
        to_row(partner, bulk, bulk, back_send, back_recv.at[half]).wait_recv()
        for index in range(chips - 1 + far):
            total = total + back_in[half, index].astype(jnp.float32)
        bulk = direct_in.at[pl.ds(0, others)]
        to_grp(grp_peers[0], bulk, bulk, direct_send, direct_recv).wait_recv()
        for peer in grp_peers:
            total = total + direct_in[peer].astype(jnp.float32)
        total = 0.5 * total
        if step > 0:
            total = total - rest
        image = dot_nn(inverse, total)
        current = image + ahead
        send_vectors(1 - half, current.astype(jnp.bfloat16), step < steps - 1)
        basis[step * width : (step + 1) * width, :] = now
        images[step * width : (step + 1) * width, :] = image
        if step > 0:
            proj_ref[step - 1] = cross + coef
            fac_ref[step - 1] = upper.T
        unit = jnp.where(lane == step * width + sub, 1.0, 0.0)
        if step == 0:
            transform[:width, :] = dot_nn(inverse, unit)
            coef = -MIDDLE * unit
        else:
            transform[step * width : (step + 1) * width, :] = dot_nn(inverse, unit - dot_nn(cross, transform[...]))
            wide = jnp.concatenate([upper] * (total_cols // width), axis=1)
            coef = -MIDDLE * unit + jnp.where((lane >= (step - 1) * width) & (lane < step * width), wide, 0.0)
        bulk = pair_out.at[near_rows]
        to_row(partner, bulk, bulk, pair_send, pair_recv.at[half]).wait_send()
        bulk = back_out.at[pl.ds(0, chips - 1 + far)]
        to_row(partner, bulk, bulk, back_send, back_recv.at[half]).wait_send()
        bulk = direct_out.at[pl.ds(0, others)]
        to_grp(grp_peers[0], bulk, bulk, direct_send, direct_recv).wait_send()
        dots_sent(step, half)

    half = steps % 2
    dots = take_gathered(steps, half)
    send_dots(steps, half, dots)
    take_own()
    keep_own(steps)
    sent_vectors(False)
    cross, gram = take_dots(steps, half)
    combine = dot_nn(cross, transform[...])
    high = combine.astype(jnp.bfloat16)
    low = (combine - high.astype(jnp.float32)).astype(jnp.bfloat16)
    both = jnp.dot(
        jnp.concatenate([high, low], axis=0), own_history[:total_cols, :], preferred_element_type=jnp.float32
    )
    left = own_history[total_cols:, :].astype(jnp.float32) - both[:width] - both[width:]
    upper, inverse = factor_and_inverse(gram)
    proj_ref[steps - 1] = cross + coef
    fac_ref[steps - 1] = upper.T
    next_ref[...] = dot_nn(inverse, left)
    dots_sent(steps, half)


def hand_on(proj_in, fac_in, next_in, proj_ref, fac_ref, next_ref):
    proj_ref[...] = proj_in[...]
    fac_ref[...] = fac_in[...]
    next_ref[...] = next_in[...]


def per_device(tiles, tile_rows, tile_cols, live_tiles, dual_shift, start_block):
    matrix = tiles[0, 0]
    tile_count, edge = matrix.shape[0], matrix.shape[1]
    width, row_count = start_block.shape
    group_count = lax.axis_size("grp")
    owner_count = lax.axis_size("row")
    owned = row_count // edge
    part = row_count // group_count
    total_cols = ITERS * width
    vmem = pl.BlockSpec(memory_space=pltpu.VMEM)
    smem = pl.BlockSpec(memory_space=pltpu.SMEM)
    hbm = pl.BlockSpec(memory_space=pltpu.HBM)
    dma = pltpu.SemaphoreType.DMA
    chips = owner_count // 2
    far = sum(away(d, chips) > NEAR for d in far_first(chips))
    back_count = chips - 1 + far
    pair_count = chips
    packed = 16 + (ITERS + 1) // 2 * 16
    shapes = (
            jax.ShapeDtypeStruct((ITERS, width, total_cols), jnp.float32),
            jax.ShapeDtypeStruct((ITERS, width, width), jnp.float32),
            jax.ShapeDtypeStruct((width, row_count), jnp.float32),
    )
    outs = pl.pallas_call(
        functools.partial(kernel, ITERS, group_count, owner_count),
        out_shape=tuple(pltpu.VMEM(x.shape, x.dtype) for x in shapes),
        in_specs=[hbm, hbm, hbm, hbm, smem, hbm],
        out_specs=(vmem, vmem, vmem),
        scratch_shapes=[
            pltpu.VMEM((width, row_count), jnp.float32),
            pltpu.VMEM((1, row_count), jnp.float32),
            pltpu.SMEM((tile_count,), jnp.int32),
            pltpu.SMEM((tile_count,), jnp.int32),
            dma((4,)),
            pltpu.VMEM(matrix.shape, jnp.bfloat16),
            pltpu.VMEM(matrix.shape, jnp.bfloat16),
            pltpu.VMEM((tile_count, owned, 8, 128), jnp.float32),
            pltpu.VMEM((tile_count + 1, width, part), jnp.float32),
            pltpu.VMEM((2, owner_count, width, part), jnp.bfloat16),
            pltpu.VMEM((owner_count, width, part), jnp.bfloat16),
            pltpu.VMEM((owner_count, total_cols, part), jnp.bfloat16),
            pltpu.VMEM((group_count, width, part), jnp.bfloat16),
            pltpu.VMEM((total_cols + width, row_count), jnp.bfloat16),
            pltpu.VMEM((back_count, width, part), jnp.bfloat16),
            pltpu.VMEM((2, back_count, width, part), jnp.bfloat16),
            pltpu.VMEM((group_count, width, part), jnp.bfloat16),
            pltpu.VMEM((group_count, width, part), jnp.bfloat16),
            pltpu.VMEM((pair_count, width, part), jnp.bfloat16),
            pltpu.VMEM((2, pair_count, width, part), jnp.bfloat16),
            pltpu.VMEM((2, 2 * group_count, packed, total_cols), jnp.bfloat16),
            pltpu.VMEM((total_cols, part), jnp.float32),
            pltpu.VMEM((total_cols, part), jnp.float32),
            pltpu.VMEM((total_cols, total_cols), jnp.float32),
            pltpu.VMEM((8, owned * owner_count), jnp.int32),
            pltpu.SMEM((8, owned * owner_count), jnp.int32),
            dma, dma,
            dma, dma((2, owner_count // 2 - 1)), dma, dma((2,)), dma, dma,
            dma, dma((2,)), dma, dma((2,)), dma, dma, dma, dma((2,)),
        ],
        compiler_params=pltpu.CompilerParams(
            collective_id=0, has_side_effects=True, vmem_limit_bytes=60 * 1024 * 1024
        ),
    )(start_block, dual_shift[None, :], tile_rows[0, 0], tile_cols[0, 0], live_tiles[0], matrix)
    return pl.pallas_call(hand_on, out_shape=shapes, in_specs=[vmem] * 3, out_specs=(vmem,) * 3,
        compiler_params=pltpu.CompilerParams(vmem_limit_bytes=2 * 1024 * 1024))(*outs)


def solution(mesh):
    in_specs = (
        P("grp", "row", None, None, None),
        P("grp", "row", None),
        P("grp", "row", None),
        P("grp", "row"),
        P("row"),
        P(None, "row"),
    )
    out_specs = (P(), P(), P(None, "row"))
    return jax.shard_map(
        per_device, mesh=mesh, in_specs=in_specs, out_specs=out_specs, check_vma=False
    )
```

```python
import functools

import jax
import jax.numpy as jnp
from jax import lax
from jax.experimental import pallas as pl
from jax.experimental.pallas import tpu as pltpu
from jax.sharding import PartitionSpec as P

ITERS = 4
MESH = pl.DeviceIdType.MESH
HIGH = lax.Precision.HIGHEST
NT = (((1,), (1,)), ((), ()))
MIDDLE = 1.25
PANEL = 16
SIDE = 4
NEAR = 2


def dot_nt(a, b):
    return lax.dot_general(a, b, NT, precision=HIGH, preferred_element_type=jnp.float32)


def dot_nn(a, b):
    return jnp.dot(a, b, precision=HIGH, preferred_element_type=jnp.float32)


def factor_and_inverse(gram):
    n = gram.shape[0]
    row = lax.broadcasted_iota(jnp.int32, (n, n), 0)
    lane = lax.broadcasted_iota(jnp.int32, (n, n), 1)
    within = lax.broadcasted_iota(jnp.int32, (PANEL, 2 * n), 0)
    work = jnp.concatenate([gram, jnp.where(row == lane, 1.0, 0.0)], axis=1)
    blocks = []
    for start in range(0, n, PANEL):
        columns = [jnp.broadcast_to(work[:, k : k + 1], work.shape) for k in range(start, start + PANEL)]
        rows = [work[i : i + 1, :] for i in range(PANEL)]
        block = jnp.zeros((PANEL, 2 * n), jnp.float32)
        for i in range(0, PANEL, 2):
            first, second = columns[i], columns[i + 1]
            corner, cross, other = first[i : i + 1, :], first[i + 1 : i + 2, :], second[i + 1 : i + 2, :]
            det = corner * other - cross * cross
            scale, root = lax.rsqrt(corner), lax.rsqrt(det)
            left, right = root * scale * corner, root * scale * cross
            columns[i] = first * scale
            columns[i + 1] = second * left - first * right
            upper_row, lower_row = rows[i], rows[i + 1]
            rows[i] = upper_row * scale
            rows[i + 1] = lower_row * left - upper_row * right
            for later in range(i + 2, PANEL):
                for k in (i, i + 1):
                    weight = columns[k][later : later + 1, :]
                    columns[later] = columns[later] - columns[k] * weight
                    rows[later] = rows[later] - rows[k] * weight
            block = jnp.where(within == i, rows[i], block)
            block = jnp.where(within == i + 1, rows[i + 1], block)
        blocks.append(block)
        work = work[PANEL:]
        if start + PANEL < n:
            for i in range(PANEL):
                work = work - columns[i][PANEL:] * rows[i]
    whole = jnp.concatenate(blocks, axis=0)
    return jnp.where(lane >= row, whole[:, :n], 0.0), whole[:, n:]


def away(d, chips):
    return min(d % SIDE, SIDE - d % SIDE) + min(d // SIDE, chips // SIDE - d // SIDE)


def far_first(chips):
    return sorted(range(1, chips), key=lambda d: -away(d, chips))


def kernel(
    steps, group_count, owner_count,
    start_hbm, shift_hbm, rows_hbm, cols_hbm, live_ref, tiles_hbm,
    proj_ref, fac_ref, next_ref,
    start_ref, shift_ref, rows_ref, cols_ref, input_sem, tiles_ref, turned, masks, products, gathered, stage, history, own, own_history, back_out, back_in, direct_out, direct_in,
    pair_out, pair_in, dots_grp, chip_out, chip_in, basis, images, transform, place_vector, place_ref, tile_sem, place_sem,
    gather_send, gather_recv, relay_send, relay_recv, own_send, own_recv,
    pair_send, pair_recv, back_send, back_recv, direct_send, direct_recv, dots_send, dots_recv, chip_send, chip_recv,
):
    g = lax.axis_index("grp")
    r = lax.axis_index("row")
    width = start_ref.shape[0]
    row_count = start_ref.shape[1]
    part = row_count // group_count
    tile_count = tiles_ref.shape[0]
    owned = row_count // tiles_ref.shape[1]
    chips = owner_count // 2
    chip, core = r // 2, lax.rem(r, 2)
    partner = chip * 2 + 1 - core
    chip_x, chip_z = lax.rem(chip, SIDE), chip // SIDE

    offsets = far_first(chips)

    def chip_at(d, sign):
        z_count = chips // SIDE
        return lax.rem(chip_z + (sign * (d // SIDE)) % z_count, z_count) * SIDE + lax.rem(
            chip_x + (sign * (d % SIDE)) % SIDE, SIDE
        )

    far_count = sum(away(d, chips) > NEAR for d in offsets)
    sources = [chip_at(d, -1) for d in offsets]
    targets = [chip_at(d, 1) for d in offsets]
    grp_order = sorted(range(1, group_count), key=lambda d: -min(d, group_count - d))
    grp_peers = [lax.rem(g + d, group_count) for d in grp_order]
    total_cols = steps * width

    inputs = [
        pltpu.make_async_copy(src, dst, input_sem.at[i])
        for i, (src, dst) in enumerate(
            [(start_hbm, start_ref), (shift_hbm, shift_ref), (rows_hbm, rows_ref), (cols_hbm, cols_ref)]
        )
    ]
    for copy in inputs:
        copy.start()
    load = pltpu.make_async_copy(tiles_hbm, tiles_ref, tile_sem)
    load.start()
    barrier = pltpu.get_barrier_semaphore()
    for peer in targets:
        pl.semaphore_signal(barrier, inc=1, device_id=(g, peer * 2 + core), device_id_type=MESH)
    pl.semaphore_signal(barrier, inc=1, device_id=(g, partner), device_id_type=MESH)
    for peer in grp_peers:
        pl.semaphore_signal(barrier, inc=1, device_id=(peer, r), device_id_type=MESH)

    def to_row(peer, src, dst, send, recv):
        return pltpu.make_async_remote_copy(
            src_ref=src, dst_ref=dst, send_sem=send, recv_sem=recv,
            device_id=(g, peer), device_id_type=MESH,
        )

    def to_grp(peer, src, dst, send, recv):
        return pltpu.make_async_remote_copy(
            src_ref=src, dst_ref=dst, send_sem=send, recv_sem=recv,
            device_id=(peer, r), device_id_type=MESH,
        )

    others = group_count - 1

    def send_own(operand):
        own[g] = operand
        for peer in grp_peers:
            to_grp(peer, own.at[g], own.at[g], own_send, own_recv).start()

    def send_vectors(half, operand, own_too=True):
        gathered[half, r] = operand
        if own_too:
            send_own(operand)
        for i, peer in enumerate(targets):
            to_row(
                peer * 2 + core, gathered.at[half, r], gathered.at[half, r], gather_send, gather_recv.at[half, i]
            ).start()
        to_row(partner, gathered.at[half, r], gathered.at[half, r], gather_send, relay_recv.at[half]).start()
        stage[r] = operand

    def sent_own():
        bulk = own.at[pl.ds(0, others)]
        to_grp(grp_peers[0], bulk, bulk, own_send, own_send).wait_send()

    def sent_vectors():
        bulk = gathered.at[0, pl.ds(0, chips)]
        to_row(partner, bulk, bulk, gather_send, gather_send).wait_send()

    def take_own():
        bulk = own.at[pl.ds(0, others)]
        to_grp(grp_peers[0], bulk, bulk, own_recv, own_recv).wait_recv()

    def keep_own(step):
        for i in range(group_count):
            own_history[step * width : (step + 1) * width, i * part : (i + 1) * part] = own[i]

    def take_gathered(step, half):
        dots, batch = None, [r]
        for count, (i, peer) in enumerate(reversed(list(enumerate(sources)))):
            slot = peer * 2 + core
            block = gathered.at[half, slot]
            to_row(slot, block, block, gather_send, gather_recv.at[half, i]).wait_recv()
            to_row(partner, block, block, relay_send, relay_recv.at[half]).start()
            stage[slot] = gathered[half, slot]
            batch.append(slot)
            if count % 5 == 4:
                value = slot_dots(step, batch)
                dots = value if dots is None else dots + value
                batch = []
        return dots

    def relays_sent():
        bulk = gathered.at[0, pl.ds(0, chips - 1)]
        to_row(partner, bulk, bulk, relay_send, relay_send).wait_send()

    def take_relayed(half):
        bulk = gathered.at[half, pl.ds(0, chips)]
        to_row(partner, bulk, bulk, gather_send, relay_recv.at[half]).wait_recv()
        for peer in range(chips):
            slot = peer * 2 + 1 - core
            stage[slot] = gathered[half, slot]

    def pack(dots):
        pieces, done, count = [], 0, dots.shape[1]
        for size in (128, 64, 32):
            while count - done >= size:
                height = width * size // 128
                piece = dots[:, done : done + size]
                pieces.append(
                    jnp.concatenate([piece[i * height : (i + 1) * height] for i in range(width // height)], axis=1)
                )
                done += size
        return jnp.concatenate(pieces, axis=0)

    def unpack(packed, count):
        pieces, done, row = [], 0, 0
        for size in (128, 64, 32):
            while count - done >= size:
                height = width * size // 128
                piece = packed[row : row + height]
                pieces.append(
                    jnp.concatenate([piece[:, i * size : (i + 1) * size] for i in range(width // height)], axis=0)
                )
                done += size
                row += height
        return pieces

    def packed_rows(step):
        return pl.ds(0, 16 + (step + 1) // 2 * 16)

    def slot_dots(step, slots):
        dots = jnp.zeros((width, (step + 1) * width), jnp.float32)
        for slot in slots:
            vector = stage[slot]
            right = vector
            if step > 0:
                right = jnp.concatenate([vector, history[slot, : step * width, :]], axis=0)
            dots = dots + lax.dot_general(vector, right, NT, preferred_element_type=jnp.float32)
        return dots

    def encode(step, dots):
        gram, cross = dots
        high = gram.astype(jnp.bfloat16).astype(jnp.float32)
        pieces = [high, gram - high]
        if step > 0:
            pieces.append(cross)
        if step % 2 == 1:
            pieces.append(jnp.zeros((8, 128), jnp.float32))
        return jnp.concatenate(pieces, axis=0).astype(jnp.bfloat16)

    def pack_both(step, dots):
        return pack(dots[:, :width]), pack(dots[:, width:]) if step > 0 else None

    def send_dots(step, half, dots):
        rows = packed_rows(step)
        me = g * 2 + core
        dots_grp[half, me, rows] = encode(step, dots)
        block = dots_grp.at[half, me, rows]
        for peer in grp_peers:
            to_grp(peer, block, block, dots_send, dots_recv.at[half]).start()
            pltpu.make_async_remote_copy(
                src_ref=block, dst_ref=block, send_sem=dots_send, recv_sem=dots_recv.at[half],
                device_id=(peer, partner), device_id_type=MESH,
            ).start()
        to_row(partner, block, block, dots_send, dots_recv.at[half]).start()

    def take_dots(step, half):
        rows = packed_rows(step)
        bulk = dots_grp.at[half, pl.ds(0, 2 * group_count - 1), rows]
        to_grp(grp_peers[0], bulk, bulk, dots_send, dots_recv.at[half]).wait_recv()
        summed = dots_grp[half, 0, rows].astype(jnp.float32)
        for index in range(1, 2 * group_count):
            summed = summed + dots_grp[half, index, rows].astype(jnp.float32)
        gram = unpack(summed[:8] + summed[8:16], width)[0]
        if step == 0:
            return None, gram
        pieces = unpack(summed[16:], step * width)
        whole = jnp.concatenate(pieces, axis=1) if len(pieces) > 1 else pieces[0]
        cross = dot_nt(whole, transform[:, : step * width])
        return cross, gram - dot_nt(cross, cross)

    def dots_sent(step, half):
        bulk = dots_grp.at[half, pl.ds(0, 2 * group_count - 1), packed_rows(step)]
        to_grp(grp_peers[0], bulk, bulk, dots_send, dots_recv.at[half]).wait_send()

    def back_product(slot):
        value = products[place_ref[0, slot]]
        for i in range(1, owned):
            value = value + products[place_ref[0, i * owner_count + slot]]
        return value

    def take_pair(peer, half):
        return pair_in[half, peer].astype(jnp.float32)

    mine = pl.ds(pl.multiple_of(g * part, part), part)
    for copy in inputs:
        copy.wait()
    current = start_ref[:, mine]
    shift = shift_ref[:, mine]
    pl.semaphore_wait(barrier, chips + others)
    send_vectors(0, current.astype(jnp.bfloat16), own_too=False)
    for i in range(group_count):
        own[i] = start_ref[:, i * part : (i + 1) * part].astype(jnp.bfloat16)
    lanes = lax.broadcasted_iota(jnp.int32, place_vector.shape, 1)
    place = jnp.full(place_vector.shape, tile_count, jnp.int32)
    for k in range(tile_count):
        alive = k < live_ref[0]
        position = jnp.where(alive, rows_ref[k] * owner_count + cols_ref[k], -1)
        place = jnp.where(lanes == position, k, place)
        row = jnp.full((8, 128), jnp.where(alive, rows_ref[k], -1), jnp.int32)
        for i in range(owned):
            masks[k, i] = jnp.where(row == i, 1.0, 0.0)
    place_vector[...] = place
    place_copy = pltpu.make_async_copy(place_vector, place_ref, place_sem)
    place_copy.start()
    basis[...] = jnp.zeros_like(basis)
    images[...] = jnp.zeros_like(images)
    transform[...] = jnp.zeros_like(transform)
    products[tile_count] = jnp.zeros((width, part), jnp.float32)
    load.wait()
    place_copy.wait()

    def turn(j, carry):
        for i in range(4):
            turned[j * 4 + i] = tiles_ref[j * 4 + i].T
        return carry

    coef = None
    lane = lax.broadcasted_iota(jnp.int32, (width, total_cols), 1)
    sub = lax.broadcasted_iota(jnp.int32, (width, total_cols), 0)
    for step in range(steps):
        half = step % 2
        far = far_count if step > 0 else 0
        near_rows = pl.ds(0, chips - far)
        if step > 0:
            take_own()
        for k in range(tile_count):
            products[k] = jnp.dot(own[rows_ref[k]], tiles_ref[k], preferred_element_type=jnp.float32)
        for i, peer in enumerate(targets[far:] + [chip]):
            pair_out[i] = back_product(peer * 2 + 1 - core).astype(jnp.bfloat16)
            to_row(partner, pair_out.at[i], pair_in.at[half, i], pair_send, pair_recv.at[half]).start()
        for i, peer in enumerate(targets[:far]):
            for side, slot in enumerate([peer * 2 + core, peer * 2 + 1 - core]):
                index = 2 * i + side
                back_out[index] = back_product(slot).astype(jnp.bfloat16)
                to_row(
                    slot, back_out.at[index], back_in.at[half, index], back_send, back_recv.at[half]
                ).start()
        keep_own(step)
        if step == 0:
            lax.fori_loop(0, tile_count // 4, turn, 0)
        def send_back():
            to_row(
                partner, pair_out.at[near_rows], pair_in.at[half, near_rows], pair_send, pair_recv.at[half]
            ).wait_recv()
            for i, peer in enumerate(targets[far:]):
                index = 2 * far + i
                back_out[index] = (back_product(peer * 2 + core) + take_pair(i, half)).astype(jnp.bfloat16)
                to_row(
                    peer * 2 + core, back_out.at[index], back_in.at[half, index], back_send, back_recv.at[half]
                ).start()
            total = back_product(r) + take_pair(len(targets) - far, half)
            return total

        if step == 0:
            total = send_back()
        dots = take_gathered(step, half)
        send_dots(step, half, pack_both(step, dots))
        if step > 0:
            total = send_back()
        take_relayed(half)
        forward = [jnp.zeros((width, part), jnp.float32)] * owned
        for k in range(tile_count):
            value = jnp.dot(stage[cols_ref[k]], turned[k], preferred_element_type=jnp.float32)
            for i in range(owned):
                mask = jnp.concatenate([masks[k, i]] * (part // 128), axis=1)
                forward[i] = forward[i] + value * jnp.concatenate([mask] * (width // 8), axis=0)
        for i in range(owned):
            direct_out[i] = forward[i].astype(jnp.bfloat16)
        for peer in grp_peers:
            to_grp(peer, direct_out.at[peer], direct_in.at[g], direct_send, direct_recv).start()
        for i in range(owned):
            total = total + forward[i] * jnp.where(g == i, 1.0, 0.0)
        for slot in range(owner_count):
            history[slot, step * width : (step + 1) * width, :] = stage[slot]
        sent_vectors()
        if step > 0:
            sent_own()
        relays_sent()
        cross, gram = take_dots(step, half)
        left, rest = current, None
        if step > 0:
            left = left - dot_nn(cross, basis[...])
            rest = dot_nn(cross, images[...])
        upper, inverse = factor_and_inverse(gram)
        now = dot_nn(inverse, left)
        ahead = now * (MIDDLE - shift)
        if step > 0:
            ahead = ahead - dot_nn(upper, basis[(step - 1) * width : step * width, :])
        bulk = back_in.at[half, pl.ds(0, chips - 1 + far)]
        to_row(partner, bulk, bulk, back_send, back_recv.at[half]).wait_recv()
        for index in range(chips - 1 + far):
            total = total + back_in[half, index].astype(jnp.float32)
        bulk = direct_in.at[pl.ds(0, others)]
        to_grp(grp_peers[0], bulk, bulk, direct_send, direct_recv).wait_recv()
        for peer in grp_peers:
            total = total + direct_in[peer].astype(jnp.float32)
        total = 0.5 * total
        if step > 0:
            total = total - rest
        image = dot_nn(inverse, total)
        current = image + ahead
        if step < steps - 1:
            send_vectors(1 - half, current.astype(jnp.bfloat16))
        else:
            send_own(current.astype(jnp.bfloat16))
            stage[r] = current.astype(jnp.bfloat16)
            local = pack_both(steps, slot_dots(steps, [r]))
            chip_out[...] = encode(steps, local)
            for i, peer in enumerate(targets):
                to_row(peer * 2 + core, chip_out, chip_in.at[i], chip_send, chip_recv).start()
        basis[step * width : (step + 1) * width, :] = now
        images[step * width : (step + 1) * width, :] = image
        if step > 0:
            proj_ref[step - 1] = cross + coef
            fac_ref[step - 1] = upper.T
        unit = jnp.where(lane == step * width + sub, 1.0, 0.0)
        if step == 0:
            transform[:width, :] = dot_nn(inverse, unit)
            coef = -MIDDLE * unit
        else:
            transform[step * width : (step + 1) * width, :] = dot_nn(inverse, unit - dot_nn(cross, transform[...]))
            wide = jnp.concatenate([upper] * (total_cols // width), axis=1)
            coef = -MIDDLE * unit + jnp.where((lane >= (step - 1) * width) & (lane < step * width), wide, 0.0)
        bulk = pair_out.at[near_rows]
        to_row(partner, bulk, bulk, pair_send, pair_recv.at[half]).wait_send()
        bulk = back_out.at[pl.ds(0, chips - 1 + far)]
        to_row(partner, bulk, bulk, back_send, back_recv.at[half]).wait_send()
        bulk = direct_out.at[pl.ds(0, others)]
        to_grp(grp_peers[0], bulk, bulk, direct_send, direct_recv).wait_send()
        dots_sent(step, half)

    half = steps % 2
    take_own()
    keep_own(steps)
    sent_own()
    to_row(partner, chip_in, chip_in, chip_send, chip_recv).wait_recv()
    summed = chip_in[0].astype(jnp.float32)
    for i in range(1, chips - 1):
        summed = summed + chip_in[i].astype(jnp.float32)
    send_dots(steps, half, (local[0] + summed[:8] + summed[8:16], local[1] + summed[16:]))
    to_row(partner, chip_in, chip_in, chip_send, chip_recv).wait_send()
    cross, gram = take_dots(steps, half)
    combine = dot_nn(cross, transform[...])
    high = combine.astype(jnp.bfloat16)
    low = (combine - high.astype(jnp.float32)).astype(jnp.bfloat16)
    both = jnp.dot(
        jnp.concatenate([high, low], axis=0), own_history[:total_cols, :], preferred_element_type=jnp.float32
    )
    left = own_history[total_cols:, :].astype(jnp.float32) - both[:width] - both[width:]
    upper, inverse = factor_and_inverse(gram)
    proj_ref[steps - 1] = cross + coef
    fac_ref[steps - 1] = upper.T
    next_ref[...] = dot_nn(inverse, left)
    dots_sent(steps, half)


def hand_on(proj_in, fac_in, next_in, proj_ref, fac_ref, next_ref):
    proj_ref[...] = proj_in[...]
    fac_ref[...] = fac_in[...]
    next_ref[...] = next_in[...]


def per_device(tiles, tile_rows, tile_cols, live_tiles, dual_shift, start_block):
    matrix = tiles[0, 0]
    tile_count, edge = matrix.shape[0], matrix.shape[1]
    width, row_count = start_block.shape
    group_count = lax.axis_size("grp")
    owner_count = lax.axis_size("row")
    owned = row_count // edge
    part = row_count // group_count
    total_cols = ITERS * width
    vmem = pl.BlockSpec(memory_space=pltpu.VMEM)
    smem = pl.BlockSpec(memory_space=pltpu.SMEM)
    hbm = pl.BlockSpec(memory_space=pltpu.HBM)
    dma = pltpu.SemaphoreType.DMA
    chips = owner_count // 2
    far = sum(away(d, chips) > NEAR for d in far_first(chips))
    back_count = chips - 1 + far
    pair_count = chips
    packed = 16 + (ITERS + 1) // 2 * 16
    shapes = (
            jax.ShapeDtypeStruct((ITERS, width, total_cols), jnp.float32),
            jax.ShapeDtypeStruct((ITERS, width, width), jnp.float32),
            jax.ShapeDtypeStruct((width, row_count), jnp.float32),
    )
    outs = pl.pallas_call(
        functools.partial(kernel, ITERS, group_count, owner_count),
        out_shape=tuple(pltpu.VMEM(x.shape, x.dtype) for x in shapes),
        in_specs=[hbm, hbm, hbm, hbm, smem, hbm],
        out_specs=(vmem, vmem, vmem),
        scratch_shapes=[
            pltpu.VMEM((width, row_count), jnp.float32),
            pltpu.VMEM((1, row_count), jnp.float32),
            pltpu.SMEM((tile_count,), jnp.int32),
            pltpu.SMEM((tile_count,), jnp.int32),
            dma((4,)),
            pltpu.VMEM(matrix.shape, jnp.bfloat16),
            pltpu.VMEM(matrix.shape, jnp.bfloat16),
            pltpu.VMEM((tile_count, owned, 8, 128), jnp.float32),
            pltpu.VMEM((tile_count + 1, width, part), jnp.float32),
            pltpu.VMEM((2, owner_count, width, part), jnp.bfloat16),
            pltpu.VMEM((owner_count, width, part), jnp.bfloat16),
            pltpu.VMEM((owner_count, total_cols, part), jnp.bfloat16),
            pltpu.VMEM((group_count, width, part), jnp.bfloat16),
            pltpu.VMEM((total_cols + width, row_count), jnp.bfloat16),
            pltpu.VMEM((back_count, width, part), jnp.bfloat16),
            pltpu.VMEM((2, back_count, width, part), jnp.bfloat16),
            pltpu.VMEM((group_count, width, part), jnp.bfloat16),
            pltpu.VMEM((group_count, width, part), jnp.bfloat16),
            pltpu.VMEM((pair_count, width, part), jnp.bfloat16),
            pltpu.VMEM((2, pair_count, width, part), jnp.bfloat16),
            pltpu.VMEM((2, 2 * group_count, packed, total_cols), jnp.bfloat16),
            pltpu.VMEM((packed, total_cols), jnp.bfloat16),
            pltpu.VMEM((chips - 1, packed, total_cols), jnp.bfloat16),
            pltpu.VMEM((total_cols, part), jnp.float32),
            pltpu.VMEM((total_cols, part), jnp.float32),
            pltpu.VMEM((total_cols, total_cols), jnp.float32),
            pltpu.VMEM((8, owned * owner_count), jnp.int32),
            pltpu.SMEM((8, owned * owner_count), jnp.int32),
            dma, dma,
            dma, dma((2, owner_count // 2 - 1)), dma, dma((2,)), dma, dma,
            dma, dma((2,)), dma, dma((2,)), dma, dma, dma, dma((2,)), dma, dma,
        ],
        compiler_params=pltpu.CompilerParams(
            collective_id=0, has_side_effects=True, vmem_limit_bytes=60 * 1024 * 1024
        ),
    )(start_block, dual_shift[None, :], tile_rows[0, 0], tile_cols[0, 0], live_tiles[0], matrix)
    return pl.pallas_call(hand_on, out_shape=shapes, in_specs=[vmem] * 3, out_specs=(vmem,) * 3,
        compiler_params=pltpu.CompilerParams(vmem_limit_bytes=2 * 1024 * 1024))(*outs)


def solution(mesh):
    in_specs = (
        P("grp", "row", None, None, None),
        P("grp", "row", None),
        P("grp", "row", None),
        P("grp", "row"),
        P("row"),
        P(None, "row"),
    )
    out_specs = (P(), P(), P(None, "row"))
    return jax.shard_map(
        per_device, mesh=mesh, in_specs=in_specs, out_specs=out_specs, check_vma=False
    )
```

```python
import functools

import jax
import jax.numpy as jnp
from jax import lax
from jax.experimental import pallas as pl
from jax.experimental.pallas import tpu as pltpu
from jax.sharding import PartitionSpec as P

ITERS = 4
MESH = pl.DeviceIdType.MESH
HIGH = lax.Precision.HIGHEST
NT = (((1,), (1,)), ((), ()))
MIDDLE = 1.25
PANEL = 16
SIDE = 4
NEAR = 2


def dot_nt(a, b):
    return lax.dot_general(a, b, NT, precision=HIGH, preferred_element_type=jnp.float32)


def dot_nn(a, b):
    return jnp.dot(a, b, precision=HIGH, preferred_element_type=jnp.float32)


def factor_and_inverse(gram):
    n = gram.shape[0]
    row = lax.broadcasted_iota(jnp.int32, (n, n), 0)
    lane = lax.broadcasted_iota(jnp.int32, (n, n), 1)
    within = lax.broadcasted_iota(jnp.int32, (PANEL, 2 * n), 0)
    work = jnp.concatenate([gram, jnp.where(row == lane, 1.0, 0.0)], axis=1)
    blocks = []
    for start in range(0, n, PANEL):
        columns = [jnp.broadcast_to(work[:, k : k + 1], work.shape) for k in range(start, start + PANEL)]
        rows = [work[i : i + 1, :] for i in range(PANEL)]
        block = jnp.zeros((PANEL, 2 * n), jnp.float32)
        for i in range(0, PANEL, 2):
            first, second = columns[i], columns[i + 1]
            corner, cross, other = first[i : i + 1, :], first[i + 1 : i + 2, :], second[i + 1 : i + 2, :]
            det = corner * other - cross * cross
            scale, root = lax.rsqrt(corner), lax.rsqrt(det)
            left, right = root * scale * corner, root * scale * cross
            columns[i] = first * scale
            columns[i + 1] = second * left - first * right
            upper_row, lower_row = rows[i], rows[i + 1]
            rows[i] = upper_row * scale
            rows[i + 1] = lower_row * left - upper_row * right
            for later in range(i + 2, PANEL):
                for k in (i, i + 1):
                    weight = columns[k][later : later + 1, :]
                    columns[later] = columns[later] - columns[k] * weight
                    rows[later] = rows[later] - rows[k] * weight
            block = jnp.where(within == i, rows[i], block)
            block = jnp.where(within == i + 1, rows[i + 1], block)
        blocks.append(block)
        work = work[PANEL:]
        if start + PANEL < n:
            for i in range(PANEL):
                work = work - columns[i][PANEL:] * rows[i]
    whole = jnp.concatenate(blocks, axis=0)
    return jnp.where(lane >= row, whole[:, :n], 0.0), whole[:, n:]


def away(d, chips):
    return min(d % SIDE, SIDE - d % SIDE) + min(d // SIDE, chips // SIDE - d // SIDE)


def far_first(chips):
    return sorted(range(1, chips), key=lambda d: -away(d, chips))


def kernel(
    steps, group_count, owner_count,
    start_hbm, shift_hbm, rows_hbm, cols_hbm, live_ref, tiles_hbm,
    proj_ref, fac_ref, next_ref,
    start_ref, shift_ref, rows_ref, cols_ref, input_sem, tiles_ref, turned, masks, products, gathered, stage, history, own, own_history, back_out, back_in, direct_out, direct_in,
    pair_out, pair_in, dots_grp, chip_out, chip_in, basis, images, transform, place_vector, place_ref, tile_sem, place_sem,
    gather_send, gather_recv, relay_send, relay_recv, own_send, own_recv,
    pair_send, pair_recv, back_send, back_recv, direct_send, direct_recv, dots_send, dots_recv, chip_send, chip_recv,
):
    g = lax.axis_index("grp")
    r = lax.axis_index("row")
    width = start_ref.shape[0]
    row_count = start_ref.shape[1]
    part = row_count // group_count
    tile_count = tiles_ref.shape[0]
    owned = row_count // tiles_ref.shape[1]
    chips = owner_count // 2
    chip, core = r // 2, lax.rem(r, 2)
    partner = chip * 2 + 1 - core
    chip_x, chip_z = lax.rem(chip, SIDE), chip // SIDE

    offsets = far_first(chips)

    def chip_at(d, sign):
        z_count = chips // SIDE
        return lax.rem(chip_z + (sign * (d // SIDE)) % z_count, z_count) * SIDE + lax.rem(
            chip_x + (sign * (d % SIDE)) % SIDE, SIDE
        )

    far_count = sum(away(d, chips) > NEAR for d in offsets)
    sources = [chip_at(d, -1) for d in offsets]
    targets = [chip_at(d, 1) for d in offsets]
    grp_order = sorted(range(1, group_count), key=lambda d: -min(d, group_count - d))
    grp_peers = [lax.rem(g + d, group_count) for d in grp_order]
    total_cols = steps * width

    inputs = [
        pltpu.make_async_copy(src, dst, input_sem.at[i])
        for i, (src, dst) in enumerate(
            [(start_hbm, start_ref), (shift_hbm, shift_ref), (rows_hbm, rows_ref), (cols_hbm, cols_ref)]
        )
    ]
    for copy in inputs:
        copy.start()
    load = pltpu.make_async_copy(tiles_hbm, tiles_ref, tile_sem)
    load.start()
    barrier = pltpu.get_barrier_semaphore()
    for peer in targets:
        pl.semaphore_signal(barrier, inc=1, device_id=(g, peer * 2 + core), device_id_type=MESH)
    pl.semaphore_signal(barrier, inc=1, device_id=(g, partner), device_id_type=MESH)
    for peer in grp_peers:
        pl.semaphore_signal(barrier, inc=1, device_id=(peer, r), device_id_type=MESH)

    def to_row(peer, src, dst, send, recv):
        return pltpu.make_async_remote_copy(
            src_ref=src, dst_ref=dst, send_sem=send, recv_sem=recv,
            device_id=(g, peer), device_id_type=MESH,
        )

    def to_grp(peer, src, dst, send, recv):
        return pltpu.make_async_remote_copy(
            src_ref=src, dst_ref=dst, send_sem=send, recv_sem=recv,
            device_id=(peer, r), device_id_type=MESH,
        )

    others = group_count - 1

    def send_own(operand):
        own[g] = operand
        for peer in grp_peers:
            to_grp(peer, own.at[g], own.at[g], own_send, own_recv).start()

    def send_vectors(half, operand, own_too=True):
        gathered[half, r] = operand
        if own_too:
            send_own(operand)
        for i, peer in enumerate(targets):
            to_row(
                peer * 2 + core, gathered.at[half, r], gathered.at[half, r], gather_send, gather_recv.at[half, i]
            ).start()
        to_row(partner, gathered.at[half, r], gathered.at[half, r], gather_send, relay_recv.at[half]).start()
        stage[r] = operand

    def sent_own():
        bulk = own.at[pl.ds(0, others)]
        to_grp(grp_peers[0], bulk, bulk, own_send, own_send).wait_send()

    def sent_vectors():
        bulk = gathered.at[0, pl.ds(0, chips)]
        to_row(partner, bulk, bulk, gather_send, gather_send).wait_send()

    def take_own():
        bulk = own.at[pl.ds(0, others)]
        to_grp(grp_peers[0], bulk, bulk, own_recv, own_recv).wait_recv()

    def keep_own(step):
        for i in range(group_count):
            own_history[step * width : (step + 1) * width, i * part : (i + 1) * part] = own[i]

    def take_gathered(step, half):
        dots, batch = None, [r]
        for count, (i, peer) in enumerate(reversed(list(enumerate(sources)))):
            slot = peer * 2 + core
            block = gathered.at[half, slot]
            to_row(slot, block, block, gather_send, gather_recv.at[half, i]).wait_recv()
            to_row(partner, block, block, relay_send, relay_recv.at[half]).start()
            stage[slot] = gathered[half, slot]
            batch.append(slot)
            if count % 5 == 4:
                value = slot_dots(step, batch)
                dots = value if dots is None else dots + value
                batch = []
        return dots

    def relays_sent():
        bulk = gathered.at[0, pl.ds(0, chips - 1)]
        to_row(partner, bulk, bulk, relay_send, relay_send).wait_send()

    def take_relayed(half):
        bulk = gathered.at[half, pl.ds(0, chips)]
        to_row(partner, bulk, bulk, gather_send, relay_recv.at[half]).wait_recv()
        for peer in range(chips):
            slot = peer * 2 + 1 - core
            stage[slot] = gathered[half, slot]

    def pack(dots):
        pieces, done, count = [], 0, dots.shape[1]
        for size in (128, 64, 32):
            while count - done >= size:
                height = width * size // 128
                piece = dots[:, done : done + size]
                pieces.append(
                    jnp.concatenate([piece[i * height : (i + 1) * height] for i in range(width // height)], axis=1)
                )
                done += size
        return jnp.concatenate(pieces, axis=0)

    def unpack(packed, count):
        pieces, done, row = [], 0, 0
        for size in (128, 64, 32):
            while count - done >= size:
                height = width * size // 128
                piece = packed[row : row + height]
                pieces.append(
                    jnp.concatenate([piece[:, i * size : (i + 1) * size] for i in range(width // height)], axis=0)
                )
                done += size
                row += height
        return pieces

    def packed_rows(step):
        return pl.ds(0, 16 + (step + 1) // 2 * 16)

    def slot_dots(step, slots):
        dots = jnp.zeros((width, (step + 1) * width), jnp.float32)
        for slot in slots:
            vector = stage[slot]
            right = vector
            if step > 0:
                right = jnp.concatenate([vector, history[slot, : step * width, :]], axis=0)
            dots = dots + lax.dot_general(vector, right, NT, preferred_element_type=jnp.float32)
        return dots

    def encode(step, dots):
        gram, cross = dots
        high = gram.astype(jnp.bfloat16).astype(jnp.float32)
        pieces = [high, gram - high]
        if step > 0:
            pieces.append(cross)
        if step % 2 == 1:
            newest = cross[cross.shape[0] - 8 :]
            pieces.append(newest - newest.astype(jnp.bfloat16).astype(jnp.float32))
        return jnp.concatenate(pieces, axis=0).astype(jnp.bfloat16)

    def pack_both(step, dots):
        return pack(dots[:, :width]), pack(dots[:, width:]) if step > 0 else None

    def send_dots(step, half, dots):
        rows = packed_rows(step)
        me = g * 2 + core
        dots_grp[half, me, rows] = encode(step, dots)
        block = dots_grp.at[half, me, rows]
        for peer in grp_peers:
            to_grp(peer, block, block, dots_send, dots_recv.at[half]).start()
            pltpu.make_async_remote_copy(
                src_ref=block, dst_ref=block, send_sem=dots_send, recv_sem=dots_recv.at[half],
                device_id=(peer, partner), device_id_type=MESH,
            ).start()
        to_row(partner, block, block, dots_send, dots_recv.at[half]).start()

    def take_dots(step, half):
        rows = packed_rows(step)
        bulk = dots_grp.at[half, pl.ds(0, 2 * group_count - 1), rows]
        to_grp(grp_peers[0], bulk, bulk, dots_send, dots_recv.at[half]).wait_recv()
        summed = dots_grp[half, 0, rows].astype(jnp.float32)
        for index in range(1, 2 * group_count):
            summed = summed + dots_grp[half, index, rows].astype(jnp.float32)
        gram = unpack(summed[:8] + summed[8:16], width)[0]
        if step == 0:
            return None, gram
        old = summed[16 : 16 + step * 8]
        if step % 2 == 1:
            newest = old[step * 8 - 8 :] + summed[16 + step * 8 :]
            old = newest if step == 1 else jnp.concatenate([old[: step * 8 - 8], newest], axis=0)
        pieces = unpack(old, step * width)
        whole = jnp.concatenate(pieces, axis=1) if len(pieces) > 1 else pieces[0]
        cross = dot_nt(whole, transform[:, : step * width])
        return cross, gram - dot_nt(cross, cross)

    def dots_sent(step, half):
        bulk = dots_grp.at[half, pl.ds(0, 2 * group_count - 1), packed_rows(step)]
        to_grp(grp_peers[0], bulk, bulk, dots_send, dots_recv.at[half]).wait_send()

    def back_product(slot):
        value = products[place_ref[0, slot]]
        for i in range(1, owned):
            value = value + products[place_ref[0, i * owner_count + slot]]
        return value

    def take_pair(peer, half):
        return pair_in[half, peer].astype(jnp.float32)

    mine = pl.ds(pl.multiple_of(g * part, part), part)
    for copy in inputs:
        copy.wait()
    current = start_ref[:, mine]
    shift = shift_ref[:, mine]
    pl.semaphore_wait(barrier, chips + others)
    send_vectors(0, current.astype(jnp.bfloat16), own_too=False)
    for i in range(group_count):
        own[i] = start_ref[:, i * part : (i + 1) * part].astype(jnp.bfloat16)
    lanes = lax.broadcasted_iota(jnp.int32, place_vector.shape, 1)
    place = jnp.full(place_vector.shape, tile_count, jnp.int32)
    for k in range(tile_count):
        alive = k < live_ref[0]
        position = jnp.where(alive, rows_ref[k] * owner_count + cols_ref[k], -1)
        place = jnp.where(lanes == position, k, place)
        row = jnp.full((8, 128), jnp.where(alive, rows_ref[k], -1), jnp.int32)
        for i in range(owned):
            masks[k, i] = jnp.where(row == i, 1.0, 0.0)
    place_vector[...] = place
    place_copy = pltpu.make_async_copy(place_vector, place_ref, place_sem)
    place_copy.start()
    basis[...] = jnp.zeros_like(basis)
    images[...] = jnp.zeros_like(images)
    transform[...] = jnp.zeros_like(transform)
    products[tile_count] = jnp.zeros((width, part), jnp.float32)
    load.wait()
    place_copy.wait()

    def turn(j, carry):
        for i in range(4):
            turned[j * 4 + i] = tiles_ref[j * 4 + i].T
        return carry

    coef, middle = None, MIDDLE
    lane = lax.broadcasted_iota(jnp.int32, (width, total_cols), 1)
    sub = lax.broadcasted_iota(jnp.int32, (width, total_cols), 0)
    for step in range(steps):
        half = step % 2
        far = far_count if step > 0 else 0
        near_rows = pl.ds(0, chips - far)
        if step > 0:
            take_own()
        for k in range(tile_count):
            products[k] = jnp.dot(own[rows_ref[k]], tiles_ref[k], preferred_element_type=jnp.float32)
        for i, peer in enumerate(targets[far:] + [chip]):
            pair_out[i] = back_product(peer * 2 + 1 - core).astype(jnp.bfloat16)
            to_row(partner, pair_out.at[i], pair_in.at[half, i], pair_send, pair_recv.at[half]).start()
        for i, peer in enumerate(targets[:far]):
            for side, slot in enumerate([peer * 2 + core, peer * 2 + 1 - core]):
                index = 2 * i + side
                back_out[index] = back_product(slot).astype(jnp.bfloat16)
                to_row(
                    slot, back_out.at[index], back_in.at[half, index], back_send, back_recv.at[half]
                ).start()
        keep_own(step)
        if step == 0:
            lax.fori_loop(0, tile_count // 4, turn, 0)
        def send_back():
            to_row(
                partner, pair_out.at[near_rows], pair_in.at[half, near_rows], pair_send, pair_recv.at[half]
            ).wait_recv()
            for i, peer in enumerate(targets[far:]):
                index = 2 * far + i
                back_out[index] = (back_product(peer * 2 + core) + take_pair(i, half)).astype(jnp.bfloat16)
                to_row(
                    peer * 2 + core, back_out.at[index], back_in.at[half, index], back_send, back_recv.at[half]
                ).start()
            total = back_product(r) + take_pair(len(targets) - far, half)
            return total

        if step == 0:
            total = send_back()
        dots = take_gathered(step, half)
        send_dots(step, half, pack_both(step, dots))
        if step > 0:
            total = send_back()
        take_relayed(half)
        forward = [jnp.zeros((width, part), jnp.float32)] * owned
        for k in range(tile_count):
            value = jnp.dot(stage[cols_ref[k]], turned[k], preferred_element_type=jnp.float32)
            for i in range(owned):
                mask = jnp.concatenate([masks[k, i]] * (part // 128), axis=1)
                forward[i] = forward[i] + value * jnp.concatenate([mask] * (width // 8), axis=0)
        for i in range(owned):
            direct_out[i] = forward[i].astype(jnp.bfloat16)
        for peer in grp_peers:
            to_grp(peer, direct_out.at[peer], direct_in.at[g], direct_send, direct_recv).start()
        for i in range(owned):
            total = total + forward[i] * jnp.where(g == i, 1.0, 0.0)
        for slot in range(owner_count):
            history[slot, step * width : (step + 1) * width, :] = stage[slot]
        sent_vectors()
        if step > 0:
            sent_own()
        relays_sent()
        cross, gram = take_dots(step, half)
        left, rest = current, None
        if step > 0:
            left = left - dot_nn(cross, basis[...])
            rest = dot_nn(cross, images[...])
            first = cross + coef
            newest = jnp.where(lane == (step - 1) * width + sub, first, 0.0)
            middle = -jnp.sum(newest, axis=(0, 1), keepdims=True) / width
        upper, inverse = factor_and_inverse(gram)
        now = dot_nn(inverse, left)
        ahead = now * (middle - shift)
        if step > 0:
            ahead = ahead - dot_nn(upper, basis[(step - 1) * width : step * width, :])
        bulk = back_in.at[half, pl.ds(0, chips - 1 + far)]
        to_row(partner, bulk, bulk, back_send, back_recv.at[half]).wait_recv()
        for index in range(chips - 1 + far):
            total = total + back_in[half, index].astype(jnp.float32)
        bulk = direct_in.at[pl.ds(0, others)]
        to_grp(grp_peers[0], bulk, bulk, direct_send, direct_recv).wait_recv()
        for peer in grp_peers:
            total = total + direct_in[peer].astype(jnp.float32)
        total = 0.5 * total
        if step > 0:
            total = total - rest
        image = dot_nn(inverse, total)
        current = image + ahead
        if step < steps - 1:
            send_vectors(1 - half, current.astype(jnp.bfloat16))
        else:
            send_own(current.astype(jnp.bfloat16))
            stage[r] = current.astype(jnp.bfloat16)
            local = pack_both(steps, slot_dots(steps, [r]))
            chip_out[...] = encode(steps, local)
            for i, peer in enumerate(targets):
                to_row(peer * 2 + core, chip_out, chip_in.at[i], chip_send, chip_recv).start()
        basis[step * width : (step + 1) * width, :] = now
        images[step * width : (step + 1) * width, :] = image
        if step > 0:
            proj_ref[step - 1] = first
            fac_ref[step - 1] = upper.T
        unit = jnp.where(lane == step * width + sub, 1.0, 0.0)
        if step == 0:
            transform[:width, :] = dot_nn(inverse, unit)
            coef = -MIDDLE * unit
        else:
            transform[step * width : (step + 1) * width, :] = dot_nn(inverse, unit - dot_nn(cross, transform[...]))
            wide = jnp.concatenate([upper] * (total_cols // width), axis=1)
            coef = -middle * unit + jnp.where((lane >= (step - 1) * width) & (lane < step * width), wide, 0.0)
        bulk = pair_out.at[near_rows]
        to_row(partner, bulk, bulk, pair_send, pair_recv.at[half]).wait_send()
        bulk = back_out.at[pl.ds(0, chips - 1 + far)]
        to_row(partner, bulk, bulk, back_send, back_recv.at[half]).wait_send()
        bulk = direct_out.at[pl.ds(0, others)]
        to_grp(grp_peers[0], bulk, bulk, direct_send, direct_recv).wait_send()
        dots_sent(step, half)

    half = steps % 2
    take_own()
    keep_own(steps)
    sent_own()
    to_row(partner, chip_in, chip_in, chip_send, chip_recv).wait_recv()
    summed = chip_in[0].astype(jnp.float32)
    for i in range(1, chips - 1):
        summed = summed + chip_in[i].astype(jnp.float32)
    send_dots(steps, half, (local[0] + summed[:8] + summed[8:16], local[1] + summed[16:]))
    to_row(partner, chip_in, chip_in, chip_send, chip_recv).wait_send()
    cross, gram = take_dots(steps, half)
    combine = dot_nn(cross, transform[...])
    high = combine.astype(jnp.bfloat16)
    low = (combine - high.astype(jnp.float32)).astype(jnp.bfloat16)
    both = jnp.dot(
        jnp.concatenate([high, low], axis=0), own_history[:total_cols, :], preferred_element_type=jnp.float32
    )
    left = own_history[total_cols:, :].astype(jnp.float32) - both[:width] - both[width:]
    upper, inverse = factor_and_inverse(gram)
    proj_ref[steps - 1] = cross + coef
    fac_ref[steps - 1] = upper.T
    next_ref[...] = dot_nn(inverse, left)
    dots_sent(steps, half)


def hand_on(proj_in, fac_in, next_in, proj_ref, fac_ref, next_ref):
    proj_ref[...] = proj_in[...]
    fac_ref[...] = fac_in[...]
    next_ref[...] = next_in[...]


def per_device(tiles, tile_rows, tile_cols, live_tiles, dual_shift, start_block):
    matrix = tiles[0, 0]
    tile_count, edge = matrix.shape[0], matrix.shape[1]
    width, row_count = start_block.shape
    group_count = lax.axis_size("grp")
    owner_count = lax.axis_size("row")
    owned = row_count // edge
    part = row_count // group_count
    total_cols = ITERS * width
    vmem = pl.BlockSpec(memory_space=pltpu.VMEM)
    smem = pl.BlockSpec(memory_space=pltpu.SMEM)
    hbm = pl.BlockSpec(memory_space=pltpu.HBM)
    dma = pltpu.SemaphoreType.DMA
    chips = owner_count // 2
    far = sum(away(d, chips) > NEAR for d in far_first(chips))
    back_count = chips - 1 + far
    pair_count = chips
    packed = 16 + (ITERS + 1) // 2 * 16
    shapes = (
            jax.ShapeDtypeStruct((ITERS, width, total_cols), jnp.float32),
            jax.ShapeDtypeStruct((ITERS, width, width), jnp.float32),
            jax.ShapeDtypeStruct((width, row_count), jnp.float32),
    )
    outs = pl.pallas_call(
        functools.partial(kernel, ITERS, group_count, owner_count),
        out_shape=tuple(pltpu.VMEM(x.shape, x.dtype) for x in shapes),
        in_specs=[hbm, hbm, hbm, hbm, smem, hbm],
        out_specs=(vmem, vmem, vmem),
        scratch_shapes=[
            pltpu.VMEM((width, row_count), jnp.float32),
            pltpu.VMEM((1, row_count), jnp.float32),
            pltpu.SMEM((tile_count,), jnp.int32),
            pltpu.SMEM((tile_count,), jnp.int32),
            dma((4,)),
            pltpu.VMEM(matrix.shape, jnp.bfloat16),
            pltpu.VMEM(matrix.shape, jnp.bfloat16),
            pltpu.VMEM((tile_count, owned, 8, 128), jnp.float32),
            pltpu.VMEM((tile_count + 1, width, part), jnp.float32),
            pltpu.VMEM((2, owner_count, width, part), jnp.bfloat16),
            pltpu.VMEM((owner_count, width, part), jnp.bfloat16),
            pltpu.VMEM((owner_count, total_cols, part), jnp.bfloat16),
            pltpu.VMEM((group_count, width, part), jnp.bfloat16),
            pltpu.VMEM((total_cols + width, row_count), jnp.bfloat16),
            pltpu.VMEM((back_count, width, part), jnp.bfloat16),
            pltpu.VMEM((2, back_count, width, part), jnp.bfloat16),
            pltpu.VMEM((group_count, width, part), jnp.bfloat16),
            pltpu.VMEM((group_count, width, part), jnp.bfloat16),
            pltpu.VMEM((pair_count, width, part), jnp.bfloat16),
            pltpu.VMEM((2, pair_count, width, part), jnp.bfloat16),
            pltpu.VMEM((2, 2 * group_count, packed, total_cols), jnp.bfloat16),
            pltpu.VMEM((packed, total_cols), jnp.bfloat16),
            pltpu.VMEM((chips - 1, packed, total_cols), jnp.bfloat16),
            pltpu.VMEM((total_cols, part), jnp.float32),
            pltpu.VMEM((total_cols, part), jnp.float32),
            pltpu.VMEM((total_cols, total_cols), jnp.float32),
            pltpu.VMEM((8, owned * owner_count), jnp.int32),
            pltpu.SMEM((8, owned * owner_count), jnp.int32),
            dma, dma,
            dma, dma((2, owner_count // 2 - 1)), dma, dma((2,)), dma, dma,
            dma, dma((2,)), dma, dma((2,)), dma, dma, dma, dma((2,)), dma, dma,
        ],
        compiler_params=pltpu.CompilerParams(
            collective_id=0, has_side_effects=True, vmem_limit_bytes=60 * 1024 * 1024
        ),
    )(start_block, dual_shift[None, :], tile_rows[0, 0], tile_cols[0, 0], live_tiles[0], matrix)
    return pl.pallas_call(hand_on, out_shape=shapes, in_specs=[vmem] * 3, out_specs=(vmem,) * 3,
        compiler_params=pltpu.CompilerParams(vmem_limit_bytes=2 * 1024 * 1024))(*outs)


def solution(mesh):
    in_specs = (
        P("grp", "row", None, None, None),
        P("grp", "row", None),
        P("grp", "row", None),
        P("grp", "row"),
        P("row"),
        P(None, "row"),
    )
    out_specs = (P(), P(), P(None, "row"))
    return jax.shard_map(
        per_device, mesh=mesh, in_specs=in_specs, out_specs=out_specs, check_vma=False
    )
```

```python
import functools

import jax
import jax.numpy as jnp
from jax import lax
from jax.experimental import pallas as pl
from jax.experimental.pallas import tpu as pltpu
from jax.sharding import PartitionSpec as P

ITERS = 4
MESH = pl.DeviceIdType.MESH
HIGH = lax.Precision.HIGHEST
NT = (((1,), (1,)), ((), ()))
MIDDLE = 1.25
PANEL = 16
SIDE = 4
NEAR = 2


def dot_nt(a, b):
    return lax.dot_general(a, b, NT, precision=HIGH, preferred_element_type=jnp.float32)


def dot_nn(a, b):
    return jnp.dot(a, b, precision=HIGH, preferred_element_type=jnp.float32)


def factor_and_inverse(gram):
    n = gram.shape[0]
    row = lax.broadcasted_iota(jnp.int32, (n, n), 0)
    lane = lax.broadcasted_iota(jnp.int32, (n, n), 1)
    within = lax.broadcasted_iota(jnp.int32, (PANEL, 2 * n), 0)
    work = jnp.concatenate([gram, jnp.where(row == lane, 1.0, 0.0)], axis=1)
    blocks = []
    for start in range(0, n, PANEL):
        columns = [jnp.broadcast_to(work[:, k : k + 1], work.shape) for k in range(start, start + PANEL)]
        rows = [work[i : i + 1, :] for i in range(PANEL)]
        block = jnp.zeros((PANEL, 2 * n), jnp.float32)
        for i in range(0, PANEL, 2):
            first, second = columns[i], columns[i + 1]
            corner, cross, other = first[i : i + 1, :], first[i + 1 : i + 2, :], second[i + 1 : i + 2, :]
            det = corner * other - cross * cross
            scale, root = lax.rsqrt(corner), lax.rsqrt(det)
            left, right = root * scale * corner, root * scale * cross
            columns[i] = first * scale
            columns[i + 1] = second * left - first * right
            upper_row, lower_row = rows[i], rows[i + 1]
            rows[i] = upper_row * scale
            rows[i + 1] = lower_row * left - upper_row * right
            for later in range(i + 2, PANEL):
                for k in (i, i + 1):
                    weight = columns[k][later : later + 1, :]
                    columns[later] = columns[later] - columns[k] * weight
                    rows[later] = rows[later] - rows[k] * weight
            block = jnp.where(within == i, rows[i], block)
            block = jnp.where(within == i + 1, rows[i + 1], block)
        blocks.append(block)
        work = work[PANEL:]
        if start + PANEL < n:
            for i in range(PANEL):
                work = work - columns[i][PANEL:] * rows[i]
    whole = jnp.concatenate(blocks, axis=0)
    return jnp.where(lane >= row, whole[:, :n], 0.0), whole[:, n:]


def away(d, chips):
    return min(d % SIDE, SIDE - d % SIDE) + min(d // SIDE, chips // SIDE - d // SIDE)


def far_first(chips):
    return sorted(range(1, chips), key=lambda d: (-away(d, chips), -min(d // SIDE, 4 - d // SIDE)))


def kernel(
    steps, group_count, owner_count,
    start_hbm, shift_hbm, rows_hbm, cols_hbm, live_ref, tiles_hbm,
    proj_ref, fac_ref, next_ref,
    start_ref, shift_ref, rows_ref, cols_ref, input_sem, tiles_ref, turned, masks, products, gathered, stage, history, own, own_history, back_out, back_in, direct_out, direct_in,
    pair_out, pair_in, dots_grp, chip_out, chip_in, basis, images, transform, place_vector, place_ref, tile_sem, place_sem,
    gather_send, gather_recv, relay_send, relay_recv, own_send, own_recv,
    pair_send, pair_recv, back_send, back_recv, direct_send, direct_recv, dots_send, dots_recv, chip_send, chip_recv,
):
    g = lax.axis_index("grp")
    r = lax.axis_index("row")
    width = start_ref.shape[0]
    row_count = start_ref.shape[1]
    part = row_count // group_count
    tile_count = tiles_ref.shape[0]
    owned = row_count // tiles_ref.shape[1]
    chips = owner_count // 2
    chip, core = r // 2, lax.rem(r, 2)
    partner = chip * 2 + 1 - core
    chip_x, chip_z = lax.rem(chip, SIDE), chip // SIDE

    offsets = far_first(chips)

    def chip_at(d, sign):
        z_count = chips // SIDE
        return lax.rem(chip_z + (sign * (d // SIDE)) % z_count, z_count) * SIDE + lax.rem(
            chip_x + (sign * (d % SIDE)) % SIDE, SIDE
        )

    far_count = sum(away(d, chips) > NEAR for d in offsets)
    sources = [chip_at(d, -1) for d in offsets]
    targets = [chip_at(d, 1) for d in offsets]
    grp_order = sorted(range(1, group_count), key=lambda d: -min(d, group_count - d))
    grp_peers = [lax.rem(g + d, group_count) for d in grp_order]
    total_cols = steps * width

    inputs = [
        pltpu.make_async_copy(src, dst, input_sem.at[i])
        for i, (src, dst) in enumerate(
            [(start_hbm, start_ref), (shift_hbm, shift_ref), (rows_hbm, rows_ref), (cols_hbm, cols_ref)]
        )
    ]
    for copy in inputs:
        copy.start()
    load = pltpu.make_async_copy(tiles_hbm, tiles_ref, tile_sem)
    load.start()
    barrier = pltpu.get_barrier_semaphore()
    for peer in targets:
        pl.semaphore_signal(barrier, inc=1, device_id=(g, peer * 2 + core), device_id_type=MESH)
    pl.semaphore_signal(barrier, inc=1, device_id=(g, partner), device_id_type=MESH)
    for peer in grp_peers:
        pl.semaphore_signal(barrier, inc=1, device_id=(peer, r), device_id_type=MESH)

    def to_row(peer, src, dst, send, recv):
        return pltpu.make_async_remote_copy(
            src_ref=src, dst_ref=dst, send_sem=send, recv_sem=recv,
            device_id=(g, peer), device_id_type=MESH,
        )

    def to_grp(peer, src, dst, send, recv):
        return pltpu.make_async_remote_copy(
            src_ref=src, dst_ref=dst, send_sem=send, recv_sem=recv,
            device_id=(peer, r), device_id_type=MESH,
        )

    others = group_count - 1

    def send_own(operand):
        own[g] = operand
        for peer in grp_peers:
            to_grp(peer, own.at[g], own.at[g], own_send, own_recv).start()

    def send_vectors(half, operand, own_too=True):
        gathered[half, r] = operand
        if own_too:
            send_own(operand)
        for i, peer in enumerate(targets):
            to_row(
                peer * 2 + core, gathered.at[half, r], gathered.at[half, r], gather_send, gather_recv.at[half, i]
            ).start()
        to_row(partner, gathered.at[half, r], gathered.at[half, r], gather_send, relay_recv.at[half]).start()
        stage[r] = operand

    def sent_own():
        bulk = own.at[pl.ds(0, others)]
        to_grp(grp_peers[0], bulk, bulk, own_send, own_send).wait_send()

    def sent_vectors():
        bulk = gathered.at[0, pl.ds(0, chips)]
        to_row(partner, bulk, bulk, gather_send, gather_send).wait_send()

    def take_own():
        bulk = own.at[pl.ds(0, others)]
        to_grp(grp_peers[0], bulk, bulk, own_recv, own_recv).wait_recv()

    def keep_own(step):
        for i in range(group_count):
            own_history[step * width : (step + 1) * width, i * part : (i + 1) * part] = own[i]

    def take_gathered(step, half):
        dots, batch = None, [r]
        for count, (i, peer) in enumerate(list(enumerate(sources))):
            slot = peer * 2 + core
            block = gathered.at[half, slot]
            to_row(slot, block, block, gather_send, gather_recv.at[half, i]).wait_recv()
            to_row(partner, block, block, relay_send, relay_recv.at[half]).start()
            stage[slot] = gathered[half, slot]
            batch.append(slot)
            if count % 5 == 4:
                value = slot_dots(step, batch)
                dots = value if dots is None else dots + value
                batch = []
        return dots

    def relays_sent():
        bulk = gathered.at[0, pl.ds(0, chips - 1)]
        to_row(partner, bulk, bulk, relay_send, relay_send).wait_send()

    def take_relayed(half):
        bulk = gathered.at[half, pl.ds(0, chips)]
        to_row(partner, bulk, bulk, gather_send, relay_recv.at[half]).wait_recv()
        for peer in range(chips):
            slot = peer * 2 + 1 - core
            stage[slot] = gathered[half, slot]

    def pack(dots):
        pieces, done, count = [], 0, dots.shape[1]
        for size in (128, 64, 32):
            while count - done >= size:
                height = width * size // 128
                piece = dots[:, done : done + size]
                pieces.append(
                    jnp.concatenate([piece[i * height : (i + 1) * height] for i in range(width // height)], axis=1)
                )
                done += size
        return jnp.concatenate(pieces, axis=0)

    def unpack(packed, count):
        pieces, done, row = [], 0, 0
        for size in (128, 64, 32):
            while count - done >= size:
                height = width * size // 128
                piece = packed[row : row + height]
                pieces.append(
                    jnp.concatenate([piece[:, i * size : (i + 1) * size] for i in range(width // height)], axis=0)
                )
                done += size
                row += height
        return pieces

    def packed_rows(step):
        return pl.ds(0, 16 + (step + 1) // 2 * 16)

    def slot_dots(step, slots):
        dots = jnp.zeros((width, (step + 1) * width), jnp.float32)
        for slot in slots:
            vector = stage[slot]
            right = vector
            if step > 0:
                right = jnp.concatenate([vector, history[slot, : step * width, :]], axis=0)
            dots = dots + lax.dot_general(vector, right, NT, preferred_element_type=jnp.float32)
        return dots

    def encode(step, dots):
        gram, cross = dots
        high = gram.astype(jnp.bfloat16).astype(jnp.float32)
        pieces = [high, gram - high]
        if step > 0:
            pieces.append(cross)
        if step % 2 == 1:
            newest = cross[cross.shape[0] - 8 :]
            pieces.append(newest - newest.astype(jnp.bfloat16).astype(jnp.float32))
        return jnp.concatenate(pieces, axis=0).astype(jnp.bfloat16)

    def pack_both(step, dots):
        return pack(dots[:, :width]), pack(dots[:, width:]) if step > 0 else None

    def send_dots(step, half, dots):
        rows = packed_rows(step)
        me = g * 2 + core
        dots_grp[half, me, rows] = encode(step, dots)
        block = dots_grp.at[half, me, rows]
        for peer in grp_peers:
            to_grp(peer, block, block, dots_send, dots_recv.at[half]).start()
            pltpu.make_async_remote_copy(
                src_ref=block, dst_ref=block, send_sem=dots_send, recv_sem=dots_recv.at[half],
                device_id=(peer, partner), device_id_type=MESH,
            ).start()
        to_row(partner, block, block, dots_send, dots_recv.at[half]).start()

    def take_dots(step, half):
        rows = packed_rows(step)
        bulk = dots_grp.at[half, pl.ds(0, 2 * group_count - 1), rows]
        to_grp(grp_peers[0], bulk, bulk, dots_send, dots_recv.at[half]).wait_recv()
        summed = dots_grp[half, 0, rows].astype(jnp.float32)
        for index in range(1, 2 * group_count):
            summed = summed + dots_grp[half, index, rows].astype(jnp.float32)
        gram = unpack(summed[:8] + summed[8:16], width)[0]
        if step == 0:
            return None, gram
        old = summed[16 : 16 + step * 8]
        if step % 2 == 1:
            newest = old[step * 8 - 8 :] + summed[16 + step * 8 :]
            old = newest if step == 1 else jnp.concatenate([old[: step * 8 - 8], newest], axis=0)
        pieces = unpack(old, step * width)
        whole = jnp.concatenate(pieces, axis=1) if len(pieces) > 1 else pieces[0]
        cross = dot_nt(whole, transform[:, : step * width])
        return cross, gram - dot_nt(cross, cross)

    def dots_sent(step, half):
        bulk = dots_grp.at[half, pl.ds(0, 2 * group_count - 1), packed_rows(step)]
        to_grp(grp_peers[0], bulk, bulk, dots_send, dots_recv.at[half]).wait_send()

    def back_product(slot):
        value = products[place_ref[0, slot]]
        for i in range(1, owned):
            value = value + products[place_ref[0, i * owner_count + slot]]
        return value

    def take_pair(peer, half):
        return pair_in[half, peer].astype(jnp.float32)

    mine = pl.ds(pl.multiple_of(g * part, part), part)
    for copy in inputs:
        copy.wait()
    current = start_ref[:, mine]
    shift = shift_ref[:, mine]
    pl.semaphore_wait(barrier, chips + others)
    send_vectors(0, current.astype(jnp.bfloat16), own_too=False)
    for i in range(group_count):
        own[i] = start_ref[:, i * part : (i + 1) * part].astype(jnp.bfloat16)
    lanes = lax.broadcasted_iota(jnp.int32, place_vector.shape, 1)
    place = jnp.full(place_vector.shape, tile_count, jnp.int32)
    for k in range(tile_count):
        alive = k < live_ref[0]
        position = jnp.where(alive, rows_ref[k] * owner_count + cols_ref[k], -1)
        place = jnp.where(lanes == position, k, place)
        row = jnp.full((8, 128), jnp.where(alive, rows_ref[k], -1), jnp.int32)
        for i in range(owned):
            masks[k, i] = jnp.where(row == i, 1.0, 0.0)
    place_vector[...] = place
    place_copy = pltpu.make_async_copy(place_vector, place_ref, place_sem)
    place_copy.start()
    basis[...] = jnp.zeros_like(basis)
    images[...] = jnp.zeros_like(images)
    transform[...] = jnp.zeros_like(transform)
    products[tile_count] = jnp.zeros((width, part), jnp.float32)
    load.wait()
    place_copy.wait()

    def turn(j, carry):
        for i in range(4):
            turned[j * 4 + i] = tiles_ref[j * 4 + i].T
        return carry

    coef, middle = None, MIDDLE
    lane = lax.broadcasted_iota(jnp.int32, (width, total_cols), 1)
    sub = lax.broadcasted_iota(jnp.int32, (width, total_cols), 0)
    for step in range(steps):
        half = step % 2
        far = far_count if step > 0 else 0
        near_rows = pl.ds(0, chips - far)
        if step > 0:
            take_own()
        for k in range(tile_count):
            products[k] = jnp.dot(own[rows_ref[k]], tiles_ref[k], preferred_element_type=jnp.float32)
        for i, peer in enumerate(targets[far:] + [chip]):
            pair_out[i] = back_product(peer * 2 + 1 - core).astype(jnp.bfloat16)
            to_row(partner, pair_out.at[i], pair_in.at[half, i], pair_send, pair_recv.at[half]).start()
        for i, peer in enumerate(targets[:far]):
            for side, slot in enumerate([peer * 2 + core, peer * 2 + 1 - core]):
                index = 2 * i + side
                back_out[index] = back_product(slot).astype(jnp.bfloat16)
                to_row(
                    slot, back_out.at[index], back_in.at[half, index], back_send, back_recv.at[half]
                ).start()
        keep_own(step)
        if step == 0:
            lax.fori_loop(0, tile_count // 4, turn, 0)
        def send_back():
            to_row(
                partner, pair_out.at[near_rows], pair_in.at[half, near_rows], pair_send, pair_recv.at[half]
            ).wait_recv()
            for i, peer in enumerate(targets[far:]):
                index = 2 * far + i
                back_out[index] = (back_product(peer * 2 + core) + take_pair(i, half)).astype(jnp.bfloat16)
                to_row(
                    peer * 2 + core, back_out.at[index], back_in.at[half, index], back_send, back_recv.at[half]
                ).start()
            total = back_product(r) + take_pair(len(targets) - far, half)
            return total

        if step == 0:
            total = send_back()
        dots = take_gathered(step, half)
        send_dots(step, half, pack_both(step, dots))
        if step > 0:
            total = send_back()
        take_relayed(half)
        forward = [jnp.zeros((width, part), jnp.float32)] * owned
        for k in range(tile_count):
            value = jnp.dot(stage[cols_ref[k]], turned[k], preferred_element_type=jnp.float32)
            for i in range(owned):
                mask = jnp.concatenate([masks[k, i]] * (part // 128), axis=1)
                forward[i] = forward[i] + value * jnp.concatenate([mask] * (width // 8), axis=0)
        for i in range(owned):
            direct_out[i] = forward[i].astype(jnp.bfloat16)
        for peer in grp_peers:
            to_grp(peer, direct_out.at[peer], direct_in.at[g], direct_send, direct_recv).start()
        for i in range(owned):
            total = total + forward[i] * jnp.where(g == i, 1.0, 0.0)
        for slot in range(owner_count):
            history[slot, step * width : (step + 1) * width, :] = stage[slot]
        sent_vectors()
        if step > 0:
            sent_own()
        relays_sent()
        cross, gram = take_dots(step, half)
        left, rest = current, None
        if step > 0:
            left = left - dot_nn(cross, basis[...])
            rest = dot_nn(cross, images[...])
            first = cross + coef
            newest = jnp.where(lane == (step - 1) * width + sub, first, 0.0)
            middle = -jnp.sum(newest, axis=(0, 1), keepdims=True) / width
        upper, inverse = factor_and_inverse(gram)
        now = dot_nn(inverse, left)
        ahead = now * (middle - shift)
        if step > 0:
            ahead = ahead - dot_nn(upper, basis[(step - 1) * width : step * width, :])
        bulk = back_in.at[half, pl.ds(0, chips - 1 + far)]
        to_row(partner, bulk, bulk, back_send, back_recv.at[half]).wait_recv()
        for index in range(chips - 1 + far):
            total = total + back_in[half, index].astype(jnp.float32)
        bulk = direct_in.at[pl.ds(0, others)]
        to_grp(grp_peers[0], bulk, bulk, direct_send, direct_recv).wait_recv()
        for peer in grp_peers:
            total = total + direct_in[peer].astype(jnp.float32)
        total = 0.5 * total
        if step > 0:
            total = total - rest
        image = dot_nn(inverse, total)
        current = image + ahead
        if step < steps - 1:
            send_vectors(1 - half, current.astype(jnp.bfloat16))
        else:
            send_own(current.astype(jnp.bfloat16))
            stage[r] = current.astype(jnp.bfloat16)
            local = pack_both(steps, slot_dots(steps, [r]))
            chip_out[...] = encode(steps, local)
            for i, peer in enumerate(targets):
                to_row(peer * 2 + core, chip_out, chip_in.at[i], chip_send, chip_recv).start()
        basis[step * width : (step + 1) * width, :] = now
        images[step * width : (step + 1) * width, :] = image
        if step > 0:
            proj_ref[step - 1] = first
            fac_ref[step - 1] = upper.T
        unit = jnp.where(lane == step * width + sub, 1.0, 0.0)
        if step == 0:
            transform[:width, :] = dot_nn(inverse, unit)
            coef = -MIDDLE * unit
        else:
            transform[step * width : (step + 1) * width, :] = dot_nn(inverse, unit - dot_nn(cross, transform[...]))
            wide = jnp.concatenate([upper] * (total_cols // width), axis=1)
            coef = -middle * unit + jnp.where((lane >= (step - 1) * width) & (lane < step * width), wide, 0.0)
        bulk = pair_out.at[near_rows]
        to_row(partner, bulk, bulk, pair_send, pair_recv.at[half]).wait_send()
        bulk = back_out.at[pl.ds(0, chips - 1 + far)]
        to_row(partner, bulk, bulk, back_send, back_recv.at[half]).wait_send()
        bulk = direct_out.at[pl.ds(0, others)]
        to_grp(grp_peers[0], bulk, bulk, direct_send, direct_recv).wait_send()
        dots_sent(step, half)

    half = steps % 2
    take_own()
    keep_own(steps)
    sent_own()
    to_row(partner, chip_in, chip_in, chip_send, chip_recv).wait_recv()
    summed = chip_in[0].astype(jnp.float32)
    for i in range(1, chips - 1):
        summed = summed + chip_in[i].astype(jnp.float32)
    send_dots(steps, half, (local[0] + summed[:8] + summed[8:16], local[1] + summed[16:]))
    to_row(partner, chip_in, chip_in, chip_send, chip_recv).wait_send()
    cross, gram = take_dots(steps, half)
    combine = dot_nn(cross, transform[...])
    high = combine.astype(jnp.bfloat16)
    low = (combine - high.astype(jnp.float32)).astype(jnp.bfloat16)
    both = jnp.dot(
        jnp.concatenate([high, low], axis=0), own_history[:total_cols, :], preferred_element_type=jnp.float32
    )
    left = own_history[total_cols:, :].astype(jnp.float32) - both[:width] - both[width:]
    upper, inverse = factor_and_inverse(gram)
    proj_ref[steps - 1] = cross + coef
    fac_ref[steps - 1] = upper.T
    next_ref[...] = dot_nn(inverse, left)
    dots_sent(steps, half)


def hand_on(proj_in, fac_in, next_in, proj_ref, fac_ref, next_ref):
    proj_ref[...] = proj_in[...]
    fac_ref[...] = fac_in[...]
    next_ref[...] = next_in[...]


def per_device(tiles, tile_rows, tile_cols, live_tiles, dual_shift, start_block):
    matrix = tiles[0, 0]
    tile_count, edge = matrix.shape[0], matrix.shape[1]
    width, row_count = start_block.shape
    group_count = lax.axis_size("grp")
    owner_count = lax.axis_size("row")
    owned = row_count // edge
    part = row_count // group_count
    total_cols = ITERS * width
    vmem = pl.BlockSpec(memory_space=pltpu.VMEM)
    smem = pl.BlockSpec(memory_space=pltpu.SMEM)
    hbm = pl.BlockSpec(memory_space=pltpu.HBM)
    dma = pltpu.SemaphoreType.DMA
    chips = owner_count // 2
    far = sum(away(d, chips) > NEAR for d in far_first(chips))
    back_count = chips - 1 + far
    pair_count = chips
    packed = 16 + (ITERS + 1) // 2 * 16
    shapes = (
            jax.ShapeDtypeStruct((ITERS, width, total_cols), jnp.float32),
            jax.ShapeDtypeStruct((ITERS, width, width), jnp.float32),
            jax.ShapeDtypeStruct((width, row_count), jnp.float32),
    )
    outs = pl.pallas_call(
        functools.partial(kernel, ITERS, group_count, owner_count),
        out_shape=tuple(pltpu.VMEM(x.shape, x.dtype) for x in shapes),
        in_specs=[hbm, hbm, hbm, hbm, smem, hbm],
        out_specs=(vmem, vmem, vmem),
        scratch_shapes=[
            pltpu.VMEM((width, row_count), jnp.float32),
            pltpu.VMEM((1, row_count), jnp.float32),
            pltpu.SMEM((tile_count,), jnp.int32),
            pltpu.SMEM((tile_count,), jnp.int32),
            dma((4,)),
            pltpu.VMEM(matrix.shape, jnp.bfloat16),
            pltpu.VMEM(matrix.shape, jnp.bfloat16),
            pltpu.VMEM((tile_count, owned, 8, 128), jnp.float32),
            pltpu.VMEM((tile_count + 1, width, part), jnp.float32),
            pltpu.VMEM((2, owner_count, width, part), jnp.bfloat16),
            pltpu.VMEM((owner_count, width, part), jnp.bfloat16),
            pltpu.VMEM((owner_count, total_cols, part), jnp.bfloat16),
            pltpu.VMEM((group_count, width, part), jnp.bfloat16),
            pltpu.VMEM((total_cols + width, row_count), jnp.bfloat16),
            pltpu.VMEM((back_count, width, part), jnp.bfloat16),
            pltpu.VMEM((2, back_count, width, part), jnp.bfloat16),
            pltpu.VMEM((group_count, width, part), jnp.bfloat16),
            pltpu.VMEM((group_count, width, part), jnp.bfloat16),
            pltpu.VMEM((pair_count, width, part), jnp.bfloat16),
            pltpu.VMEM((2, pair_count, width, part), jnp.bfloat16),
            pltpu.VMEM((2, 2 * group_count, packed, total_cols), jnp.bfloat16),
            pltpu.VMEM((packed, total_cols), jnp.bfloat16),
            pltpu.VMEM((chips - 1, packed, total_cols), jnp.bfloat16),
            pltpu.VMEM((total_cols, part), jnp.float32),
            pltpu.VMEM((total_cols, part), jnp.float32),
            pltpu.VMEM((total_cols, total_cols), jnp.float32),
            pltpu.VMEM((8, owned * owner_count), jnp.int32),
            pltpu.SMEM((8, owned * owner_count), jnp.int32),
            dma, dma,
            dma, dma((2, owner_count // 2 - 1)), dma, dma((2,)), dma, dma,
            dma, dma((2,)), dma, dma((2,)), dma, dma, dma, dma((2,)), dma, dma,
        ],
        compiler_params=pltpu.CompilerParams(
            collective_id=0, has_side_effects=True, vmem_limit_bytes=60 * 1024 * 1024
        ),
    )(start_block, dual_shift[None, :], tile_rows[0, 0], tile_cols[0, 0], live_tiles[0], matrix)
    return pl.pallas_call(hand_on, out_shape=shapes, in_specs=[vmem] * 3, out_specs=(vmem,) * 3,
        compiler_params=pltpu.CompilerParams(vmem_limit_bytes=2 * 1024 * 1024))(*outs)


def solution(mesh):
    in_specs = (
        P("grp", "row", None, None, None),
        P("grp", "row", None),
        P("grp", "row", None),
        P("grp", "row"),
        P("row"),
        P(None, "row"),
    )
    out_specs = (P(), P(), P(None, "row"))
    return jax.shard_map(
        per_device, mesh=mesh, in_specs=in_specs, out_specs=out_specs, check_vma=False
    )
```

```python
import functools

import jax
import jax.numpy as jnp
from jax import lax
from jax.experimental import pallas as pl
from jax.experimental.pallas import tpu as pltpu
from jax.sharding import PartitionSpec as P

ITERS = 4
MESH = pl.DeviceIdType.MESH
NT = (((1,), (1,)), ((), ()))
MIDDLE = 1.25
PANEL = 16
SIDE = 4
NEAR = 2


def halves(x):
    high = x.astype(jnp.bfloat16)
    return high, (x - high.astype(jnp.float32)).astype(jnp.bfloat16)


def dot_split(a, b, dims):
    (a_high, a_low), (b_high, b_low) = halves(a), halves(b)

    def dot(x, y):
        return lax.dot_general(x, y, dims, preferred_element_type=jnp.float32)

    return dot(a_high, b_low) + dot(a_low, b_high) + dot(a_high, b_high)


def dot_nt(a, b):
    return dot_split(a, b, NT)


def dot_nn(a, b):
    return dot_split(a, b, (((1,), (0,)), ((), ())))


def factor_and_inverse(gram):
    n = gram.shape[0]
    row = lax.broadcasted_iota(jnp.int32, (n, n), 0)
    lane = lax.broadcasted_iota(jnp.int32, (n, n), 1)
    within = lax.broadcasted_iota(jnp.int32, (PANEL, 2 * n), 0)
    work = jnp.concatenate([gram, jnp.where(row == lane, 1.0, 0.0)], axis=1)
    blocks = []
    for start in range(0, n, PANEL):
        columns = [jnp.broadcast_to(work[:, k : k + 1], work.shape) for k in range(start, start + PANEL)]
        rows = [work[i : i + 1, :] for i in range(PANEL)]
        block = jnp.zeros((PANEL, 2 * n), jnp.float32)
        for i in range(0, PANEL, 2):
            first, second = columns[i], columns[i + 1]
            corner, cross, other = first[i : i + 1, :], first[i + 1 : i + 2, :], second[i + 1 : i + 2, :]
            det = corner * other - cross * cross
            scale, root = lax.rsqrt(corner), lax.rsqrt(det)
            left, right = root * scale * corner, root * scale * cross
            columns[i] = first * scale
            columns[i + 1] = second * left - first * right
            upper_row, lower_row = rows[i], rows[i + 1]
            rows[i] = upper_row * scale
            rows[i + 1] = lower_row * left - upper_row * right
            for later in range(i + 2, PANEL):
                for k in (i, i + 1):
                    weight = columns[k][later : later + 1, :]
                    columns[later] = columns[later] - columns[k] * weight
                    rows[later] = rows[later] - rows[k] * weight
            block = jnp.where(within == i, rows[i], block)
            block = jnp.where(within == i + 1, rows[i + 1], block)
        blocks.append(block)
        work = work[PANEL:]
        if start + PANEL < n:
            for i in range(PANEL):
                work = work - columns[i][PANEL:] * rows[i]
    whole = jnp.concatenate(blocks, axis=0)
    return jnp.where(lane >= row, whole[:, :n], 0.0), whole[:, n:]


def away(d, chips):
    return min(d % SIDE, SIDE - d % SIDE) + min(d // SIDE, chips // SIDE - d // SIDE)


def far_first(chips):
    return sorted(range(1, chips), key=lambda d: (-away(d, chips), -min(d // SIDE, 4 - d // SIDE)))


def kernel(
    steps, group_count, owner_count,
    start_hbm, shift_hbm, rows_hbm, cols_hbm, live_ref, tiles_hbm,
    proj_ref, fac_ref, next_ref,
    start_ref, shift_ref, rows_ref, cols_ref, input_sem, tiles_ref, turned, masks, products, gathered, stage, history, own, own_history, back_out, back_in, direct_out, direct_in,
    pair_out, pair_in, dots_grp, chip_out, chip_in, basis, images, transform, place_vector, place_ref, tile_sem, place_sem,
    gather_send, gather_recv, relay_send, relay_recv, own_send, own_recv,
    pair_send, pair_recv, back_send, back_recv, direct_send, direct_recv, dots_send, dots_recv, chip_send, chip_recv,
):
    g = lax.axis_index("grp")
    r = lax.axis_index("row")
    width = start_ref.shape[0]
    row_count = start_ref.shape[1]
    part = row_count // group_count
    tile_count = tiles_ref.shape[0]
    owned = row_count // tiles_ref.shape[1]
    chips = owner_count // 2
    chip, core = r // 2, lax.rem(r, 2)
    partner = chip * 2 + 1 - core
    chip_x, chip_z = lax.rem(chip, SIDE), chip // SIDE

    offsets = far_first(chips)

    def chip_at(d, sign):
        z_count = chips // SIDE
        return lax.rem(chip_z + (sign * (d // SIDE)) % z_count, z_count) * SIDE + lax.rem(
            chip_x + (sign * (d % SIDE)) % SIDE, SIDE
        )

    far_count = sum(away(d, chips) > NEAR for d in offsets)
    sources = [chip_at(d, -1) for d in offsets]
    targets = [chip_at(d, 1) for d in offsets]
    grp_order = sorted(range(1, group_count), key=lambda d: -min(d, group_count - d))
    grp_peers = [lax.rem(g + d, group_count) for d in grp_order]
    total_cols = steps * width

    inputs = [
        pltpu.make_async_copy(src, dst, input_sem.at[i])
        for i, (src, dst) in enumerate(
            [(start_hbm, start_ref), (shift_hbm, shift_ref), (rows_hbm, rows_ref), (cols_hbm, cols_ref)]
        )
    ]
    for copy in inputs:
        copy.start()
    load = pltpu.make_async_copy(tiles_hbm, tiles_ref, tile_sem)
    load.start()
    barrier = pltpu.get_barrier_semaphore()
    for peer in targets:
        pl.semaphore_signal(barrier, inc=1, device_id=(g, peer * 2 + core), device_id_type=MESH)
    pl.semaphore_signal(barrier, inc=1, device_id=(g, partner), device_id_type=MESH)
    for peer in grp_peers:
        pl.semaphore_signal(barrier, inc=1, device_id=(peer, r), device_id_type=MESH)

    def to_row(peer, src, dst, send, recv):
        return pltpu.make_async_remote_copy(
            src_ref=src, dst_ref=dst, send_sem=send, recv_sem=recv,
            device_id=(g, peer), device_id_type=MESH,
        )

    def to_grp(peer, src, dst, send, recv):
        return pltpu.make_async_remote_copy(
            src_ref=src, dst_ref=dst, send_sem=send, recv_sem=recv,
            device_id=(peer, r), device_id_type=MESH,
        )

    others = group_count - 1

    def send_own(operand):
        own[g] = operand
        for peer in grp_peers:
            to_grp(peer, own.at[g], own.at[g], own_send, own_recv).start()

    def send_vectors(half, operand, own_too=True):
        gathered[half, r] = operand
        if own_too:
            send_own(operand)
        for i, peer in enumerate(targets):
            to_row(
                peer * 2 + core, gathered.at[half, r], gathered.at[half, r], gather_send, gather_recv.at[half, i]
            ).start()
        to_row(partner, gathered.at[half, r], gathered.at[half, r], gather_send, relay_recv.at[half]).start()
        stage[r] = operand

    def sent_own():
        bulk = own.at[pl.ds(0, others)]
        to_grp(grp_peers[0], bulk, bulk, own_send, own_send).wait_send()

    def sent_vectors():
        bulk = gathered.at[0, pl.ds(0, chips)]
        to_row(partner, bulk, bulk, gather_send, gather_send).wait_send()

    def take_own():
        bulk = own.at[pl.ds(0, others)]
        to_grp(grp_peers[0], bulk, bulk, own_recv, own_recv).wait_recv()

    def keep_own(step):
        for i in range(group_count):
            own_history[step * width : (step + 1) * width, i * part : (i + 1) * part] = own[i]

    def take_gathered(step, half):
        dots, batch = None, [r]
        for count, (i, peer) in enumerate(list(enumerate(sources))):
            slot = peer * 2 + core
            block = gathered.at[half, slot]
            to_row(slot, block, block, gather_send, gather_recv.at[half, i]).wait_recv()
            to_row(partner, block, block, relay_send, relay_recv.at[half]).start()
            stage[slot] = gathered[half, slot]
            batch.append(slot)
            if count % 5 == 4:
                value = slot_dots(step, batch)
                dots = value if dots is None else dots + value
                batch = []
        return dots

    def relays_sent():
        bulk = gathered.at[0, pl.ds(0, chips - 1)]
        to_row(partner, bulk, bulk, relay_send, relay_send).wait_send()

    def take_relayed(half):
        bulk = gathered.at[half, pl.ds(0, chips)]
        to_row(partner, bulk, bulk, gather_send, relay_recv.at[half]).wait_recv()
        for peer in range(chips):
            slot = peer * 2 + 1 - core
            stage[slot] = gathered[half, slot]

    def pack(dots):
        pieces, done, count = [], 0, dots.shape[1]
        for size in (128, 64, 32):
            while count - done >= size:
                height = width * size // 128
                piece = dots[:, done : done + size]
                pieces.append(
                    jnp.concatenate([piece[i * height : (i + 1) * height] for i in range(width // height)], axis=1)
                )
                done += size
        return jnp.concatenate(pieces, axis=0)

    def unpack(packed, count):
        pieces, done, row = [], 0, 0
        for size in (128, 64, 32):
            while count - done >= size:
                height = width * size // 128
                piece = packed[row : row + height]
                pieces.append(
                    jnp.concatenate([piece[:, i * size : (i + 1) * size] for i in range(width // height)], axis=0)
                )
                done += size
                row += height
        return pieces

    def packed_rows(step):
        return pl.ds(0, 16 + (step + 1) // 2 * 16)

    def slot_dots(step, slots):
        dots = jnp.zeros((width, (step + 1) * width), jnp.float32)
        for slot in slots:
            vector = stage[slot]
            right = vector
            if step > 0:
                right = jnp.concatenate([vector, history[slot, : step * width, :]], axis=0)
            dots = dots + lax.dot_general(vector, right, NT, preferred_element_type=jnp.float32)
        return dots

    def encode(step, dots):
        gram, cross = dots
        high = gram.astype(jnp.bfloat16).astype(jnp.float32)
        pieces = [high, gram - high]
        if step > 0:
            pieces.append(cross)
        if step % 2 == 1:
            newest = cross[cross.shape[0] - 8 :]
            pieces.append(newest - newest.astype(jnp.bfloat16).astype(jnp.float32))
        return jnp.concatenate(pieces, axis=0).astype(jnp.bfloat16)

    def pack_both(step, dots):
        return pack(dots[:, :width]), pack(dots[:, width:]) if step > 0 else None

    def send_dots(step, half, dots):
        rows = packed_rows(step)
        me = g * 2 + core
        dots_grp[half, me, rows] = encode(step, dots)
        block = dots_grp.at[half, me, rows]
        for peer in grp_peers:
            to_grp(peer, block, block, dots_send, dots_recv.at[half]).start()
            pltpu.make_async_remote_copy(
                src_ref=block, dst_ref=block, send_sem=dots_send, recv_sem=dots_recv.at[half],
                device_id=(peer, partner), device_id_type=MESH,
            ).start()
        to_row(partner, block, block, dots_send, dots_recv.at[half]).start()

    def take_dots(step, half):
        rows = packed_rows(step)
        bulk = dots_grp.at[half, pl.ds(0, 2 * group_count - 1), rows]
        to_grp(grp_peers[0], bulk, bulk, dots_send, dots_recv.at[half]).wait_recv()
        summed = dots_grp[half, 0, rows].astype(jnp.float32)
        for index in range(1, 2 * group_count):
            summed = summed + dots_grp[half, index, rows].astype(jnp.float32)
        gram = unpack(summed[:8] + summed[8:16], width)[0]
        if step == 0:
            return None, gram
        old = summed[16 : 16 + step * 8]
        if step % 2 == 1:
            newest = old[step * 8 - 8 :] + summed[16 + step * 8 :]
            old = newest if step == 1 else jnp.concatenate([old[: step * 8 - 8], newest], axis=0)
        pieces = unpack(old, step * width)
        whole = jnp.concatenate(pieces, axis=1) if len(pieces) > 1 else pieces[0]
        cross = dot_nt(whole, transform[:, : step * width])
        return cross, gram - dot_nt(cross, cross)

    def dots_sent(step, half):
        bulk = dots_grp.at[half, pl.ds(0, 2 * group_count - 1), packed_rows(step)]
        to_grp(grp_peers[0], bulk, bulk, dots_send, dots_recv.at[half]).wait_send()

    def back_product(slot):
        value = products[place_ref[0, slot]]
        for i in range(1, owned):
            value = value + products[place_ref[0, i * owner_count + slot]]
        return value

    def take_pair(peer, half):
        return pair_in[half, peer].astype(jnp.float32)

    mine = pl.ds(pl.multiple_of(g * part, part), part)
    for copy in inputs:
        copy.wait()
    current = start_ref[:, mine]
    shift = shift_ref[:, mine]
    pl.semaphore_wait(barrier, chips + others)
    send_vectors(0, current.astype(jnp.bfloat16), own_too=False)
    for i in range(group_count):
        own[i] = start_ref[:, i * part : (i + 1) * part].astype(jnp.bfloat16)
    lanes = lax.broadcasted_iota(jnp.int32, place_vector.shape, 1)
    place = jnp.full(place_vector.shape, tile_count, jnp.int32)
    for k in range(tile_count):
        alive = k < live_ref[0]
        position = jnp.where(alive, rows_ref[k] * owner_count + cols_ref[k], -1)
        place = jnp.where(lanes == position, k, place)
        row = jnp.full((8, 128), jnp.where(alive, rows_ref[k], -1), jnp.int32)
        for i in range(owned):
            masks[k, i] = jnp.where(row == i, 1.0, 0.0)
    place_vector[...] = place
    place_copy = pltpu.make_async_copy(place_vector, place_ref, place_sem)
    place_copy.start()
    basis[...] = jnp.zeros_like(basis)
    images[...] = jnp.zeros_like(images)
    transform[...] = jnp.zeros_like(transform)
    products[tile_count] = jnp.zeros((width, part), jnp.float32)
    load.wait()
    place_copy.wait()

    def turn(j, carry):
        for i in range(4):
            turned[j * 4 + i] = tiles_ref[j * 4 + i].T
        return carry

    coef, middle = None, MIDDLE
    lane = lax.broadcasted_iota(jnp.int32, (width, total_cols), 1)
    sub = lax.broadcasted_iota(jnp.int32, (width, total_cols), 0)
    for step in range(steps):
        half = step % 2
        far = far_count if step > 0 else 0
        near_rows = pl.ds(0, chips - far)
        if step > 0:
            take_own()
        for k in range(tile_count):
            products[k] = jnp.dot(own[rows_ref[k]], tiles_ref[k], preferred_element_type=jnp.float32)
        for i, peer in enumerate(targets[far:] + [chip]):
            pair_out[i] = back_product(peer * 2 + 1 - core).astype(jnp.bfloat16)
            to_row(partner, pair_out.at[i], pair_in.at[half, i], pair_send, pair_recv.at[half]).start()
        for i, peer in enumerate(targets[:far]):
            for side, slot in enumerate([peer * 2 + core, peer * 2 + 1 - core]):
                index = 2 * i + side
                back_out[index] = back_product(slot).astype(jnp.bfloat16)
                to_row(
                    slot, back_out.at[index], back_in.at[half, index], back_send, back_recv.at[half]
                ).start()
        keep_own(step)
        if step == 0:
            lax.fori_loop(0, tile_count // 4, turn, 0)
        def send_back():
            to_row(
                partner, pair_out.at[near_rows], pair_in.at[half, near_rows], pair_send, pair_recv.at[half]
            ).wait_recv()
            for i, peer in enumerate(targets[far:]):
                index = 2 * far + i
                back_out[index] = (back_product(peer * 2 + core) + take_pair(i, half)).astype(jnp.bfloat16)
                to_row(
                    peer * 2 + core, back_out.at[index], back_in.at[half, index], back_send, back_recv.at[half]
                ).start()
            total = back_product(r) + take_pair(len(targets) - far, half)
            return total

        if step == 0:
            total = send_back()
        dots = take_gathered(step, half)
        send_dots(step, half, pack_both(step, dots))
        if step > 0:
            total = send_back()
        take_relayed(half)
        forward = [jnp.zeros((width, part), jnp.float32)] * owned
        for k in range(tile_count):
            value = jnp.dot(stage[cols_ref[k]], turned[k], preferred_element_type=jnp.float32)
            for i in range(owned):
                mask = jnp.concatenate([masks[k, i]] * (part // 128), axis=1)
                forward[i] = forward[i] + value * jnp.concatenate([mask] * (width // 8), axis=0)
        for i in range(owned):
            direct_out[i] = forward[i].astype(jnp.bfloat16)
        for peer in grp_peers:
            to_grp(peer, direct_out.at[peer], direct_in.at[g], direct_send, direct_recv).start()
        for i in range(owned):
            total = total + forward[i] * jnp.where(g == i, 1.0, 0.0)
        for slot in range(owner_count):
            history[slot, step * width : (step + 1) * width, :] = stage[slot]
        sent_vectors()
        if step > 0:
            sent_own()
        relays_sent()
        cross, gram = take_dots(step, half)
        left, rest = current, None
        if step > 0:
            left = left - dot_nn(cross, basis[...])
            rest = dot_nn(cross, images[...])
            first = cross + coef
            newest = jnp.where(lane == (step - 1) * width + sub, first, 0.0)
            middle = -jnp.sum(newest, axis=(0, 1), keepdims=True) / width
        upper, inverse = factor_and_inverse(gram)
        now = dot_nn(inverse, left)
        ahead = now * (middle - shift)
        if step > 0:
            ahead = ahead - dot_nn(upper, basis[(step - 1) * width : step * width, :])
        bulk = back_in.at[half, pl.ds(0, chips - 1 + far)]
        to_row(partner, bulk, bulk, back_send, back_recv.at[half]).wait_recv()
        for index in range(chips - 1 + far):
            total = total + back_in[half, index].astype(jnp.float32)
        bulk = direct_in.at[pl.ds(0, others)]
        to_grp(grp_peers[0], bulk, bulk, direct_send, direct_recv).wait_recv()
        for peer in grp_peers:
            total = total + direct_in[peer].astype(jnp.float32)
        total = 0.5 * total
        if step > 0:
            total = total - rest
        image = dot_nn(inverse, total)
        current = image + ahead
        if step < steps - 1:
            send_vectors(1 - half, current.astype(jnp.bfloat16))
        else:
            send_own(current.astype(jnp.bfloat16))
            stage[r] = current.astype(jnp.bfloat16)
            local = pack_both(steps, slot_dots(steps, [r]))
            chip_out[...] = encode(steps, local)
            for i, peer in enumerate(targets):
                to_row(peer * 2 + core, chip_out, chip_in.at[i], chip_send, chip_recv).start()
        basis[step * width : (step + 1) * width, :] = now
        images[step * width : (step + 1) * width, :] = image
        if step > 0:
            proj_ref[step - 1] = first
            fac_ref[step - 1] = upper.T
        unit = jnp.where(lane == step * width + sub, 1.0, 0.0)
        if step == 0:
            transform[:width, :] = dot_nn(inverse, unit)
            coef = -MIDDLE * unit
        else:
            transform[step * width : (step + 1) * width, :] = dot_nn(inverse, unit - dot_nn(cross, transform[...]))
            wide = jnp.concatenate([upper] * (total_cols // width), axis=1)
            coef = -middle * unit + jnp.where((lane >= (step - 1) * width) & (lane < step * width), wide, 0.0)
        bulk = pair_out.at[near_rows]
        to_row(partner, bulk, bulk, pair_send, pair_recv.at[half]).wait_send()
        bulk = back_out.at[pl.ds(0, chips - 1 + far)]
        to_row(partner, bulk, bulk, back_send, back_recv.at[half]).wait_send()
        bulk = direct_out.at[pl.ds(0, others)]
        to_grp(grp_peers[0], bulk, bulk, direct_send, direct_recv).wait_send()
        dots_sent(step, half)

    half = steps % 2
    take_own()
    keep_own(steps)
    sent_own()
    to_row(partner, chip_in, chip_in, chip_send, chip_recv).wait_recv()
    summed = chip_in[0].astype(jnp.float32)
    for i in range(1, chips - 1):
        summed = summed + chip_in[i].astype(jnp.float32)
    send_dots(steps, half, (local[0] + summed[:8] + summed[8:16], local[1] + summed[16:]))
    to_row(partner, chip_in, chip_in, chip_send, chip_recv).wait_send()
    cross, gram = take_dots(steps, half)
    combine = dot_nn(cross, transform[...])
    high = combine.astype(jnp.bfloat16)
    low = (combine - high.astype(jnp.float32)).astype(jnp.bfloat16)
    both = jnp.dot(
        jnp.concatenate([high, low], axis=0), own_history[:total_cols, :], preferred_element_type=jnp.float32
    )
    left = own_history[total_cols:, :].astype(jnp.float32) - both[:width] - both[width:]
    upper, inverse = factor_and_inverse(gram)
    proj_ref[steps - 1] = cross + coef
    fac_ref[steps - 1] = upper.T
    next_ref[...] = dot_nn(inverse, left)
    dots_sent(steps, half)


def hand_on(proj_in, fac_in, next_in, proj_ref, fac_ref, next_ref):
    proj_ref[...] = proj_in[...]
    fac_ref[...] = fac_in[...]
    next_ref[...] = next_in[...]


def per_device(tiles, tile_rows, tile_cols, live_tiles, dual_shift, start_block):
    matrix = tiles[0, 0]
    tile_count, edge = matrix.shape[0], matrix.shape[1]
    width, row_count = start_block.shape
    group_count = lax.axis_size("grp")
    owner_count = lax.axis_size("row")
    owned = row_count // edge
    part = row_count // group_count
    total_cols = ITERS * width
    vmem = pl.BlockSpec(memory_space=pltpu.VMEM)
    smem = pl.BlockSpec(memory_space=pltpu.SMEM)
    hbm = pl.BlockSpec(memory_space=pltpu.HBM)
    dma = pltpu.SemaphoreType.DMA
    chips = owner_count // 2
    far = sum(away(d, chips) > NEAR for d in far_first(chips))
    back_count = chips - 1 + far
    pair_count = chips
    packed = 16 + (ITERS + 1) // 2 * 16
    shapes = (
            jax.ShapeDtypeStruct((ITERS, width, total_cols), jnp.float32),
            jax.ShapeDtypeStruct((ITERS, width, width), jnp.float32),
            jax.ShapeDtypeStruct((width, row_count), jnp.float32),
    )
    outs = pl.pallas_call(
        functools.partial(kernel, ITERS, group_count, owner_count),
        out_shape=tuple(pltpu.VMEM(x.shape, x.dtype) for x in shapes),
        in_specs=[hbm, hbm, hbm, hbm, smem, hbm],
        out_specs=(vmem, vmem, vmem),
        scratch_shapes=[
            pltpu.VMEM((width, row_count), jnp.float32),
            pltpu.VMEM((1, row_count), jnp.float32),
            pltpu.SMEM((tile_count,), jnp.int32),
            pltpu.SMEM((tile_count,), jnp.int32),
            dma((4,)),
            pltpu.VMEM(matrix.shape, jnp.bfloat16),
            pltpu.VMEM(matrix.shape, jnp.bfloat16),
            pltpu.VMEM((tile_count, owned, 8, 128), jnp.float32),
            pltpu.VMEM((tile_count + 1, width, part), jnp.float32),
            pltpu.VMEM((2, owner_count, width, part), jnp.bfloat16),
            pltpu.VMEM((owner_count, width, part), jnp.bfloat16),
            pltpu.VMEM((owner_count, total_cols, part), jnp.bfloat16),
            pltpu.VMEM((group_count, width, part), jnp.bfloat16),
            pltpu.VMEM((total_cols + width, row_count), jnp.bfloat16),
            pltpu.VMEM((back_count, width, part), jnp.bfloat16),
            pltpu.VMEM((2, back_count, width, part), jnp.bfloat16),
            pltpu.VMEM((group_count, width, part), jnp.bfloat16),
            pltpu.VMEM((group_count, width, part), jnp.bfloat16),
            pltpu.VMEM((pair_count, width, part), jnp.bfloat16),
            pltpu.VMEM((2, pair_count, width, part), jnp.bfloat16),
            pltpu.VMEM((2, 2 * group_count, packed, total_cols), jnp.bfloat16),
            pltpu.VMEM((packed, total_cols), jnp.bfloat16),
            pltpu.VMEM((chips - 1, packed, total_cols), jnp.bfloat16),
            pltpu.VMEM((total_cols, part), jnp.float32),
            pltpu.VMEM((total_cols, part), jnp.float32),
            pltpu.VMEM((total_cols, total_cols), jnp.float32),
            pltpu.VMEM((8, owned * owner_count), jnp.int32),
            pltpu.SMEM((8, owned * owner_count), jnp.int32),
            dma, dma,
            dma, dma((2, owner_count // 2 - 1)), dma, dma((2,)), dma, dma,
            dma, dma((2,)), dma, dma((2,)), dma, dma, dma, dma((2,)), dma, dma,
        ],
        compiler_params=pltpu.CompilerParams(
            collective_id=0, has_side_effects=True, vmem_limit_bytes=60 * 1024 * 1024
        ),
    )(start_block, dual_shift[None, :], tile_rows[0, 0], tile_cols[0, 0], live_tiles[0], matrix)
    return pl.pallas_call(hand_on, out_shape=shapes, in_specs=[vmem] * 3, out_specs=(vmem,) * 3,
        compiler_params=pltpu.CompilerParams(vmem_limit_bytes=2 * 1024 * 1024))(*outs)


def solution(mesh):
    in_specs = (
        P("grp", "row", None, None, None),
        P("grp", "row", None),
        P("grp", "row", None),
        P("grp", "row"),
        P("row"),
        P(None, "row"),
    )
    out_specs = (P(), P(), P(None, "row"))
    return jax.shard_map(
        per_device, mesh=mesh, in_specs=in_specs, out_specs=out_specs, check_vma=False
    )
```

```python
import functools

import jax
import jax.numpy as jnp
from jax import lax
from jax.experimental import pallas as pl
from jax.experimental.pallas import tpu as pltpu
from jax.sharding import PartitionSpec as P

ITERS = 4
MESH = pl.DeviceIdType.MESH
NT = (((1,), (1,)), ((), ()))
MIDDLE = 1.25
PANEL = 32
SIDE = 4
NEAR = 2


def halves(x):
    high = x.astype(jnp.bfloat16)
    return high, (x - high.astype(jnp.float32)).astype(jnp.bfloat16)


def dot_split(a, b, dims):
    (a_high, a_low), (b_high, b_low) = halves(a), halves(b)

    def dot(x, y):
        return lax.dot_general(x, y, dims, preferred_element_type=jnp.float32)

    return dot(a_high, b_low) + dot(a_low, b_high) + dot(a_high, b_high)


def dot_nt(a, b):
    return dot_split(a, b, NT)


def dot_nn(a, b):
    return dot_split(a, b, (((1,), (0,)), ((), ())))


def factor_and_inverse(gram):
    n = gram.shape[0]
    row = lax.broadcasted_iota(jnp.int32, (n, n), 0)
    lane = lax.broadcasted_iota(jnp.int32, (n, n), 1)
    within = lax.broadcasted_iota(jnp.int32, (PANEL, 2 * n), 0)
    work = jnp.concatenate([gram, jnp.where(row == lane, 1.0, 0.0)], axis=1)
    blocks = []
    for start in range(0, n, PANEL):
        columns = [jnp.broadcast_to(work[:, k : k + 1], work.shape) for k in range(start, start + PANEL)]
        rows = [work[i : i + 1, :] for i in range(PANEL)]
        block = jnp.zeros((PANEL, 2 * n), jnp.float32)
        for i in range(0, PANEL, 2):
            first, second = columns[i], columns[i + 1]
            corner, cross, other = first[i : i + 1, :], first[i + 1 : i + 2, :], second[i + 1 : i + 2, :]
            det = corner * other - cross * cross
            scale, root = lax.rsqrt(corner), lax.rsqrt(det)
            left, right = root * scale * corner, root * scale * cross
            columns[i] = first * scale
            columns[i + 1] = second * left - first * right
            upper_row, lower_row = rows[i], rows[i + 1]
            rows[i] = upper_row * scale
            rows[i + 1] = lower_row * left - upper_row * right
            for later in range(i + 2, PANEL):
                for k in (i, i + 1):
                    weight = columns[k][later : later + 1, :]
                    columns[later] = columns[later] - columns[k] * weight
                    rows[later] = rows[later] - rows[k] * weight
            block = jnp.where(within == i, rows[i], block)
            block = jnp.where(within == i + 1, rows[i + 1], block)
        blocks.append(block)
        work = work[PANEL:]
        if start + PANEL < n:
            for i in range(PANEL):
                work = work - columns[i][PANEL:] * rows[i]
    whole = jnp.concatenate(blocks, axis=0)
    return jnp.where(lane >= row, whole[:, :n], 0.0), whole[:, n:]


def away(d, chips):
    return min(d % SIDE, SIDE - d % SIDE) + min(d // SIDE, chips // SIDE - d // SIDE)


def far_first(chips):
    return sorted(range(1, chips), key=lambda d: (-away(d, chips), -min(d // SIDE, 4 - d // SIDE)))


def kernel(
    steps, group_count, owner_count,
    start_hbm, shift_hbm, rows_hbm, cols_hbm, live_ref, tiles_hbm,
    proj_ref, fac_ref, next_ref,
    start_ref, shift_ref, rows_ref, cols_ref, input_sem, tiles_ref, turned, masks, products, gathered, stage, history, own, own_history, back_out, back_in, direct_out, direct_in,
    pair_out, pair_in, dots_grp, chip_out, chip_in, basis, images, transform, place_vector, place_ref, tile_sem, place_sem,
    gather_send, gather_recv, relay_send, relay_recv, own_send, own_recv,
    pair_send, pair_recv, back_send, back_recv, direct_send, direct_recv, dots_send, dots_recv, chip_send, chip_recv,
):
    g = lax.axis_index("grp")
    r = lax.axis_index("row")
    width = start_ref.shape[0]
    row_count = start_ref.shape[1]
    part = row_count // group_count
    tile_count = tiles_ref.shape[0]
    owned = row_count // tiles_ref.shape[1]
    chips = owner_count // 2
    chip, core = r // 2, lax.rem(r, 2)
    partner = chip * 2 + 1 - core
    chip_x, chip_z = lax.rem(chip, SIDE), chip // SIDE

    offsets = far_first(chips)

    def chip_at(d, sign):
        z_count = chips // SIDE
        return lax.rem(chip_z + (sign * (d // SIDE)) % z_count, z_count) * SIDE + lax.rem(
            chip_x + (sign * (d % SIDE)) % SIDE, SIDE
        )

    far_count = sum(away(d, chips) > NEAR for d in offsets)
    sources = [chip_at(d, -1) for d in offsets]
    targets = [chip_at(d, 1) for d in offsets]
    grp_order = sorted(range(1, group_count), key=lambda d: -min(d, group_count - d))
    grp_peers = [lax.rem(g + d, group_count) for d in grp_order]
    total_cols = steps * width

    inputs = [
        pltpu.make_async_copy(src, dst, input_sem.at[i])
        for i, (src, dst) in enumerate(
            [(start_hbm, start_ref), (shift_hbm, shift_ref), (rows_hbm, rows_ref), (cols_hbm, cols_ref)]
        )
    ]
    for copy in inputs:
        copy.start()
    load = pltpu.make_async_copy(tiles_hbm, tiles_ref, tile_sem)
    load.start()
    barrier = pltpu.get_barrier_semaphore()
    for peer in targets:
        pl.semaphore_signal(barrier, inc=1, device_id=(g, peer * 2 + core), device_id_type=MESH)
    pl.semaphore_signal(barrier, inc=1, device_id=(g, partner), device_id_type=MESH)
    for peer in grp_peers:
        pl.semaphore_signal(barrier, inc=1, device_id=(peer, r), device_id_type=MESH)

    def to_row(peer, src, dst, send, recv):
        return pltpu.make_async_remote_copy(
            src_ref=src, dst_ref=dst, send_sem=send, recv_sem=recv,
            device_id=(g, peer), device_id_type=MESH,
        )

    def to_grp(peer, src, dst, send, recv):
        return pltpu.make_async_remote_copy(
            src_ref=src, dst_ref=dst, send_sem=send, recv_sem=recv,
            device_id=(peer, r), device_id_type=MESH,
        )

    others = group_count - 1

    def send_own(operand):
        own[g] = operand
        for peer in grp_peers:
            to_grp(peer, own.at[g], own.at[g], own_send, own_recv).start()

    def send_vectors(half, operand, own_too=True):
        gathered[half, r] = operand
        if own_too:
            send_own(operand)
        for i, peer in enumerate(targets):
            to_row(
                peer * 2 + core, gathered.at[half, r], gathered.at[half, r], gather_send, gather_recv.at[half, i]
            ).start()
        to_row(partner, gathered.at[half, r], gathered.at[half, r], gather_send, relay_recv.at[half]).start()
        stage[r] = operand

    def sent_own():
        bulk = own.at[pl.ds(0, others)]
        to_grp(grp_peers[0], bulk, bulk, own_send, own_send).wait_send()

    def sent_vectors():
        bulk = gathered.at[0, pl.ds(0, chips)]
        to_row(partner, bulk, bulk, gather_send, gather_send).wait_send()

    def take_own():
        bulk = own.at[pl.ds(0, others)]
        to_grp(grp_peers[0], bulk, bulk, own_recv, own_recv).wait_recv()

    def keep_own(step):
        for i in range(group_count):
            own_history[step * width : (step + 1) * width, i * part : (i + 1) * part] = own[i]

    def take_gathered(step, half):
        dots, batch = None, [r]
        for count, (i, peer) in enumerate(list(enumerate(sources))):
            slot = peer * 2 + core
            block = gathered.at[half, slot]
            to_row(slot, block, block, gather_send, gather_recv.at[half, i]).wait_recv()
            to_row(partner, block, block, relay_send, relay_recv.at[half]).start()
            stage[slot] = gathered[half, slot]
            batch.append(slot)
            if count % 5 == 4:
                value = slot_dots(step, batch)
                dots = value if dots is None else dots + value
                batch = []
        return dots

    def relays_sent():
        bulk = gathered.at[0, pl.ds(0, chips - 1)]
        to_row(partner, bulk, bulk, relay_send, relay_send).wait_send()

    def take_relayed(half):
        bulk = gathered.at[half, pl.ds(0, chips)]
        to_row(partner, bulk, bulk, gather_send, relay_recv.at[half]).wait_recv()
        for peer in range(chips):
            slot = peer * 2 + 1 - core
            stage[slot] = gathered[half, slot]

    def pack(dots):
        pieces, done, count = [], 0, dots.shape[1]
        for size in (128, 64, 32):
            while count - done >= size:
                height = width * size // 128
                piece = dots[:, done : done + size]
                pieces.append(
                    jnp.concatenate([piece[i * height : (i + 1) * height] for i in range(width // height)], axis=1)
                )
                done += size
        return jnp.concatenate(pieces, axis=0)

    def unpack(packed, count):
        pieces, done, row = [], 0, 0
        for size in (128, 64, 32):
            while count - done >= size:
                height = width * size // 128
                piece = packed[row : row + height]
                pieces.append(
                    jnp.concatenate([piece[:, i * size : (i + 1) * size] for i in range(width // height)], axis=0)
                )
                done += size
                row += height
        return pieces

    def packed_rows(step):
        return pl.ds(0, 16 + (step + 1) // 2 * 16)

    def slot_dots(step, slots):
        dots = jnp.zeros((width, (step + 1) * width), jnp.float32)
        for slot in slots:
            vector = stage[slot]
            right = vector
            if step > 0:
                right = jnp.concatenate([vector, history[slot, : step * width, :]], axis=0)
            dots = dots + lax.dot_general(vector, right, NT, preferred_element_type=jnp.float32)
        return dots

    def encode(step, dots):
        gram, cross = dots
        high = gram.astype(jnp.bfloat16).astype(jnp.float32)
        pieces = [high, gram - high]
        if step > 0:
            pieces.append(cross)
        if step % 2 == 1:
            newest = cross[cross.shape[0] - 8 :]
            pieces.append(newest - newest.astype(jnp.bfloat16).astype(jnp.float32))
        return jnp.concatenate(pieces, axis=0).astype(jnp.bfloat16)

    def pack_both(step, dots):
        return pack(dots[:, :width]), pack(dots[:, width:]) if step > 0 else None

    def send_dots(step, half, dots):
        rows = packed_rows(step)
        me = g * 2 + core
        dots_grp[half, me, rows] = encode(step, dots)
        block = dots_grp.at[half, me, rows]
        for peer in grp_peers:
            to_grp(peer, block, block, dots_send, dots_recv.at[half]).start()
            pltpu.make_async_remote_copy(
                src_ref=block, dst_ref=block, send_sem=dots_send, recv_sem=dots_recv.at[half],
                device_id=(peer, partner), device_id_type=MESH,
            ).start()
        to_row(partner, block, block, dots_send, dots_recv.at[half]).start()

    def take_dots(step, half):
        rows = packed_rows(step)
        bulk = dots_grp.at[half, pl.ds(0, 2 * group_count - 1), rows]
        to_grp(grp_peers[0], bulk, bulk, dots_send, dots_recv.at[half]).wait_recv()
        summed = dots_grp[half, 0, rows].astype(jnp.float32)
        for index in range(1, 2 * group_count):
            summed = summed + dots_grp[half, index, rows].astype(jnp.float32)
        gram = unpack(summed[:8] + summed[8:16], width)[0]
        if step == 0:
            return None, gram
        old = summed[16 : 16 + step * 8]
        if step % 2 == 1:
            newest = old[step * 8 - 8 :] + summed[16 + step * 8 :]
            old = newest if step == 1 else jnp.concatenate([old[: step * 8 - 8], newest], axis=0)
        pieces = unpack(old, step * width)
        whole = jnp.concatenate(pieces, axis=1) if len(pieces) > 1 else pieces[0]
        cross = dot_nt(whole, transform[:, : step * width])
        return cross, gram - dot_nt(cross, cross)

    def dots_sent(step, half):
        bulk = dots_grp.at[half, pl.ds(0, 2 * group_count - 1), packed_rows(step)]
        to_grp(grp_peers[0], bulk, bulk, dots_send, dots_recv.at[half]).wait_send()

    def back_product(slot):
        value = products[place_ref[0, slot]]
        for i in range(1, owned):
            value = value + products[place_ref[0, i * owner_count + slot]]
        return value

    def take_pair(peer, half):
        return pair_in[half, peer].astype(jnp.float32)

    mine = pl.ds(pl.multiple_of(g * part, part), part)
    for copy in inputs:
        copy.wait()
    current = start_ref[:, mine]
    shift = shift_ref[:, mine]
    pl.semaphore_wait(barrier, chips + others)
    send_vectors(0, current.astype(jnp.bfloat16), own_too=False)
    for i in range(group_count):
        own[i] = start_ref[:, i * part : (i + 1) * part].astype(jnp.bfloat16)
    lanes = lax.broadcasted_iota(jnp.int32, place_vector.shape, 1)
    place = jnp.full(place_vector.shape, tile_count, jnp.int32)
    for k in range(tile_count):
        alive = k < live_ref[0]
        position = jnp.where(alive, rows_ref[k] * owner_count + cols_ref[k], -1)
        place = jnp.where(lanes == position, k, place)
        row = jnp.full((8, 128), jnp.where(alive, rows_ref[k], -1), jnp.int32)
        for i in range(owned):
            masks[k, i] = jnp.where(row == i, 1.0, 0.0)
    place_vector[...] = place
    place_copy = pltpu.make_async_copy(place_vector, place_ref, place_sem)
    place_copy.start()
    basis[...] = jnp.zeros_like(basis)
    images[...] = jnp.zeros_like(images)
    transform[...] = jnp.zeros_like(transform)
    products[tile_count] = jnp.zeros((width, part), jnp.float32)
    load.wait()
    place_copy.wait()

    def turn(j, carry):
        for i in range(4):
            turned[j * 4 + i] = tiles_ref[j * 4 + i].T
        return carry

    coef, middle = None, MIDDLE
    lane = lax.broadcasted_iota(jnp.int32, (width, total_cols), 1)
    sub = lax.broadcasted_iota(jnp.int32, (width, total_cols), 0)
    for step in range(steps):
        half = step % 2
        far = far_count if step > 0 else 0
        near_rows = pl.ds(0, chips - far)
        if step > 0:
            take_own()
        for k in range(tile_count):
            products[k] = jnp.dot(own[rows_ref[k]], tiles_ref[k], preferred_element_type=jnp.float32)
        for i, peer in enumerate(targets[far:] + [chip]):
            pair_out[i] = back_product(peer * 2 + 1 - core).astype(jnp.bfloat16)
            to_row(partner, pair_out.at[i], pair_in.at[half, i], pair_send, pair_recv.at[half]).start()
        for i, peer in enumerate(targets[:far]):
            for side, slot in enumerate([peer * 2 + core, peer * 2 + 1 - core]):
                index = 2 * i + side
                back_out[index] = back_product(slot).astype(jnp.bfloat16)
                to_row(
                    slot, back_out.at[index], back_in.at[half, index], back_send, back_recv.at[half]
                ).start()
        keep_own(step)
        if step == 0:
            lax.fori_loop(0, tile_count // 4, turn, 0)
        def send_back():
            to_row(
                partner, pair_out.at[near_rows], pair_in.at[half, near_rows], pair_send, pair_recv.at[half]
            ).wait_recv()
            for i, peer in enumerate(targets[far:]):
                index = 2 * far + i
                back_out[index] = (back_product(peer * 2 + core) + take_pair(i, half)).astype(jnp.bfloat16)
                to_row(
                    peer * 2 + core, back_out.at[index], back_in.at[half, index], back_send, back_recv.at[half]
                ).start()
            total = back_product(r) + take_pair(len(targets) - far, half)
            return total

        if step == 0:
            total = send_back()
        dots = take_gathered(step, half)
        send_dots(step, half, pack_both(step, dots))
        if step > 0:
            total = send_back()
        take_relayed(half)
        forward = [jnp.zeros((width, part), jnp.float32)] * owned
        for k in range(tile_count):
            value = jnp.dot(stage[cols_ref[k]], turned[k], preferred_element_type=jnp.float32)
            for i in range(owned):
                mask = jnp.concatenate([masks[k, i]] * (part // 128), axis=1)
                forward[i] = forward[i] + value * jnp.concatenate([mask] * (width // 8), axis=0)
        for i in range(owned):
            direct_out[i] = forward[i].astype(jnp.bfloat16)
        for peer in grp_peers:
            to_grp(peer, direct_out.at[peer], direct_in.at[g], direct_send, direct_recv).start()
        for i in range(owned):
            total = total + forward[i] * jnp.where(g == i, 1.0, 0.0)
        for slot in range(owner_count):
            history[slot, step * width : (step + 1) * width, :] = stage[slot]
        sent_vectors()
        if step > 0:
            sent_own()
        relays_sent()
        cross, gram = take_dots(step, half)
        left, rest = current, None
        if step > 0:
            left = left - dot_nn(cross, basis[...])
            rest = dot_nn(cross, images[...])
            first = cross + coef
            newest = jnp.where(lane == (step - 1) * width + sub, first, 0.0)
            middle = -jnp.sum(newest, axis=(0, 1), keepdims=True) / width
        upper, inverse = factor_and_inverse(gram)
        now = dot_nn(inverse, left)
        ahead = now * (middle - shift)
        if step > 0:
            ahead = ahead - dot_nn(upper, basis[(step - 1) * width : step * width, :])
        bulk = back_in.at[half, pl.ds(0, chips - 1 + far)]
        to_row(partner, bulk, bulk, back_send, back_recv.at[half]).wait_recv()
        for index in range(chips - 1 + far):
            total = total + back_in[half, index].astype(jnp.float32)
        bulk = direct_in.at[pl.ds(0, others)]
        to_grp(grp_peers[0], bulk, bulk, direct_send, direct_recv).wait_recv()
        for peer in grp_peers:
            total = total + direct_in[peer].astype(jnp.float32)
        total = 0.5 * total
        if step > 0:
            total = total - rest
        image = dot_nn(inverse, total)
        current = image + ahead
        if step < steps - 1:
            send_vectors(1 - half, current.astype(jnp.bfloat16))
        else:
            send_own(current.astype(jnp.bfloat16))
            stage[r] = current.astype(jnp.bfloat16)
            local = pack_both(steps, slot_dots(steps, [r]))
            chip_out[...] = encode(steps, local)
            for i, peer in enumerate(targets):
                to_row(peer * 2 + core, chip_out, chip_in.at[i], chip_send, chip_recv).start()
        basis[step * width : (step + 1) * width, :] = now
        images[step * width : (step + 1) * width, :] = image
        if step > 0:
            proj_ref[step - 1] = first
            fac_ref[step - 1] = upper.T
        unit = jnp.where(lane == step * width + sub, 1.0, 0.0)
        if step == 0:
            transform[:width, :] = dot_nn(inverse, unit)
            coef = -MIDDLE * unit
        else:
            transform[step * width : (step + 1) * width, :] = dot_nn(inverse, unit - dot_nn(cross, transform[...]))
            wide = jnp.concatenate([upper] * (total_cols // width), axis=1)
            coef = -middle * unit + jnp.where((lane >= (step - 1) * width) & (lane < step * width), wide, 0.0)
        bulk = pair_out.at[near_rows]
        to_row(partner, bulk, bulk, pair_send, pair_recv.at[half]).wait_send()
        bulk = back_out.at[pl.ds(0, chips - 1 + far)]
        to_row(partner, bulk, bulk, back_send, back_recv.at[half]).wait_send()
        bulk = direct_out.at[pl.ds(0, others)]
        to_grp(grp_peers[0], bulk, bulk, direct_send, direct_recv).wait_send()
        dots_sent(step, half)

    half = steps % 2
    take_own()
    keep_own(steps)
    sent_own()
    to_row(partner, chip_in, chip_in, chip_send, chip_recv).wait_recv()
    summed = chip_in[0].astype(jnp.float32)
    for i in range(1, chips - 1):
        summed = summed + chip_in[i].astype(jnp.float32)
    send_dots(steps, half, (local[0] + summed[:8] + summed[8:16], local[1] + summed[16:]))
    to_row(partner, chip_in, chip_in, chip_send, chip_recv).wait_send()
    cross, gram = take_dots(steps, half)
    combine = dot_nn(cross, transform[...])
    high = combine.astype(jnp.bfloat16)
    low = (combine - high.astype(jnp.float32)).astype(jnp.bfloat16)
    both = jnp.dot(
        jnp.concatenate([high, low], axis=0), own_history[:total_cols, :], preferred_element_type=jnp.float32
    )
    left = own_history[total_cols:, :].astype(jnp.float32) - both[:width] - both[width:]
    upper, inverse = factor_and_inverse(gram)
    proj_ref[steps - 1] = cross + coef
    fac_ref[steps - 1] = upper.T
    next_ref[...] = dot_nn(inverse, left)
    dots_sent(steps, half)


def hand_on(proj_in, fac_in, next_in, proj_ref, fac_ref, next_ref):
    proj_ref[...] = proj_in[...]
    fac_ref[...] = fac_in[...]
    next_ref[...] = next_in[...]


def per_device(tiles, tile_rows, tile_cols, live_tiles, dual_shift, start_block):
    matrix = tiles[0, 0]
    tile_count, edge = matrix.shape[0], matrix.shape[1]
    width, row_count = start_block.shape
    group_count = lax.axis_size("grp")
    owner_count = lax.axis_size("row")
    owned = row_count // edge
    part = row_count // group_count
    total_cols = ITERS * width
    vmem = pl.BlockSpec(memory_space=pltpu.VMEM)
    smem = pl.BlockSpec(memory_space=pltpu.SMEM)
    hbm = pl.BlockSpec(memory_space=pltpu.HBM)
    dma = pltpu.SemaphoreType.DMA
    chips = owner_count // 2
    far = sum(away(d, chips) > NEAR for d in far_first(chips))
    back_count = chips - 1 + far
    pair_count = chips
    packed = 16 + (ITERS + 1) // 2 * 16
    shapes = (
            jax.ShapeDtypeStruct((ITERS, width, total_cols), jnp.float32),
            jax.ShapeDtypeStruct((ITERS, width, width), jnp.float32),
            jax.ShapeDtypeStruct((width, row_count), jnp.float32),
    )
    outs = pl.pallas_call(
        functools.partial(kernel, ITERS, group_count, owner_count),
        out_shape=tuple(pltpu.VMEM(x.shape, x.dtype) for x in shapes),
        in_specs=[hbm, hbm, hbm, hbm, smem, hbm],
        out_specs=(vmem, vmem, vmem),
        scratch_shapes=[
            pltpu.VMEM((width, row_count), jnp.float32),
            pltpu.VMEM((1, row_count), jnp.float32),
            pltpu.SMEM((tile_count,), jnp.int32),
            pltpu.SMEM((tile_count,), jnp.int32),
            dma((4,)),
            pltpu.VMEM(matrix.shape, jnp.bfloat16),
            pltpu.VMEM(matrix.shape, jnp.bfloat16),
            pltpu.VMEM((tile_count, owned, 8, 128), jnp.float32),
            pltpu.VMEM((tile_count + 1, width, part), jnp.float32),
            pltpu.VMEM((2, owner_count, width, part), jnp.bfloat16),
            pltpu.VMEM((owner_count, width, part), jnp.bfloat16),
            pltpu.VMEM((owner_count, total_cols, part), jnp.bfloat16),
            pltpu.VMEM((group_count, width, part), jnp.bfloat16),
            pltpu.VMEM((total_cols + width, row_count), jnp.bfloat16),
            pltpu.VMEM((back_count, width, part), jnp.bfloat16),
            pltpu.VMEM((2, back_count, width, part), jnp.bfloat16),
            pltpu.VMEM((group_count, width, part), jnp.bfloat16),
            pltpu.VMEM((group_count, width, part), jnp.bfloat16),
            pltpu.VMEM((pair_count, width, part), jnp.bfloat16),
            pltpu.VMEM((2, pair_count, width, part), jnp.bfloat16),
            pltpu.VMEM((2, 2 * group_count, packed, total_cols), jnp.bfloat16),
            pltpu.VMEM((packed, total_cols), jnp.bfloat16),
            pltpu.VMEM((chips - 1, packed, total_cols), jnp.bfloat16),
            pltpu.VMEM((total_cols, part), jnp.float32),
            pltpu.VMEM((total_cols, part), jnp.float32),
            pltpu.VMEM((total_cols, total_cols), jnp.float32),
            pltpu.VMEM((8, owned * owner_count), jnp.int32),
            pltpu.SMEM((8, owned * owner_count), jnp.int32),
            dma, dma,
            dma, dma((2, owner_count // 2 - 1)), dma, dma((2,)), dma, dma,
            dma, dma((2,)), dma, dma((2,)), dma, dma, dma, dma((2,)), dma, dma,
        ],
        compiler_params=pltpu.CompilerParams(
            collective_id=0, has_side_effects=True, vmem_limit_bytes=60 * 1024 * 1024
        ),
    )(start_block, dual_shift[None, :], tile_rows[0, 0], tile_cols[0, 0], live_tiles[0], matrix)
    return pl.pallas_call(hand_on, out_shape=shapes, in_specs=[vmem] * 3, out_specs=(vmem,) * 3,
        compiler_params=pltpu.CompilerParams(vmem_limit_bytes=2 * 1024 * 1024))(*outs)


def solution(mesh):
    in_specs = (
        P("grp", "row", None, None, None),
        P("grp", "row", None),
        P("grp", "row", None),
        P("grp", "row"),
        P("row"),
        P(None, "row"),
    )
    out_specs = (P(), P(), P(None, "row"))
    return jax.shard_map(
        per_device, mesh=mesh, in_specs=in_specs, out_specs=out_specs, check_vma=False
    )
```
